128 devices in a mesh: wide: 16 (over x, z), narrow: 8 (over y, core).
Axes of the slice: x: 4, y: 4, z: 4, core: 2. Of those that a mesh axis runs over, the one named last changes fastest.
Arguments:
- positions: float32 [3, 16384], P(None, ('wide', 'narrow')), may hold values from -1 to 69, as said below
- noise: float32 [3, 16, 16384], P(None, None, ('wide', 'narrow')), may hold values from -6 to 6
Outputs:
- displacement: float32 [3, 16, 16384], P(None, None, ('wide', 'narrow'))
The draws below stay inside these ranges and needn't reach their ends.
Inputs may be any that keep to these rules, and one draw needn't show every extreme that they name: `positions`: any two particles lie at least 1.2 apart.
All inputs are finite; a program needn't handle non-finite values.
Results may differ from the reference program's by a relative error of at most 0.0003.
Values sent between devices are 32-bit elements; how exact they have to be, the bound alone decides.
A program may use at most 64 MiB of HBM per device.

```python
import math
import jax
import jax.numpy as jnp
from jax import lax

S = 16
ITERS = 3
ROOT_STEPS = 30
PARTICLES = 16384


def draw_positions(key, part):
    sites = jnp.arange(PARTICLES, dtype=jnp.int32)
    lattice = jnp.stack([sites % 32, sites // 32 % 32, sites // 1024]).astype(jnp.float32) * 2.2
    jitter = jax.random.uniform(key, (3, PARTICLES), jnp.float32, -0.5, 0.5)
    return lattice + jitter


def shard_levels(stream_key, shape, cuts, smallest, top_value):
    def one(position, blocks):
        draws = jax.random.uniform(jax.random.fold_in(jax.random.fold_in(stream_key, 6), position), (blocks,), jnp.float32, smallest / len(cuts), top_value / len(cuts))
        return jnp.repeat(jnp.exp(draws), shape[position] // blocks).reshape((-1,) + (1,) * (len(shape) - position - 1))

    factor_of = one(*cuts[0])
    for cut in cuts[1:]:
        factor_of = factor_of * one(*cut)
    return factor_of


def normal_values(stream_key, shape, scale, reach, cuts=(), kind=jnp.bfloat16):
    drawn = scale * jax.random.normal(stream_key, shape, jnp.float32)
    if cuts:
        drawn = drawn * shard_levels(stream_key, shape, cuts, -0.22, 0.18)
    return jnp.clip(drawn, -reach, reach).astype(kind)


def setup_inputs(seed: int = 0) -> dict:
    key_list = jax.random.split(jax.random.key(seed), 3)
    positions = draw_positions(jax.random.fold_in(key_list[2], 71), 0)
    noise = normal_values(key_list[1], (3, S, PARTICLES), 1.0, 6.0, ((2, 128),), jnp.float32)
    return dict(positions=positions, noise=noise)


highest = lax.Precision.HIGHEST

def tile_factors(dist_sq, itself):
    safe_sq = jnp.where(itself, 4.0, dist_sq)
    radial = jnp.sqrt(safe_sq)
    inverse = 1.0 / radial
    far_scalar = 0.75 * inverse + 0.5 * inverse * inverse * inverse
    far_outer = (0.75 * inverse - 1.5 * inverse * inverse * inverse) * inverse * inverse
    near_scalar = 1.0 - 0.28125 * radial
    near_outer = 0.09375 * inverse
    nearby = radial < 2.0
    scalar = jnp.where(itself, 1.0, jnp.where(nearby, near_scalar, far_scalar))
    outer_part = jnp.where(itself, 0.0, jnp.where(nearby, near_outer, far_outer))
    return (scalar, outer_part)

def contract(left, kernel):
    return lax.dot_general(left, kernel, (((1,), (1,)), ((), ())), precision=highest, preferred_element_type=jnp.float32)

def tile_product(row_pos, row_ids, col_pos, col_ids, vectors):
    width = vectors.shape[1]
    delta = row_pos[:, :, None] - col_pos[:, None, :]
    dist_sq = delta[0] * delta[0] + delta[1] * delta[1] + delta[2] * delta[2]
    itself = row_ids[:, None] == col_ids[None, :]
    scalar, outer_part = tile_factors(dist_sq, itself)
    result = []
    for component in range(3):
        diag_kernel = scalar + outer_part * delta[component] * delta[component]
        result.append(contract(vectors[component], diag_kernel))
    for first, second in ((0, 1), (0, 2), (1, 2)):
        cross = outer_part * delta[first] * delta[second]
        both = contract(jnp.concatenate([vectors[second], vectors[first]], axis=0), cross)
        result[first] = result[first] + both[:width]
        result[second] = result[second] + both[width:]
    return jnp.stack(result)

def blocked_product(row_pos, row_ids, col_pos, col_ids, vectors):
    rows = row_pos.shape[1]
    block = math.gcd(rows, 512)

    def row_block(index):
        begin = index * block
        pos_block = lax.dynamic_slice_in_dim(row_pos, begin, block, 1)
        id_block = lax.dynamic_slice_in_dim(row_ids, begin, block, 0)
        return tile_product(pos_block, id_block, col_pos, col_ids, vectors)
    pieces = lax.map(row_block, jnp.arange(rows // block, dtype=jnp.int32))
    return jnp.moveaxis(pieces, 0, 2).reshape(3, vectors.shape[1], rows)

def gram_of(left, right):
    return jnp.einsum('asp,atp->st', left, right, precision=highest)

def stacked_gram(stacked, right):
    return jnp.einsum('kasp,atp->kst', stacked, right, precision=highest)

def stacked_remove(stacked, weights):
    return jnp.einsum('kasp,kst->atp', stacked, weights, precision=highest)

def rotate(block, matrix):
    return jnp.einsum('atp,ts->asp', block, matrix, precision=highest)

def cholesky_pair(gram):
    order = gram.shape[0]
    places = jnp.arange(order, dtype=jnp.int32)
    lower = jnp.zeros((order, order), jnp.float32)
    for column in range(order):
        needed = gram[:, column] - jnp.dot(lower, lower[column, :], precision=highest, preferred_element_type=jnp.float32)
        pivot = jnp.sqrt(needed[column])
        entries = jnp.where(places >= column, needed / pivot, 0.0)
        marker = (places == column).astype(jnp.float32)
        lower = lower + entries[:, None] * marker[None, :]
    solved = jnp.zeros((order, order), jnp.float32)
    for row in range(order):
        marker = (places == row).astype(jnp.float32)
        fresh = (marker - jnp.dot(lower[row, :], solved, precision=highest, preferred_element_type=jnp.float32)) / lower[row, row]
        solved = solved + marker[:, None] * fresh[None, :]
    return (lower.T, solved.T)

def tridiagonal(diagonal_blocks, lower_blocks):
    width = diagonal_blocks[0].shape[0]
    order = len(diagonal_blocks) * width
    matrix = jnp.zeros((order, order), jnp.float32)
    for index, block in enumerate(diagonal_blocks):
        offset = index * width
        matrix = matrix.at[offset:offset + width, offset:offset + width].set(block)
    for index, block in enumerate(lower_blocks):
        offset = index * width
        matrix = matrix.at[offset + width:offset + 2 * width, offset:offset + width].set(block)
        matrix = matrix.at[offset:offset + width, offset + width:offset + 2 * width].set(block.T)
    return matrix

def matrix_root(matrix):
    identity = jnp.eye(matrix.shape[0], dtype=jnp.float32)
    scale = jnp.sqrt(jnp.sum(matrix * matrix))

    def newton(turn, carry):
        current, other = carry
        factor = 1.5 * identity - 0.5 * jnp.dot(other, current, precision=highest, preferred_element_type=jnp.float32)
        return (jnp.dot(current, factor, precision=highest, preferred_element_type=jnp.float32), jnp.dot(factor, other, precision=highest, preferred_element_type=jnp.float32))
    current, other = lax.fori_loop(0, ROOT_STEPS, newton, (matrix / scale, identity))
    return current * jnp.sqrt(scale)

def reference(positions, noise):
    width = noise.shape[1]
    ids = jnp.arange(positions.shape[1], dtype=jnp.int32)
    start_upper, start_inverse = cholesky_pair(gram_of(noise, noise))
    basis = [rotate(noise, start_inverse)]
    diagonal_blocks = []
    lower_blocks = []
    for index in range(ITERS):
        image = blocked_product(positions, ids, positions, ids, basis[index])
        stacked = jnp.stack(basis)
        projections = stacked_gram(stacked, image)
        current_block = projections[-1]
        diagonal_blocks.append(0.5 * (current_block + current_block.T))
        if index + 1 < ITERS:
            work = image - stacked_remove(stacked, projections)
            again = stacked_gram(stacked, work)
            work = work - stacked_remove(stacked, again)
            upper, inverse = cholesky_pair(gram_of(work, work))
            lower_blocks.append(upper)
            basis.append(rotate(work, inverse))
    root = matrix_root(tridiagonal(diagonal_blocks, lower_blocks))
    mixing = jnp.dot(root[:, :width], start_upper, precision=highest, preferred_element_type=jnp.float32).reshape(ITERS, width, width)
    return jnp.einsum('katp,kts->asp', jnp.stack(basis), mixing, precision=highest)
```

```python
import functools

import jax
import jax.numpy as jnp
from jax import lax
from jax.experimental import pallas as pl
from jax.experimental.pallas import tpu as pltpu
from jax.sharding import PartitionSpec as P

ROOT_STEPS = 30
NW = 16
NN = 8
S = 16
L = 128
CENTRE = 34.0
MESH = pl.DeviceIdType.MESH
HI = lax.Precision.HIGHEST
F32 = jnp.float32
BF16 = jnp.bfloat16


def mm(a, b):
    return lax.dot_general(a, b, (((1,), (0,)), ((), ())), precision=HI, preferred_element_type=F32)


def mt(a, b):
    return lax.dot_general(a, b, (((1,), (1,)), ((), ())), precision=HI, preferred_element_type=F32)


def eye(n):
    return (lax.broadcasted_iota(jnp.int32, (n, n), 0) == lax.broadcasted_iota(jnp.int32, (n, n), 1)).astype(F32)


def transposed(a):
    return mt(eye(a.shape[1]), a)


def cholesky_pair(gram):
    n = gram.shape[0]
    rows = lax.broadcasted_iota(jnp.int32, (n, n), 0)
    cols = lax.broadcasted_iota(jnp.int32, (n, n), 1)
    left, right = gram, eye(n)
    upper, inverse = jnp.zeros((n, n), F32), jnp.zeros((n, n), F32)
    for c in range(n):
        scale = lax.rsqrt(jnp.broadcast_to(left[c : c + 1, c : c + 1], (1, n)))
        row = left[c : c + 1, :] * scale
        other = right[c : c + 1, :] * scale
        upper = jnp.where((rows == c) & (cols >= c), jnp.broadcast_to(row, (n, n)), upper)
        inverse = jnp.where((rows == c) & (cols <= c), jnp.broadcast_to(other, (n, n)), inverse)
        if c + 1 < n:
            factor = jnp.broadcast_to(left[:, c : c + 1], (n, n)) * scale
            left = left - factor * row
            right = right - jnp.where(rows > c, factor * other, 0.0)
    return upper, inverse


def split(value):
    high = value.astype(BF16)
    low = (value - high.astype(F32)).astype(BF16)
    return high, low


def main_kernel(
    pos_ref,
    noise_ref,
    vec_ref,
    small_ref,
    tot_ref,
    ztot_ref,
    cpos,
    rpos,
    xg0,
    xg1,
    xg2,
    xr,
    pb1,
    pb2,
    rb1,
    rb2,
    pz,
    lhi,
    llo,
    rmat,
    acc,
    accl,
    xjb,
    ga1,
    gb1,
    ga2,
    gb2,
    za,
    zb,
    send_w,
    recv_w,
    send_n,
    recv_n,
):
    w = lax.axis_index("wide")
    n = lax.axis_index("narrow")

    def wide_copy(phase, src, dst, target, slot):
        return pltpu.make_async_remote_copy(
            src_ref=src,
            dst_ref=dst.at[slot],
            send_sem=send_w.at[phase, target],
            recv_sem=recv_w.at[phase, slot],
            device_id={"wide": target},
            device_id_type=MESH,
        )

    def narrow_copy(phase, src, dst, target, slot):
        return pltpu.make_async_remote_copy(
            src_ref=src,
            dst_ref=dst.at[slot],
            send_sem=send_n.at[phase, target],
            recv_sem=recv_n.at[phase, slot],
            device_id={"narrow": target},
            device_id_type=MESH,
        )

    def loop(count, body):
        def step(i, carry):
            body(i)
            return carry

        lax.fori_loop(0, count, step, 0)

    def wide_send(phase, dst):
        loop(NW - 1, lambda p: wide_copy(phase, dst.at[w], dst, lax.rem(w + p + 1, NW), w).start())

    def wide_recv(phase, dst):
        def one(p):
            s = lax.rem(w + p + 1, NW)
            wide_copy(phase, dst.at[s], dst, s, s).wait_recv()

        loop(NW - 1, one)

    def wide_sent(phase, dst):
        def one(p):
            s = lax.rem(w + p + 1, NW)
            wide_copy(phase, dst.at[w], dst, s, w).wait_send()

        loop(NW - 1, one)

    def narrow_send(phase, dst, scatter=None):
        def one(p):
            t = lax.rem(n + p + 1, NN)
            narrow_copy(phase, dst.at[n] if scatter is None else scatter.at[t], dst, t, n).start()

        loop(NN - 1, one)

    def narrow_recv(phase, dst):
        def one(p):
            s = lax.rem(n + p + 1, NN)
            narrow_copy(phase, dst.at[s], dst, s, s).wait_recv()

        loop(NN - 1, one)

    def narrow_sent(phase, dst):
        def one(p):
            s = lax.rem(n + p + 1, NN)
            narrow_copy(phase, dst.at[n], dst, s, n).wait_send()

        loop(NN - 1, one)

    def all_of(buffer, count):
        total = buffer[0]
        for i in range(1, count):
            total = total + buffer[i]
        return total

    barrier = pltpu.get_barrier_semaphore()

    def greet_wide(p):
        pl.semaphore_signal(barrier, inc=1, device_id={"wide": lax.rem(w + p + 1, NW)}, device_id_type=MESH)

    def greet_narrow(p):
        pl.semaphore_signal(barrier, inc=1, device_id={"narrow": lax.rem(n + p + 1, NN)}, device_id_type=MESH)

    loop(NW - 1, greet_wide)
    loop(NN - 1, greet_narrow)
    own_pos = jnp.concatenate([pos_ref[...], jnp.zeros((5, L), F32)], axis=0)
    cpos[w] = own_pos
    rpos[n] = own_pos
    xg0[w] = noise_ref[...]
    za[n] = jnp.zeros((S, L), F32)
    pl.semaphore_wait(barrier, NW + NN - 2)

    wide_send(0, cpos)
    narrow_send(0, rpos)
    wide_send(1, xg0)
    narrow_recv(0, rpos)
    wide_recv(0, cpos)

    def build(jb):
        columns = cpos[jb].T
        for c in range(3):
            xjb[c] = jnp.broadcast_to(columns[:, c : c + 1], (L, L))

        def rows_of(ic):
            for half in range(2):
                ib = ic * 2 + half
                xi = [jnp.broadcast_to(rpos[ib, c : c + 1, :], (16, L)) for c in range(3)]
                lanes = pl.ds(pl.multiple_of(ib * L, L), L)
                for jt in range(8):
                    d = [xi[c] - xjb[c, jt * 16 : jt * 16 + 16, :] for c in range(3)]
                    sq = jnp.maximum(d[0] * d[0] + d[1] * d[1] + d[2] * d[2], 1e-20)
                    inv = lax.rsqrt(sq)
                    inv2 = inv * inv
                    near = sq < 4.0
                    iso = jnp.where(near, 1.0 - 0.28125 * (sq * inv), inv * (0.75 + 0.5 * inv2))
                    outer = inv * jnp.where(near, 0.09375, inv2 * (0.75 - 1.5 * inv2))
                    places = pl.ds(pl.multiple_of(jb * L + jt * 16, 16), 16)
                    for k, value in enumerate([outer * d[0], outer * d[1], outer * d[2], iso]):
                        high, low = split(value)
                        lhi[k, places, lanes] = high
                        llo[k, places, lanes] = low

        loop(NN // 2, rows_of)

    loop(NW, build)

    def product(xg, out):
        def expand(jb):
            lanes = pl.ds(pl.multiple_of(jb * L, L), L)
            x = [cpos[jb, c : c + 1, :] - CENTRE for c in range(3)]
            v = [xg[jb, e] for e in range(3)]
            pieces = [jnp.concatenate([v[e], x[0] * v[e], x[1] * v[e], x[2] * v[e]], axis=0) for e in range(3)]
            pieces.append(jnp.concatenate([jnp.zeros((S, L), F32), -v[0], -v[1], -v[2]], axis=0))
            for k in range(4):
                high, low = split(pieces[k])
                rmat[k, 0:64, lanes] = high
                rmat[k, 64:128, lanes] = low

        loop(NW, expand)
        acc[...] = jnp.zeros_like(acc)
        accl[...] = jnp.zeros_like(accl)

        def multiply(k):
            acc[...] += jnp.dot(rmat[k], lhi[k], preferred_element_type=F32)
            accl[...] += jnp.dot(rmat[k, 0:64, :], llo[k], preferred_element_type=F32)

        loop(4, multiply)
        for b in range(NN):
            lanes = slice(b * L, b * L + L)
            total = acc[0:64, lanes] + (acc[64:128, lanes] + accl[:, lanes])
            for c in range(3):
                out[b, c] = (rpos[b, c : c + 1, :] - CENTRE) * total[0:16] - total[16 + 16 * c : 32 + 16 * c]

    lane = lax.broadcasted_iota(jnp.int32, (S, L), 1)

    wide_recv(1, xg0)
    product(xg0, pb1)
    rb1[n] = pb1[n]
    narrow_send(1, rb1, pb1)
    narrow_recv(1, rb1)
    xg1[w] = all_of(rb1, NN)
    wide_send(2, xg1)

    part = jnp.zeros((2 * S, L), F32)
    for c in range(3):
        a, b = noise_ref[c], xg1[w, c]
        part = part + mt(jnp.concatenate([a, b], axis=0), jnp.concatenate([a, b, b, b, b, b, b, b], axis=0))
    ga1[n] = jnp.where(lane < 32, part[0:16], part[16:32])
    narrow_send(2, ga1)
    narrow_recv(2, ga1)
    gb1[w] = all_of(ga1, NN)
    wide_send(3, gb1)

    wide_recv(2, xg1)
    product(xg1, pb2)
    rb2[n] = pb2[n]
    narrow_send(3, rb2, pb2)
    narrow_recv(3, rb2)
    y1 = all_of(rb2, NN)
    xg2[w] = y1
    xr[n] = y1
    wide_send(4, xg2)
    narrow_send(4, xr)

    wide_recv(3, gb1)
    total = all_of(gb1, NW)
    g00, g01, g11 = total[:, 0:16], total[:, 16:32], total[:, 32:48]
    upper0, inv0 = cholesky_pair(g00)

    def inside(g):
        return mt(mm(inv0, g), inv0)

    h1, c11, k1 = inside(g01), inside(g00), inside(g11)
    f1 = h1 + (h1 - mm(c11, h1))
    f1t = transposed(f1)
    fh = mm(f1t, h1)
    gram = k1 - fh - transposed(fh) + mm(f1t, mm(c11, f1))
    upper1, inv1 = cholesky_pair(gram)
    p21t = mm(inv1, inv0)
    p20t = -mm(mm(inv1, f1t), inv0)
    for c in range(3):
        a, b, d = noise_ref[c], xg1[w, c], xg2[w, c]
        vec_ref[0, c] = mm(inv0, a)
        vec_ref[1, c] = mm(p20t, a) + mm(p21t, b)
        vec_ref[2, c] = mm(p20t, b) + mm(p21t, d)
    for i, value in enumerate([upper0, upper1, h1, f1, p20t, p21t]):
        small_ref[i] = value

    part = jnp.zeros((5 * S, L), F32)
    for c in range(3):
        q1, q2, wv, y0, y1 = vec_ref[0, c], vec_ref[1, c], vec_ref[2, c], xg1[w, c], xg2[w, c]
        part = part + mt(
            jnp.concatenate([q1, q2, wv, y0, y1], axis=0), jnp.concatenate([q1, q2, wv, q2, wv, wv, y1, y1], axis=0)
        )
    packed = jnp.where(lane < 48, part[0:16], part[16:32])
    packed = jnp.where(lane < 80, packed, part[32:48])
    packed = jnp.where(lane < 96, packed, part[48:64])
    ga2[n] = jnp.where(lane < 112, packed, part[64:80])
    narrow_send(5, ga2)
    narrow_recv(5, ga2)
    gb2[w] = all_of(ga2, NN)
    wide_send(5, gb2)

    wide_recv(4, xg2)
    product(xg2, pz)
    narrow_recv(4, xr)
    part = jnp.zeros((S, S), F32)
    for c in range(3):
        part = part + mt(
            jnp.concatenate([xr[b, c] for b in range(NN)], axis=1), jnp.concatenate([pz[b, c] for b in range(NN)], axis=1)
        )
    za[n, :, 0:16] = part
    narrow_send(6, za)
    narrow_recv(6, za)
    zb[w] = all_of(za, NN)
    wide_send(6, zb)
    wide_recv(5, gb2)
    tot_ref[...] = all_of(gb2, NW)
    wide_recv(6, zb)
    ztot_ref[...] = all_of(zb, NW)

    for phase, buffer in enumerate([cpos, xg0, xg1, gb1, xg2, gb2, zb]):
        wide_sent(phase, buffer)
    for phase, buffer in enumerate([rpos, rb1, ga1, rb2, xr, ga2, za]):
        narrow_sent(phase, buffer)


def last_kernel(vec_ref, small_ref, tot_ref, ztot_ref, out_ref, y_ref, z_ref):
    upper0, upper1, h1, f1, p20t, p21t = [small_ref[i] for i in range(6)]
    total = tot_ref[...]
    c11, c12, ha, c22, hb, k, g12, g22 = [total[:, 16 * i : 16 * i + 16] for i in range(8)]
    zraw = ztot_ref[:, 0:16]
    p20, p21 = transposed(p20t), transposed(p21t)
    ga = ha - mm(c11, ha) - mm(c12, hb)
    gb = hb - mm(transposed(c12), ha) - mm(c22, hb)
    fa, fb = ha + ga, hb + gb
    fat, fbt = transposed(fa), transposed(fb)
    hat, hbt = transposed(ha), transposed(hb)
    fh = mm(fat, ha) + mm(fbt, hb)
    cf = mm(fat, mm(c11, fa) + mm(c12, fb)) + mm(fbt, mm(transposed(c12), fa) + mm(c22, fb))
    upper2, inv2 = cholesky_pair(k - fh - transposed(fh) + cf)
    zz = mm(p20t, mm(g12, p20) + mm(g22, p21)) + mm(p21t, mm(g22, p20) + mm(zraw, p21))
    wmq1 = mm(hat, f1) + mm(hbt, upper1)
    side = mm(wmq1, fa) + mm(k, fb)
    inner = zz - side - transposed(side) + mm(fat, mm(h1, fa) + mm(ha, fb)) + mm(fbt, mm(hat, fa) + mm(hb, fb))
    a3 = mt(mm(inv2, inner), inv2)

    def sym(a):
        return 0.5 * (a + transposed(a))

    order = 3 * S
    tri = jnp.zeros((order, order), F32)
    low = [
        (lax.broadcasted_iota(jnp.int32, (order, S), 0) == lax.broadcasted_iota(jnp.int32, (order, S), 1) + S * i).astype(F32)
        for i in range(3)
    ]
    blocks = [(0, 0, sym(h1)), (1, 1, sym(hb)), (2, 2, sym(a3)), (1, 0, upper1), (2, 1, upper2)]
    blocks += [(0, 1, transposed(upper1)), (1, 2, transposed(upper2))]
    for i, j, block in blocks:
        tri = tri + mt(mm(low[i], block), low[j])
    scale = jnp.sqrt(jnp.sum(tri * tri))
    ident = eye(order)
    y_ref[...] = tri / scale
    z_ref[...] = ident

    def more(carry):
        step, gap = carry
        return jnp.logical_and(step < ROOT_STEPS, jnp.logical_not(gap < 1e-8))

    def newton(carry):
        step, _ = carry
        y, z = y_ref[...], z_ref[...]
        zy = mm(z, y)
        factor = 1.5 * ident - 0.5 * zy
        y_ref[...] = mm(y, factor)
        z_ref[...] = mm(factor, z)
        off = zy - ident
        return step + 1, jnp.sum(off * off)

    lax.while_loop(more, newton, (jnp.int32(0), jnp.float32(1.0)))
    root = y_ref[...] * jnp.sqrt(scale)
    mixing = mm(transposed(upper0), mt(transposed(low[0]), root))
    for c in range(3):
        q1, q2, wv = vec_ref[0, c], vec_ref[1, c], vec_ref[2, c]
        q3 = mm(inv2, wv - mm(fat, q1) - mm(fbt, q2))
        out_ref[c] = mm(mixing, jnp.concatenate([q1, q2, q3], axis=0))


def per_device(positions, noise):
    block = (3, S, L)
    vmem = pl.BlockSpec(memory_space=pltpu.VMEM)
    vec, small, tot, ztot = pl.pallas_call(
        main_kernel,
        out_shape=[
            jax.ShapeDtypeStruct((3, *block), F32),
            jax.ShapeDtypeStruct((6, S, S), F32),
            jax.ShapeDtypeStruct((S, L), F32),
            jax.ShapeDtypeStruct((S, L), F32),
        ],
        in_specs=[vmem] * 2,
        out_specs=[vmem] * 4,
        scratch_shapes=[
            pltpu.VMEM((NW, 8, L), F32),
            pltpu.VMEM((NN, 8, L), F32),
            pltpu.VMEM((NW, *block), F32),
            pltpu.VMEM((NW, *block), F32),
            pltpu.VMEM((NW, *block), F32),
            pltpu.VMEM((NN, *block), F32),
            pltpu.VMEM((NN, *block), F32),
            pltpu.VMEM((NN, *block), F32),
            pltpu.VMEM((NN, *block), F32),
            pltpu.VMEM((NN, *block), F32),
            pltpu.VMEM((NN, *block), F32),
            pltpu.VMEM((4, NW * L, NN * L), BF16),
            pltpu.VMEM((4, NW * L, NN * L), BF16),
            pltpu.VMEM((4, L, NW * L), BF16),
            pltpu.VMEM((L, NN * L), F32),
            pltpu.VMEM((64, NN * L), F32),
            pltpu.VMEM((3, L, L), F32),
            pltpu.VMEM((NN, S, L), F32),
            pltpu.VMEM((NW, S, L), F32),
            pltpu.VMEM((NN, S, L), F32),
            pltpu.VMEM((NW, S, L), F32),
            pltpu.VMEM((NN, S, L), F32),
            pltpu.VMEM((NW, S, L), F32),
            pltpu.SemaphoreType.DMA((7, NW)),
            pltpu.SemaphoreType.DMA((7, NW)),
            pltpu.SemaphoreType.DMA((7, NN)),
            pltpu.SemaphoreType.DMA((7, NN)),
        ],
        compiler_params=pltpu.CompilerParams(
            collective_id=0, has_side_effects=True, vmem_limit_bytes=56 * 1024 * 1024
        ),
        name="lanczos",
    )(positions, noise)
    return pl.pallas_call(
        last_kernel,
        out_shape=jax.ShapeDtypeStruct(block, F32),
        in_specs=[vmem] * 4,
        out_specs=vmem,
        scratch_shapes=[pltpu.VMEM((3 * S, 3 * S), F32), pltpu.VMEM((3 * S, 3 * S), F32)],
        name="finish",
    )(vec, small, tot, ztot)


def solution(mesh):
    axes = ("wide", "narrow")
    return jax.shard_map(
        per_device,
        mesh=mesh,
        in_specs=(P(None, axes), P(None, None, axes)),
        out_specs=P(None, None, axes),
        check_vma=False,
    )
```

```python
import functools

import jax
import jax.numpy as jnp
from jax import lax
from jax.experimental import pallas as pl
from jax.experimental.pallas import tpu as pltpu
from jax.sharding import PartitionSpec as P

ROOT_STEPS = 30
NW = 16
NN = 8
S = 16
L = 128
CENTRE = 34.0
MESH = pl.DeviceIdType.MESH
HI = lax.Precision.HIGHEST
F32 = jnp.float32
BF16 = jnp.bfloat16


def mm(a, b):
    return lax.dot_general(a, b, (((1,), (0,)), ((), ())), precision=HI, preferred_element_type=F32)


def mt(a, b):
    return lax.dot_general(a, b, (((1,), (1,)), ((), ())), precision=HI, preferred_element_type=F32)


def eye(n):
    return (lax.broadcasted_iota(jnp.int32, (n, n), 0) == lax.broadcasted_iota(jnp.int32, (n, n), 1)).astype(F32)


def transposed(a):
    return mt(eye(a.shape[1]), a)


def cholesky_pair(gram):
    n = gram.shape[0]
    rows = lax.broadcasted_iota(jnp.int32, (n, n), 0)
    cols = lax.broadcasted_iota(jnp.int32, (n, n), 1)
    left, right = gram, eye(n)
    upper, inverse = jnp.zeros((n, n), F32), jnp.zeros((n, n), F32)
    for c in range(n):
        scale = lax.rsqrt(jnp.broadcast_to(left[c : c + 1, c : c + 1], (1, n)))
        row = left[c : c + 1, :] * scale
        other = right[c : c + 1, :] * scale
        upper = jnp.where((rows == c) & (cols >= c), jnp.broadcast_to(row, (n, n)), upper)
        inverse = jnp.where((rows == c) & (cols <= c), jnp.broadcast_to(other, (n, n)), inverse)
        if c + 1 < n:
            factor = jnp.broadcast_to(left[:, c : c + 1], (n, n)) * scale
            left = left - factor * row
            right = right - jnp.where(rows > c, factor * other, 0.0)
    return upper, inverse


def split(value):
    high = value.astype(BF16)
    low = (value - high.astype(F32)).astype(BF16)
    return high, low


def hops(offset):
    return sum(min(part, 4 - part) for part in offset)


OFFSETS = sorted([(a, b) for a in range(4) for b in range(4)], key=hops)


def main_kernel(
    pos_hbm,
    noise_hbm,
    vec_ref,
    tri_ref,
    mix_ref,
    low_ref,
    ztot_ref,
    cpos,
    rpos,
    xg0,
    xg1,
    xg2,
    xr,
    pb1,
    pb2,
    rb1,
    rb2,
    pz,
    lhi,
    llo,
    rmat,
    acc,
    accl,
    xjb,
    ga1,
    gb1,
    ga2,
    gb2,
    za,
    zb,
    send_b,
    recv_b,
    send_w,
    recv_w,
    send_n,
    recv_n,
    load_sem,
):
    w = lax.axis_index("wide")
    n = lax.axis_index("narrow")

    def loop(begin, end, body):
        def step(i, carry):
            body(i)
            return carry

        lax.fori_loop(begin, end, step, 0)

    def block_copy(phase, buffer, p):
        a, b = OFFSETS[p]
        x = lax.rem(w // 4 + 4 - a, 4)
        z = lax.rem(lax.rem(w, 4) + 4 - b, 4)
        return pltpu.make_async_remote_copy(
            src_ref=buffer.at[0],
            dst_ref=buffer.at[p],
            send_sem=send_b.at[phase, p],
            recv_sem=recv_b.at[phase, p],
            device_id={"wide": x * 4 + z},
            device_id_type=MESH,
        )

    def block_send(phase, buffer):
        for p in range(1, NW):
            block_copy(phase, buffer, p).start()

    def block_arrived(phase, buffer, p):
        pltpu.make_async_remote_copy(
            src_ref=buffer.at[0],
            dst_ref=buffer.at[p],
            send_sem=send_b.at[phase, p],
            recv_sem=recv_b.at[phase, p],
            device_id={"wide": w},
            device_id_type=MESH,
        ).wait_recv()

    def wide_copy(phase, src, dst, target, slot):
        return pltpu.make_async_remote_copy(
            src_ref=src,
            dst_ref=dst.at[slot],
            send_sem=send_w.at[phase, target],
            recv_sem=recv_w.at[phase, slot],
            device_id={"wide": target},
            device_id_type=MESH,
        )

    def narrow_copy(phase, src, dst, target, slot):
        return pltpu.make_async_remote_copy(
            src_ref=src,
            dst_ref=dst.at[slot],
            send_sem=send_n.at[phase, target],
            recv_sem=recv_n.at[phase, slot],
            device_id={"narrow": target},
            device_id_type=MESH,
        )

    def wide_send(phase, dst):
        loop(1, NW, lambda p: wide_copy(phase, dst.at[w], dst, lax.rem(w + p, NW), w).start())

    def wide_recv(phase, dst):
        def one(p):
            s = lax.rem(w + p, NW)
            wide_copy(phase, dst.at[s], dst, s, s).wait_recv()

        loop(1, NW, one)

    def wide_sent(phase, dst):
        def one(p):
            s = lax.rem(w + p, NW)
            wide_copy(phase, dst.at[w], dst, s, w).wait_send()

        loop(1, NW, one)

    def narrow_send(phase, dst, src=None, scatter=None):
        def one(p):
            t = lax.rem(n + p, NN)
            source = dst.at[n] if src is None else src
            narrow_copy(phase, source if scatter is None else scatter.at[t], dst, t, n).start()

        loop(1, NN, one)

    def narrow_recv(phase, dst):
        def one(p):
            s = lax.rem(n + p, NN)
            narrow_copy(phase, dst.at[s], dst, s, s).wait_recv()

        loop(1, NN, one)

    def narrow_sent(phase, dst):
        def one(p):
            s = lax.rem(n + p, NN)
            narrow_copy(phase, dst.at[n], dst, s, n).wait_send()

        loop(1, NN, one)

    def all_of(buffer, count):
        parts = [buffer[i] for i in range(count)]
        while len(parts) > 1:
            parts = [parts[i] + parts[i + 1] for i in range(0, len(parts), 2)]
        return parts[0]

    barrier = pltpu.get_barrier_semaphore()

    def greet_wide(p):
        pl.semaphore_signal(barrier, inc=1, device_id={"wide": lax.rem(w + p, NW)}, device_id_type=MESH)

    def greet_narrow(p):
        pl.semaphore_signal(barrier, inc=1, device_id={"narrow": lax.rem(n + p, NN)}, device_id_type=MESH)

    loop(1, NW, greet_wide)
    loop(1, NN, greet_narrow)
    loads = [
        pltpu.make_async_copy(pos_hbm, cpos.at[0], load_sem.at[0]),
        pltpu.make_async_copy(noise_hbm, xg0.at[0], load_sem.at[1]),
    ]
    for load in loads:
        load.start()
    za[n] = jnp.zeros((S, L), F32)
    for load in loads:
        load.wait()
    rpos[n] = cpos[0]
    pl.semaphore_wait(barrier, NW + NN - 2)

    narrow_send(0, rpos, src=cpos.at[0])
    block_send(0, cpos)
    block_send(1, xg0)
    narrow_recv(0, rpos)

    def build(jb):
        columns = jnp.concatenate([cpos[jb], jnp.zeros((5, L), F32)], axis=0).T
        for c in range(3):
            xjb[c] = jnp.broadcast_to(columns[:, c : c + 1], (L, L))

        def rows_of(ic):
            for half in range(2):
                ib = ic * 2 + half
                xi = [jnp.broadcast_to(rpos[ib, c : c + 1, :], (16, L)) for c in range(3)]
                for jt in range(8):
                    d = [xi[c] - xjb[c, jt * 16 : jt * 16 + 16, :] for c in range(3)]
                    sq = jnp.maximum(d[0] * d[0] + d[1] * d[1] + d[2] * d[2], 1e-20)
                    inv = lax.rsqrt(sq)
                    inv2 = inv * inv
                    near = sq < 4.0
                    iso = jnp.where(near, 1.0 - 0.28125 * (sq * inv), inv * (0.75 + 0.5 * inv2))
                    outer = inv * jnp.where(near, 0.09375, inv2 * (0.75 - 1.5 * inv2))
                    places = pl.ds(pl.multiple_of(jb * L + jt * 16, 16), 16)
                    for k, value in enumerate([outer * d[0], outer * d[1], outer * d[2], iso]):
                        high, low = split(value)
                        lhi[k, ib, places, :] = high
                        llo[k, ib, places, :] = low

        loop(0, NN // 2, rows_of)

    build(0)

    def arrived_build(p):
        block_arrived(0, cpos, p)
        build(p)

    loop(1, NW, arrived_build)

    half_blocks = NW // 2
    depth = half_blocks * L

    def product(phase, xg, out):
        def expand(p):
            lanes = pl.ds(pl.multiple_of(lax.rem(p, half_blocks) * L, L), L)
            half = p // half_blocks
            x = [cpos[p, c : c + 1, :] - CENTRE for c in range(3)]
            v = [xg[p, e] for e in range(3)]
            pieces = [jnp.concatenate([v[e], x[0] * v[e], x[1] * v[e], x[2] * v[e]], axis=0) for e in range(3)]
            pieces.append(jnp.concatenate([jnp.zeros((S, L), F32), -v[0], -v[1], -v[2]], axis=0))
            for k in range(4):
                high, low = split(pieces[k])
                rmat[half, k, 0:64, lanes] = high
                rmat[half, k, 64:128, lanes] = low

        def arrived_expand(p):
            block_arrived(phase, xg, p)
            expand(p)

        acc[...] = jnp.zeros_like(acc)
        accl[...] = jnp.zeros_like(accl)
        expand(0)
        for half in range(2):
            loop(max(1, half * half_blocks), (half + 1) * half_blocks, arrived_expand)
            rows = slice(half * depth, (half + 1) * depth)

            def multiply(k):
                high = jnp.concatenate([lhi[k, ib, rows, :] for ib in range(NN)], axis=1)
                low = jnp.concatenate([llo[k, ib, rows, :] for ib in range(NN)], axis=1)
                acc[...] += jnp.dot(rmat[half, k], high, preferred_element_type=F32)
                accl[...] += jnp.dot(rmat[half, k, 0:64, :], low, preferred_element_type=F32)

            loop(0, 4, multiply)
        for b in range(NN):
            lanes = slice(b * L, b * L + L)
            total = acc[0:64, lanes] + (acc[64:128, lanes] + accl[:, lanes])
            for c in range(3):
                out[b, c] = (rpos[b, c : c + 1, :] - CENTRE) * total[0:16] - total[16 + 16 * c : 32 + 16 * c]

    lane = lax.broadcasted_iota(jnp.int32, (S, L), 1)

    product(1, xg0, pb1)
    rb1[n] = pb1[n]
    narrow_send(1, rb1, scatter=pb1)
    narrow_recv(1, rb1)
    xg1[0] = all_of(rb1, NN)
    block_send(2, xg1)

    part = jnp.zeros((2 * S, L), F32)
    for c in range(3):
        a, b = xg0[0, c], xg1[0, c]
        part = part + mt(jnp.concatenate([a, b], axis=0), jnp.concatenate([a, b, b, b, b, b, b, b], axis=0))
    ga1[n] = jnp.where(lane < 32, part[0:16], part[16:32])
    narrow_send(2, ga1)
    narrow_recv(2, ga1)
    gb1[w] = all_of(ga1, NN)
    wide_send(0, gb1)

    product(2, xg1, pb2)
    rb2[n] = pb2[n]
    narrow_send(3, rb2, scatter=pb2)
    narrow_recv(3, rb2)
    y1 = all_of(rb2, NN)
    xg2[0] = y1
    block_send(3, xg2)
    xr[n] = y1
    narrow_send(4, xr)

    wide_recv(0, gb1)
    total = all_of(gb1, NW)
    g00, g01, g11 = total[:, 0:16], total[:, 16:32], total[:, 32:48]
    upper0, inv0 = cholesky_pair(g00)

    def inside(g):
        return mt(mm(inv0, g), inv0)

    h1, c11, k1 = inside(g01), inside(g00), inside(g11)
    f1 = h1 + (h1 - mm(c11, h1))
    f1t = transposed(f1)
    fh = mm(f1t, h1)
    gram = k1 - fh - transposed(fh) + mm(f1t, mm(c11, f1))
    upper1, inv1 = cholesky_pair(gram)
    p21t = mm(inv1, inv0)
    p20t = -mm(mm(inv1, f1t), inv0)
    part = jnp.zeros((5 * S, L), F32)
    for c in range(3):
        a, y0, y1c = xg0[0, c], xg1[0, c], xg2[0, c]
        q1 = mm(inv0, a)
        q2 = mm(p20t, a) + mm(p21t, y0)
        wv = mm(p20t, y0) + mm(p21t, y1c)
        vec_ref[c, 0:16] = q1
        vec_ref[c, 16:32] = q2
        vec_ref[c, 32:48] = wv
        part = part + mt(
            jnp.concatenate([q1, q2, wv, y0, y1c], axis=0), jnp.concatenate([q1, q2, wv, q2, wv, wv, y1c, y1c], axis=0)
        )
    packed = jnp.where(lane < 48, part[0:16], part[16:32])
    packed = jnp.where(lane < 80, packed, part[32:48])
    packed = jnp.where(lane < 96, packed, part[48:64])
    ga2[n] = jnp.where(lane < 112, packed, part[64:80])
    narrow_send(5, ga2)
    narrow_recv(5, ga2)
    gb2[w] = all_of(ga2, NN)
    wide_send(1, gb2)

    product(3, xg2, pz)
    narrow_recv(4, xr)
    part = jnp.zeros((S, S), F32)
    for c in range(3):
        part = part + mt(
            jnp.concatenate([xr[b, c] for b in range(NN)], axis=1), jnp.concatenate([pz[b, c] for b in range(NN)], axis=1)
        )
    za[n, :, 0:16] = part
    narrow_send(6, za)
    wide_recv(1, gb2)
    total = all_of(gb2, NW)
    narrow_recv(6, za)
    zb[w] = all_of(za, NN)
    wide_send(2, zb)

    c11, c12, ha, c22, hb, k, g12, g22 = [total[:, 16 * i : 16 * i + 16] for i in range(8)]
    p20, p21 = transposed(p20t), transposed(p21t)
    c12t = transposed(c12)
    fa = ha + (ha - mm(c11, ha) - mm(c12, hb))
    fb = hb + (hb - mm(c12t, ha) - mm(c22, hb))
    fat, fbt = transposed(fa), transposed(fb)
    hat, hbt = transposed(ha), transposed(hb)
    fh = mm(fat, ha) + mm(fbt, hb)
    cf = mm(fat, mm(c11, fa) + mm(c12, fb)) + mm(fbt, mm(c12t, fa) + mm(c22, fb))
    upper2, inv2 = cholesky_pair(k - fh - transposed(fh) + cf)
    zz = mm(p20t, mm(g12, p20) + mm(g22, p21)) + mm(p21t, mm(g22, p20))
    wmq1 = mm(hat, f1) + mm(hbt, upper1)
    side = mm(wmq1, fa) + mm(k, fb)
    inner = zz - side - transposed(side) + mm(fat, mm(h1, fa) + mm(ha, fb)) + mm(fbt, mm(hat, fa) + mm(hb, fb))
    a3 = mt(mm(inv2, inner), inv2)

    def sym(value):
        return 0.5 * (value + transposed(value))

    order = 3 * S
    tri = jnp.zeros((order, order), F32)
    low = [
        (lax.broadcasted_iota(jnp.int32, (order, S), 0) == lax.broadcasted_iota(jnp.int32, (order, S), 1) + S * i).astype(F32)
        for i in range(3)
    ]
    blocks = [(0, 0, sym(h1)), (1, 1, sym(hb)), (2, 2, sym(a3)), (1, 0, upper1), (2, 1, upper2)]
    blocks += [(0, 1, transposed(upper1)), (1, 2, transposed(upper2))]
    for i, j, block in blocks:
        tri = tri + mt(mm(low[i], block), low[j])
    tri_ref[...] = tri
    mix_ref[...] = mm(low[2], mm(inv2, p21t))
    low_ref[...] = transposed(upper0)
    for c in range(3):
        q1, q2, wv = vec_ref[c, 0:16], vec_ref[c, 16:32], vec_ref[c, 32:48]
        vec_ref[c, 32:48] = mm(inv2, wv - mm(fat, q1) - mm(fbt, q2))
    wide_recv(2, zb)
    ztot_ref[...] = all_of(zb, NW)

    for phase, buffer in enumerate([cpos, xg0, xg1, xg2]):
        for p in range(1, NW):
            block_copy(phase, buffer, p).wait_send()
    for phase, buffer in enumerate([gb1, gb2, zb]):
        wide_sent(phase, buffer)
    for phase, buffer in enumerate([rpos, rb1, ga1, rb2, xr, ga2, za]):
        narrow_sent(phase, buffer)


def last_kernel(vec_ref, tri_ref, mix_ref, low_ref, ztot_ref, out_ref, y_ref, z_ref):
    zraw = ztot_ref[:, 0:16]
    mix = mix_ref[...]
    tri = tri_ref[...] + mt(mm(mix, 0.5 * (zraw + transposed(zraw))), mix)
    order = 3 * S
    scale = jnp.sqrt(jnp.sum(tri * tri))
    ident = eye(order)
    y_ref[...] = tri / scale
    z_ref[...] = ident

    def more(carry):
        step, gap = carry
        return jnp.logical_and(step < ROOT_STEPS, jnp.logical_not(gap < 1e-8))

    def newton(carry):
        step, _ = carry
        y, z = y_ref[...], z_ref[...]
        zy = mm(z, y)
        factor = 1.5 * ident - 0.5 * zy
        y_ref[...] = mm(y, factor)
        z_ref[...] = mm(factor, z)
        off = zy - ident
        return step + 1, jnp.sum(off * off)

    lax.while_loop(more, newton, (jnp.int32(0), jnp.float32(1.0)))
    root = y_ref[...] * jnp.sqrt(scale)
    first = (
        lax.broadcasted_iota(jnp.int32, (S, order), 0) == lax.broadcasted_iota(jnp.int32, (S, order), 1)
    ).astype(F32)
    mixing = mm(low_ref[...], mt(first, root))
    for c in range(3):
        out_ref[c] = mm(mixing, vec_ref[c])


def per_device(positions, noise):
    block = (3, S, L)
    order = 3 * S
    vmem = pl.BlockSpec(memory_space=pltpu.VMEM)
    middle = pl.pallas_call(
        main_kernel,
        out_shape=[
            jax.ShapeDtypeStruct((3, order, L), F32),
            jax.ShapeDtypeStruct((order, order), F32),
            jax.ShapeDtypeStruct((order, S), F32),
            jax.ShapeDtypeStruct((S, S), F32),
            jax.ShapeDtypeStruct((S, L), F32),
        ],
        in_specs=[pl.BlockSpec(memory_space=pl.ANY)] * 2,
        out_specs=[vmem] * 5,
        scratch_shapes=[
            pltpu.VMEM((NW, 3, L), F32),
            pltpu.VMEM((NN, 3, L), F32),
            pltpu.VMEM((NW, *block), F32),
            pltpu.VMEM((NW, *block), F32),
            pltpu.VMEM((NW, *block), F32),
            pltpu.VMEM((NN, *block), F32),
            pltpu.VMEM((NN, *block), F32),
            pltpu.VMEM((NN, *block), F32),
            pltpu.VMEM((NN, *block), F32),
            pltpu.VMEM((NN, *block), F32),
            pltpu.VMEM((NN, *block), F32),
            pltpu.VMEM((4, NN, NW * L, L), BF16),
            pltpu.VMEM((4, NN, NW * L, L), BF16),
            pltpu.VMEM((2, 4, L, NW * L // 2), BF16),
            pltpu.VMEM((L, NN * L), F32),
            pltpu.VMEM((64, NN * L), F32),
            pltpu.VMEM((3, L, L), F32),
            pltpu.VMEM((NN, S, L), F32),
            pltpu.VMEM((NW, S, L), F32),
            pltpu.VMEM((NN, S, L), F32),
            pltpu.VMEM((NW, S, L), F32),
            pltpu.VMEM((NN, S, L), F32),
            pltpu.VMEM((NW, S, L), F32),
            pltpu.SemaphoreType.DMA((4, NW)),
            pltpu.SemaphoreType.DMA((4, NW)),
            pltpu.SemaphoreType.DMA((3, NW)),
            pltpu.SemaphoreType.DMA((3, NW)),
            pltpu.SemaphoreType.DMA((7, NN)),
            pltpu.SemaphoreType.DMA((7, NN)),
            pltpu.SemaphoreType.DMA((2,)),
        ],
        compiler_params=pltpu.CompilerParams(
            collective_id=0, has_side_effects=True, vmem_limit_bytes=56 * 1024 * 1024
        ),
        name="lanczos",
    )(positions, noise)
    return pl.pallas_call(
        last_kernel,
        out_shape=jax.ShapeDtypeStruct(block, F32),
        in_specs=[vmem] * 5,
        out_specs=vmem,
        scratch_shapes=[pltpu.VMEM((order, order), F32), pltpu.VMEM((order, order), F32)],
        name="finish",
    )(*middle)


def solution(mesh):
    axes = ("wide", "narrow")
    return jax.shard_map(
        per_device,
        mesh=mesh,
        in_specs=(P(None, axes), P(None, None, axes)),
        out_specs=P(None, None, axes),
        check_vma=False,
    )
```

```python
import functools

import jax
import jax.numpy as jnp
from jax import lax
from jax.experimental import pallas as pl
from jax.experimental.pallas import tpu as pltpu
from jax.sharding import PartitionSpec as P

ROOT_STEPS = 30
NW = 16
NN = 8
S = 16
L = 128
CENTRE = 34.0
MESH = pl.DeviceIdType.MESH
HI = lax.Precision.HIGHEST
F32 = jnp.float32
BF16 = jnp.bfloat16


def mm(a, b):
    return lax.dot_general(a, b, (((1,), (0,)), ((), ())), precision=HI, preferred_element_type=F32)


def mt(a, b):
    return lax.dot_general(a, b, (((1,), (1,)), ((), ())), precision=HI, preferred_element_type=F32)


def eye(n):
    return (lax.broadcasted_iota(jnp.int32, (n, n), 0) == lax.broadcasted_iota(jnp.int32, (n, n), 1)).astype(F32)


def transposed(a):
    return mt(eye(a.shape[1]), a)


def cholesky_pair(gram):
    n = gram.shape[0]
    rows = lax.broadcasted_iota(jnp.int32, (n, n), 0)
    cols = lax.broadcasted_iota(jnp.int32, (n, n), 1)
    left, right = gram, eye(n)
    upper, inverse = jnp.zeros((n, n), F32), jnp.zeros((n, n), F32)
    for c in range(n):
        scale = lax.rsqrt(jnp.broadcast_to(left[c : c + 1, c : c + 1], (1, n)))
        row = left[c : c + 1, :] * scale
        other = right[c : c + 1, :] * scale
        upper = jnp.where((rows == c) & (cols >= c), jnp.broadcast_to(row, (n, n)), upper)
        inverse = jnp.where((rows == c) & (cols <= c), jnp.broadcast_to(other, (n, n)), inverse)
        if c + 1 < n:
            factor = jnp.broadcast_to(left[:, c : c + 1], (n, n)) * scale
            left = left - factor * row
            right = right - jnp.where(rows > c, factor * other, 0.0)
    return upper, inverse


def split(value):
    high = value.astype(BF16)
    low = (value - high.astype(F32)).astype(BF16)
    return high, low


def hops(offset):
    return sum(min(part, 4 - part) for part in offset)


OFFSETS = sorted([(a, b) for a in range(4) for b in range(4)], key=hops)
ROWS = [(2, 0), (2, 1), (1, 0), (1, 1), (3, 0), (3, 1), (0, 1), (0, 0)]
OWN = NN - 1


def main_kernel(
    pos_hbm,
    noise_hbm,
    vec_ref,
    tri_ref,
    mix_ref,
    low_ref,
    ztot_ref,
    cpos,
    rpos,
    xg0,
    xg1,
    xg2,
    xr,
    pb1,
    pb2,
    rb1,
    rb2,
    pz,
    lhi,
    llo,
    rmat,
    acc,
    xjb,
    ga1,
    gb1,
    ga2,
    gb2,
    za,
    zb,
    send_b,
    recv_b,
    send_w,
    recv_w,
    send_n,
    recv_n,
    send_q,
    recv_q,
    load_sem,
):
    w = lax.axis_index("wide")
    n = lax.axis_index("narrow")

    def loop(begin, end, body):
        def step(i, carry):
            body(i)
            return carry

        lax.fori_loop(begin, end, step, 0)

    def block_copy(phase, buffer, p):
        a, b = OFFSETS[p]
        x = lax.rem(w // 4 + 4 - a, 4)
        z = lax.rem(lax.rem(w, 4) + 4 - b, 4)
        return pltpu.make_async_remote_copy(
            src_ref=buffer.at[0],
            dst_ref=buffer.at[p],
            send_sem=send_b.at[phase, p],
            recv_sem=recv_b.at[phase, p],
            device_id={"wide": x * 4 + z},
            device_id_type=MESH,
        )

    def block_send(phase, buffer):
        for p in range(1, NW):
            block_copy(phase, buffer, p).start()

    def block_arrived(phase, buffer, p):
        pltpu.make_async_remote_copy(
            src_ref=buffer.at[0],
            dst_ref=buffer.at[p],
            send_sem=send_b.at[phase, p],
            recv_sem=recv_b.at[phase, p],
            device_id={"wide": w},
            device_id_type=MESH,
        ).wait_recv()

    def wide_copy(phase, src, dst, target, slot):
        return pltpu.make_async_remote_copy(
            src_ref=src,
            dst_ref=dst.at[slot],
            send_sem=send_w.at[phase, target],
            recv_sem=recv_w.at[phase, slot],
            device_id={"wide": target},
            device_id_type=MESH,
        )

    def narrow_copy(phase, src, dst, target, slot):
        return pltpu.make_async_remote_copy(
            src_ref=src,
            dst_ref=dst.at[slot],
            send_sem=send_n.at[phase, target],
            recv_sem=recv_n.at[phase, slot],
            device_id={"narrow": target},
            device_id_type=MESH,
        )

    def row_copy(phase, src, dst, q, away):
        a, b = ROWS[q]
        y = lax.rem(n // 2 + (a if away else 4 - a), 4)
        core = lax.rem(lax.rem(n, 2) + b, 2)
        return pltpu.make_async_remote_copy(
            src_ref=src,
            dst_ref=dst.at[q],
            send_sem=send_q.at[phase, q],
            recv_sem=recv_q.at[phase, q],
            device_id={"narrow": y * 2 + core},
            device_id_type=MESH,
        )

    def wide_send(phase, dst):
        loop(1, NW, lambda p: wide_copy(phase, dst.at[w], dst, lax.rem(w + p, NW), w).start())

    def wide_recv(phase, dst):
        def one(p):
            s = lax.rem(w + p, NW)
            wide_copy(phase, dst.at[s], dst, s, s).wait_recv()

        loop(1, NW, one)

    def wide_sent(phase, dst):
        def one(p):
            s = lax.rem(w + p, NW)
            wide_copy(phase, dst.at[w], dst, s, w).wait_send()

        loop(1, NW, one)

    def narrow_send(phase, dst):
        loop(1, NN, lambda p: narrow_copy(phase, dst.at[n], dst, lax.rem(n + p, NN), n).start())

    def narrow_recv(phase, dst):
        def one(p):
            s = lax.rem(n + p, NN)
            narrow_copy(phase, dst.at[s], dst, s, s).wait_recv()

        loop(1, NN, one)

    def narrow_sent(phase, dst):
        def one(p):
            s = lax.rem(n + p, NN)
            narrow_copy(phase, dst.at[n], dst, s, n).wait_send()

        loop(1, NN, one)

    def all_of(buffer, count):
        parts = [buffer[i] for i in range(count)]
        while len(parts) > 1:
            parts = [parts[i] + parts[i + 1] for i in range(0, len(parts), 2)]
        return parts[0]

    barrier = pltpu.get_barrier_semaphore()

    def greet_wide(p):
        pl.semaphore_signal(barrier, inc=1, device_id={"wide": lax.rem(w + p, NW)}, device_id_type=MESH)

    def greet_narrow(p):
        pl.semaphore_signal(barrier, inc=1, device_id={"narrow": lax.rem(n + p, NN)}, device_id_type=MESH)

    loop(1, NW, greet_wide)
    loop(1, NN, greet_narrow)
    loads = [
        pltpu.make_async_copy(pos_hbm, cpos.at[0], load_sem.at[0]),
        pltpu.make_async_copy(noise_hbm, xg0.at[0], load_sem.at[1]),
    ]
    for load in loads:
        load.start()
    za[n] = jnp.zeros((S, L), F32)
    for load in loads:
        load.wait()
    rpos[OWN] = cpos[0]
    pl.semaphore_wait(barrier, NW + NN - 2)

    for q in range(OWN):
        row_copy(0, cpos.at[0], rpos, q, False).start()
    block_send(0, cpos)
    block_send(1, xg0)
    for q in range(OWN):
        row_copy(0, cpos.at[0], rpos, q, False).wait_recv()

    def build(jb):
        columns = jnp.concatenate([cpos[jb], jnp.zeros((5, L), F32)], axis=0).T
        for c in range(3):
            xjb[c] = jnp.broadcast_to(columns[:, c : c + 1], (L, L))

        def rows_of(ic):
            for half in range(2):
                ib = ic * 2 + half
                xi = [jnp.broadcast_to(rpos[ib, c : c + 1, :], (16, L)) for c in range(3)]
                for jt in range(8):
                    d = [xi[c] - xjb[c, jt * 16 : jt * 16 + 16, :] for c in range(3)]
                    sq = jnp.maximum(d[0] * d[0] + d[1] * d[1] + d[2] * d[2], 1e-20)
                    inv = lax.rsqrt(sq)
                    inv2 = inv * inv
                    near = sq < 4.0
                    iso = jnp.where(near, 1.0 - 0.28125 * (sq * inv), inv * (0.75 + 0.5 * inv2))
                    outer = inv * jnp.where(near, 0.09375, inv2 * (0.75 - 1.5 * inv2))
                    places = pl.ds(pl.multiple_of(jb * L + jt * 16, 16), 16)
                    for k, value in enumerate([outer * d[0], outer * d[1], outer * d[2], iso]):
                        high, low = split(value)
                        lhi[k, ib, places, :] = high
                        llo[k, ib, places, :] = low

        loop(0, NN // 2, rows_of)

    build(0)

    def arrived_build(p):
        block_arrived(0, cpos, p)
        build(p)

    loop(1, NW, arrived_build)

    half_blocks = NW // 2
    depth = half_blocks * L

    def product(phase, xg, out, between, emit):
        def expand(p):
            lanes = pl.ds(pl.multiple_of(lax.rem(p, half_blocks) * L, L), L)
            half = p // half_blocks
            x = [cpos[p, c : c + 1, :] - CENTRE for c in range(3)]
            v = [xg[p, e] for e in range(3)]
            pieces = [jnp.concatenate([v[e], x[0] * v[e], x[1] * v[e], x[2] * v[e]], axis=0) for e in range(3)]
            pieces.append(jnp.concatenate([jnp.zeros((S, L), F32), -v[0], -v[1], -v[2]], axis=0))
            for k in range(4):
                high, low = split(pieces[k])
                rmat[half, k, 0:64, lanes] = high
                rmat[half, k, 64:128, lanes] = low

        def arrived_expand(p):
            block_arrived(phase, xg, p)
            expand(p)

        def pair_of(half, q):
            rows = slice(half * depth, (half + 1) * depth)
            total, small = None, None
            for k in range(4):
                high = jnp.concatenate([lhi[k, q, rows, :], lhi[k, q + 1, rows, :]], axis=1)
                low = jnp.concatenate([llo[k, q, rows, :], llo[k, q + 1, rows, :]], axis=1)
                one = jnp.dot(rmat[half, k], high, preferred_element_type=F32)
                two = jnp.dot(rmat[half, k, 0:64, :], low, preferred_element_type=F32)
                total = one if total is None else total + one
                small = two if small is None else small + two
            return total[0:64] + (total[64:128] + small)

        expand(0)
        loop(1, half_blocks, arrived_expand)

        def first(g):
            value = pair_of(0, g * 2)
            acc[g * 2] = value[:, 0:L]
            acc[g * 2 + 1] = value[:, L : 2 * L]

        loop(0, NN // 2, first)
        between()
        loop(half_blocks, NW, arrived_expand)
        for g in range(NN // 2):
            value = pair_of(1, g * 2)
            for side in range(2):
                q = g * 2 + side
                total = acc[q] + value[:, side * L : side * L + L]
                for c in range(3):
                    out[q, c] = (rpos[q, c : c + 1, :] - CENTRE) * total[0:16] - total[16 + 16 * c : 32 + 16 * c]
                emit(q)

    def nothing(*_):
        return None

    def scatter(phase, parts, sums):
        def emit(q):
            if q != OWN:
                row_copy(phase, parts.at[q], sums, q, True).start()

        return emit

    def summed(phase, parts, sums):
        for q in range(OWN):
            row_copy(phase, parts.at[q], sums, q, True).wait_recv()
        return ((sums[0] + sums[1]) + (sums[2] + sums[3])) + ((sums[4] + sums[5]) + (sums[6] + parts[OWN]))

    lane = lax.broadcasted_iota(jnp.int32, (S, L), 1)

    product(1, xg0, pb1, nothing, scatter(1, pb1, rb1))
    xg1[0] = summed(1, pb1, rb1)
    block_send(2, xg1)

    part = jnp.zeros((2 * S, L), F32)
    for c in range(3):
        a, b = xg0[0, c], xg1[0, c]
        part = part + mt(jnp.concatenate([a, b], axis=0), jnp.concatenate([a, b, b, b, b, b, b, b], axis=0))
    ga1[n] = jnp.where(lane < 32, part[0:16], part[16:32])
    narrow_send(0, ga1)

    def forward1():
        narrow_recv(0, ga1)
        gb1[w] = all_of(ga1, NN)
        wide_send(0, gb1)

    product(2, xg1, pb2, forward1, scatter(2, pb2, rb2))

    wide_recv(0, gb1)
    total = all_of(gb1, NW)
    g00, g01, g11 = total[:, 0:16], total[:, 16:32], total[:, 32:48]
    upper0, inv0 = cholesky_pair(g00)

    def inside(g):
        return mt(mm(inv0, g), inv0)

    h1, c11, k1 = inside(g01), inside(g00), inside(g11)
    f1 = h1 + (h1 - mm(c11, h1))
    f1t = transposed(f1)
    fh = mm(f1t, h1)
    gram = k1 - fh - transposed(fh) + mm(f1t, mm(c11, f1))
    upper1, inv1 = cholesky_pair(gram)
    p21t = mm(inv1, inv0)
    p20t = -mm(mm(inv1, f1t), inv0)
    for c in range(3):
        a, y0 = xg0[0, c], xg1[0, c]
        vec_ref[c, 0:16] = mm(inv0, a)
        vec_ref[c, 16:32] = mm(p20t, a) + mm(p21t, y0)
        vec_ref[c, 32:48] = mm(p20t, y0)

    y1 = summed(2, pb2, rb2)
    xg2[0] = y1
    block_send(3, xg2)
    xr[OWN] = y1
    for q in range(OWN):
        row_copy(3, xr.at[OWN], xr, q, False).start()

    part = jnp.zeros((5 * S, L), F32)
    for c in range(3):
        y0, y1c = xg1[0, c], xg2[0, c]
        q1, q2 = vec_ref[c, 0:16], vec_ref[c, 16:32]
        wv = vec_ref[c, 32:48] + mm(p21t, y1c)
        vec_ref[c, 32:48] = wv
        part = part + mt(
            jnp.concatenate([q1, q2, wv, y0, y1c], axis=0), jnp.concatenate([q1, q2, wv, q2, wv, wv, y1c, y1c], axis=0)
        )
    packed = jnp.where(lane < 48, part[0:16], part[16:32])
    packed = jnp.where(lane < 80, packed, part[32:48])
    packed = jnp.where(lane < 96, packed, part[48:64])
    ga2[n] = jnp.where(lane < 112, packed, part[64:80])
    narrow_send(1, ga2)

    def forward2():
        narrow_recv(1, ga2)
        gb2[w] = all_of(ga2, NN)
        wide_send(1, gb2)

    product(3, xg2, pz, forward2, nothing)
    for q in range(OWN):
        row_copy(3, xr.at[OWN], xr, q, False).wait_recv()
    part = jnp.zeros((S, S), F32)
    for c in range(3):
        part = part + mt(
            jnp.concatenate([xr[b, c] for b in range(NN)], axis=1), jnp.concatenate([pz[b, c] for b in range(NN)], axis=1)
        )
    za[n, :, 0:16] = part
    narrow_send(2, za)

    wide_recv(1, gb2)
    total = all_of(gb2, NW)
    c11, c12, ha, c22, hb, k, g12, g22 = [total[:, 16 * i : 16 * i + 16] for i in range(8)]
    p20, p21 = transposed(p20t), transposed(p21t)
    c12t = transposed(c12)
    fa = ha + (ha - mm(c11, ha) - mm(c12, hb))
    fb = hb + (hb - mm(c12t, ha) - mm(c22, hb))
    fat, fbt = transposed(fa), transposed(fb)
    hat, hbt = transposed(ha), transposed(hb)
    fh = mm(fat, ha) + mm(fbt, hb)
    cf = mm(fat, mm(c11, fa) + mm(c12, fb)) + mm(fbt, mm(c12t, fa) + mm(c22, fb))
    upper2, inv2 = cholesky_pair(k - fh - transposed(fh) + cf)
    narrow_recv(2, za)
    zb[w] = all_of(za, NN)
    wide_send(2, zb)
    zz = mm(p20t, mm(g12, p20) + mm(g22, p21)) + mm(p21t, mm(g22, p20))
    wmq1 = mm(hat, f1) + mm(hbt, upper1)
    side = mm(wmq1, fa) + mm(k, fb)
    inner = zz - side - transposed(side) + mm(fat, mm(h1, fa) + mm(ha, fb)) + mm(fbt, mm(hat, fa) + mm(hb, fb))
    a3 = mt(mm(inv2, inner), inv2)

    def sym(value):
        return 0.5 * (value + transposed(value))

    order = 3 * S
    tri = jnp.zeros((order, order), F32)
    low = [
        (lax.broadcasted_iota(jnp.int32, (order, S), 0) == lax.broadcasted_iota(jnp.int32, (order, S), 1) + S * i).astype(F32)
        for i in range(3)
    ]
    blocks = [(0, 0, sym(h1)), (1, 1, sym(hb)), (2, 2, sym(a3)), (1, 0, upper1), (2, 1, upper2)]
    blocks += [(0, 1, transposed(upper1)), (1, 2, transposed(upper2))]
    for i, j, block in blocks:
        tri = tri + mt(mm(low[i], block), low[j])
    tri_ref[...] = tri
    mix_ref[...] = mm(low[2], mm(inv2, p21t))
    low_ref[...] = transposed(upper0)
    for c in range(3):
        q1, q2, wv = vec_ref[c, 0:16], vec_ref[c, 16:32], vec_ref[c, 32:48]
        vec_ref[c, 32:48] = mm(inv2, wv - mm(fat, q1) - mm(fbt, q2))
    wide_recv(2, zb)
    ztot_ref[...] = all_of(zb, NW)

    for phase, buffer in enumerate([cpos, xg0, xg1, xg2]):
        for p in range(1, NW):
            block_copy(phase, buffer, p).wait_send()
    for phase, buffer in enumerate([gb1, gb2, zb]):
        wide_sent(phase, buffer)
    for phase, buffer in enumerate([ga1, ga2, za]):
        narrow_sent(phase, buffer)
    for q in range(OWN):
        row_copy(0, cpos.at[0], rpos, q, False).wait_send()
        row_copy(1, pb1.at[q], rb1, q, True).wait_send()
        row_copy(2, pb2.at[q], rb2, q, True).wait_send()
        row_copy(3, xr.at[OWN], xr, q, False).wait_send()


def last_kernel(vec_ref, tri_ref, mix_ref, low_ref, ztot_ref, out_ref, y_ref, z_ref):
    zraw = ztot_ref[:, 0:16]
    mix = mix_ref[...]
    tri = tri_ref[...] + mt(mm(mix, 0.5 * (zraw + transposed(zraw))), mix)
    order = 3 * S
    scale = jnp.sqrt(jnp.sum(tri * tri))
    ident = eye(order)
    y_ref[...] = tri / scale
    z_ref[...] = ident

    def more(carry):
        step, gap = carry
        return jnp.logical_and(step < ROOT_STEPS, jnp.logical_not(gap < 1e-8))

    def newton(carry):
        step, _ = carry
        y, z = y_ref[...], z_ref[...]
        zy = mm(z, y)
        factor = 1.5 * ident - 0.5 * zy
        y_ref[...] = mm(y, factor)
        z_ref[...] = mm(factor, z)
        off = zy - ident
        return step + 1, jnp.sum(off * off)

    lax.while_loop(more, newton, (jnp.int32(0), jnp.float32(1.0)))
    root = y_ref[...] * jnp.sqrt(scale)
    first = (
        lax.broadcasted_iota(jnp.int32, (S, order), 0) == lax.broadcasted_iota(jnp.int32, (S, order), 1)
    ).astype(F32)
    mixing = mm(low_ref[...], mt(first, root))
    for c in range(3):
        out_ref[c] = mm(mixing, vec_ref[c])


def per_device(positions, noise):
    block = (3, S, L)
    order = 3 * S
    vmem = pl.BlockSpec(memory_space=pltpu.VMEM)
    middle = pl.pallas_call(
        main_kernel,
        out_shape=[
            jax.ShapeDtypeStruct((3, order, L), F32),
            jax.ShapeDtypeStruct((order, order), F32),
            jax.ShapeDtypeStruct((order, S), F32),
            jax.ShapeDtypeStruct((S, S), F32),
            jax.ShapeDtypeStruct((S, L), F32),
        ],
        in_specs=[pl.BlockSpec(memory_space=pl.ANY)] * 2,
        out_specs=[vmem] * 5,
        scratch_shapes=[
            pltpu.VMEM((NW, 3, L), F32),
            pltpu.VMEM((NN, 3, L), F32),
            pltpu.VMEM((NW, *block), F32),
            pltpu.VMEM((NW, *block), F32),
            pltpu.VMEM((NW, *block), F32),
            pltpu.VMEM((NN, *block), F32),
            pltpu.VMEM((NN, *block), F32),
            pltpu.VMEM((NN, *block), F32),
            pltpu.VMEM((NN, *block), F32),
            pltpu.VMEM((NN, *block), F32),
            pltpu.VMEM((NN, *block), F32),
            pltpu.VMEM((4, NN, NW * L, L), BF16),
            pltpu.VMEM((4, NN, NW * L, L), BF16),
            pltpu.VMEM((2, 4, L, NW * L // 2), BF16),
            pltpu.VMEM((NN, 64, L), F32),
            pltpu.VMEM((3, L, L), F32),
            pltpu.VMEM((NN, S, L), F32),
            pltpu.VMEM((NW, S, L), F32),
            pltpu.VMEM((NN, S, L), F32),
            pltpu.VMEM((NW, S, L), F32),
            pltpu.VMEM((NN, S, L), F32),
            pltpu.VMEM((NW, S, L), F32),
            pltpu.SemaphoreType.DMA((4, NW)),
            pltpu.SemaphoreType.DMA((4, NW)),
            pltpu.SemaphoreType.DMA((3, NW)),
            pltpu.SemaphoreType.DMA((3, NW)),
            pltpu.SemaphoreType.DMA((3, NN)),
            pltpu.SemaphoreType.DMA((3, NN)),
            pltpu.SemaphoreType.DMA((4, NN)),
            pltpu.SemaphoreType.DMA((4, NN)),
            pltpu.SemaphoreType.DMA((2,)),
        ],
        compiler_params=pltpu.CompilerParams(
            collective_id=0, has_side_effects=True, vmem_limit_bytes=56 * 1024 * 1024
        ),
        name="lanczos",
    )(positions, noise)
    return pl.pallas_call(
        last_kernel,
        out_shape=jax.ShapeDtypeStruct(block, F32),
        in_specs=[vmem] * 5,
        out_specs=vmem,
        scratch_shapes=[pltpu.VMEM((order, order), F32), pltpu.VMEM((order, order), F32)],
        name="finish",
    )(*middle)


def solution(mesh):
    axes = ("wide", "narrow")
    return jax.shard_map(
        per_device,
        mesh=mesh,
        in_specs=(P(None, axes), P(None, None, axes)),
        out_specs=P(None, None, axes),
        check_vma=False,
    )
```

```python
import functools

import jax
import jax.numpy as jnp
from jax import lax
from jax.experimental import pallas as pl
from jax.experimental.pallas import tpu as pltpu
from jax.sharding import PartitionSpec as P

ROOT_STEPS = 30
NW = 16
NN = 8
S = 16
L = 128
CENTRE = 34.0
MESH = pl.DeviceIdType.MESH
HI = lax.Precision.HIGHEST
F32 = jnp.float32
BF16 = jnp.bfloat16


def mm(a, b):
    return lax.dot_general(a, b, (((1,), (0,)), ((), ())), precision=HI, preferred_element_type=F32)


def mt(a, b):
    return lax.dot_general(a, b, (((1,), (1,)), ((), ())), precision=HI, preferred_element_type=F32)


def eye(n):
    return (lax.broadcasted_iota(jnp.int32, (n, n), 0) == lax.broadcasted_iota(jnp.int32, (n, n), 1)).astype(F32)


def transposed(a):
    return mt(eye(a.shape[1]), a)


def cholesky_pair(gram):
    n = gram.shape[0]
    rows = lax.broadcasted_iota(jnp.int32, (n, n), 0)
    cols = lax.broadcasted_iota(jnp.int32, (n, n), 1)
    left, right = gram, eye(n)
    upper, inverse = jnp.zeros((n, n), F32), jnp.zeros((n, n), F32)
    for c in range(n):
        scale = lax.rsqrt(jnp.broadcast_to(left[c : c + 1, c : c + 1], (1, n)))
        row = left[c : c + 1, :] * scale
        other = right[c : c + 1, :] * scale
        upper = jnp.where((rows == c) & (cols >= c), jnp.broadcast_to(row, (n, n)), upper)
        inverse = jnp.where((rows == c) & (cols <= c), jnp.broadcast_to(other, (n, n)), inverse)
        if c + 1 < n:
            factor = jnp.broadcast_to(left[:, c : c + 1], (n, n)) * scale
            left = left - factor * row
            right = right - jnp.where(rows > c, factor * other, 0.0)
    return upper, inverse


def split(value):
    high = value.astype(BF16)
    low = (value - high.astype(F32)).astype(BF16)
    return high, low


def hops(offset):
    return sum(min(part, 4 - part) for part in offset)


OFFSETS = sorted([(a, b) for a in range(4) for b in range(4)], key=hops)
OWN = NN - 1


def row_place(q):
    g, side = q // 2, q % 2
    return (2 + g * (g + 1) // 2) % 4, (side + g // 3) % 2


def main_kernel(
    pos_hbm,
    noise_hbm,
    vec_ref,
    tri_ref,
    mix_ref,
    low_ref,
    ztot_ref,
    cpos,
    rpos,
    xg0,
    xg1,
    xg2,
    xr,
    pb1,
    pb2,
    rb1,
    rb2,
    pz,
    lhi,
    llo,
    rmat,
    acc,
    xjb,
    ga1,
    gb1,
    ga2,
    gb2,
    za,
    zb,
    send_b,
    recv_b,
    send_w,
    recv_w,
    send_n,
    recv_n,
    send_q,
    recv_q,
    load_sem,
):
    w = lax.axis_index("wide")
    n = lax.axis_index("narrow")

    def loop(begin, end, body):
        def step(i, carry):
            body(i)
            return carry

        lax.fori_loop(begin, end, step, 0)

    def block_copy(phase, buffer, p):
        a, b = OFFSETS[p]
        x = lax.rem(w // 4 + 4 - a, 4)
        z = lax.rem(lax.rem(w, 4) + 4 - b, 4)
        return pltpu.make_async_remote_copy(
            src_ref=buffer.at[0],
            dst_ref=buffer.at[p],
            send_sem=send_b.at[phase, p],
            recv_sem=recv_b.at[phase, p],
            device_id={"wide": x * 4 + z},
            device_id_type=MESH,
        )

    def block_send(phase, buffer):
        for p in range(1, NW):
            block_copy(phase, buffer, p).start()

    def block_arrived(phase, buffer, p):
        pltpu.make_async_remote_copy(
            src_ref=buffer.at[0],
            dst_ref=buffer.at[p],
            send_sem=send_b.at[phase, p],
            recv_sem=recv_b.at[phase, p],
            device_id={"wide": w},
            device_id_type=MESH,
        ).wait_recv()

    def wide_copy(phase, src, dst, target, slot):
        return pltpu.make_async_remote_copy(
            src_ref=src,
            dst_ref=dst.at[slot],
            send_sem=send_w.at[phase, target],
            recv_sem=recv_w.at[phase, slot],
            device_id={"wide": target},
            device_id_type=MESH,
        )

    def narrow_copy(phase, src, dst, target, slot):
        return pltpu.make_async_remote_copy(
            src_ref=src,
            dst_ref=dst.at[slot],
            send_sem=send_n.at[phase, target],
            recv_sem=recv_n.at[phase, slot],
            device_id={"narrow": target},
            device_id_type=MESH,
        )

    def row_copy(phase, src, dst, q, away):
        a, b = row_place(q)
        y = lax.rem(n // 2 + (a if away else 4 - a), 4)
        core = lax.rem(lax.rem(n, 2) + b, 2)
        return pltpu.make_async_remote_copy(
            src_ref=src,
            dst_ref=dst.at[q],
            send_sem=send_q.at[phase, q],
            recv_sem=recv_q.at[phase, q],
            device_id={"narrow": y * 2 + core},
            device_id_type=MESH,
        )

    def wide_send(phase, dst):
        loop(1, NW, lambda p: wide_copy(phase, dst.at[w], dst, lax.rem(w + p, NW), w).start())

    def wide_recv(phase, dst):
        def one(p):
            s = lax.rem(w + p, NW)
            wide_copy(phase, dst.at[s], dst, s, s).wait_recv()

        loop(1, NW, one)

    def wide_sent(phase, dst):
        def one(p):
            s = lax.rem(w + p, NW)
            wide_copy(phase, dst.at[w], dst, s, w).wait_send()

        loop(1, NW, one)

    def narrow_send(phase, dst):
        loop(1, NN, lambda p: narrow_copy(phase, dst.at[n], dst, lax.rem(n + p, NN), n).start())

    def narrow_recv(phase, dst):
        def one(p):
            s = lax.rem(n + p, NN)
            narrow_copy(phase, dst.at[s], dst, s, s).wait_recv()

        loop(1, NN, one)

    def narrow_sent(phase, dst):
        def one(p):
            s = lax.rem(n + p, NN)
            narrow_copy(phase, dst.at[n], dst, s, n).wait_send()

        loop(1, NN, one)

    def all_of(buffer, count):
        parts = [buffer[i] for i in range(count)]
        while len(parts) > 1:
            parts = [parts[i] + parts[i + 1] for i in range(0, len(parts), 2)]
        return parts[0]

    barrier = pltpu.get_barrier_semaphore()

    def greet_wide(p):
        pl.semaphore_signal(barrier, inc=1, device_id={"wide": lax.rem(w + p, NW)}, device_id_type=MESH)

    def greet_narrow(p):
        pl.semaphore_signal(barrier, inc=1, device_id={"narrow": lax.rem(n + p, NN)}, device_id_type=MESH)

    loop(1, NW, greet_wide)
    loop(1, NN, greet_narrow)
    loads = [
        pltpu.make_async_copy(pos_hbm, cpos.at[0], load_sem.at[0]),
        pltpu.make_async_copy(noise_hbm, xg0.at[0], load_sem.at[1]),
    ]
    for load in loads:
        load.start()
    za[n] = jnp.zeros((S, L), F32)
    for load in loads:
        load.wait()
    rpos[OWN] = cpos[0]
    pl.semaphore_wait(barrier, NW + NN - 2)

    for q in range(OWN):
        row_copy(0, cpos.at[0], rpos, q, False).start()
    block_send(0, cpos)
    block_send(1, xg0)
    for q in range(OWN):
        row_copy(0, cpos.at[0], rpos, q, False).wait_recv()

    def build(group):
        for i in range(4):
            columns = jnp.concatenate([cpos[group * 4 + i], jnp.zeros((5, L), F32)], axis=0).T
            for c in range(3):
                xjb[i, c] = jnp.broadcast_to(columns[:, c : c + 1], (L, L))

        def one(step):
            i = step // 4
            for half in range(2):
                ib = lax.rem(step, 4) * 2 + half
                xi = [jnp.broadcast_to(rpos[ib, c : c + 1, :], (16, L)) for c in range(3)]
                for jt in range(8):
                    d = [xi[c] - xjb[i, c, jt * 16 : jt * 16 + 16, :] for c in range(3)]
                    sq = jnp.maximum(d[0] * d[0] + d[1] * d[1] + d[2] * d[2], 1e-20)
                    inv = lax.rsqrt(sq)
                    inv2 = inv * inv
                    near = sq < 4.0
                    iso = jnp.where(near, 1.0 - 0.28125 * (sq * inv), inv * (0.75 + 0.5 * inv2))
                    outer = inv * jnp.where(near, 0.09375, inv2 * (0.75 - 1.5 * inv2))
                    places = pl.ds(pl.multiple_of((group * 4 + i) * L + jt * 16, 16), 16)
                    for k, value in enumerate([outer * d[0], outer * d[1], outer * d[2], iso]):
                        high, low = split(value)
                        lhi[k, ib, places, :] = high
                        llo[k, ib, places, :] = low

        loop(0, 16, one)

    def arrived_build(group):
        def arrived(p):
            block_arrived(0, cpos, p)

        loop(jnp.maximum(group * 4, 1), group * 4 + 4, arrived)
        build(group)

    loop(0, 4, arrived_build)

    half_blocks = NW // 2
    depth = half_blocks * L

    def product(phase, xg, out, early, between, emit):
        def expand(p):
            lanes = pl.ds(pl.multiple_of(lax.rem(p, half_blocks) * L, L), L)
            half = p // half_blocks
            x = [cpos[p, c : c + 1, :] - CENTRE for c in range(3)]
            v = [xg[p, e] for e in range(3)]
            pieces = [jnp.concatenate([v[e], x[0] * v[e], x[1] * v[e], x[2] * v[e]], axis=0) for e in range(3)]
            pieces.append(jnp.concatenate([jnp.zeros((S, L), F32), -v[0], -v[1], -v[2]], axis=0))
            for k in range(4):
                high, low = split(pieces[k])
                rmat[half, k, 0:64, lanes] = high
                rmat[half, k, 64:128, lanes] = low

        def arrived_expand(p):
            block_arrived(phase, xg, p)
            expand(p)

        def pair_of(half, q):
            rows = slice(half * depth, (half + 1) * depth)
            total, small = None, None
            for k in range(4):
                high = jnp.concatenate([lhi[k, q, rows, :], lhi[k, q + 1, rows, :]], axis=1)
                low = jnp.concatenate([llo[k, q, rows, :], llo[k, q + 1, rows, :]], axis=1)
                one = jnp.dot(rmat[half, k], high, preferred_element_type=F32)
                two = jnp.dot(rmat[half, k, 0:64, :], low, preferred_element_type=F32)
                total = one if total is None else total + one
                small = two if small is None else small + two
            return total[0:64] + (total[64:128] + small)

        expand(0)
        loop(1, half_blocks, arrived_expand)

        def first(g):
            value = pair_of(0, g * 2)
            acc[g * 2] = value[:, 0:L]
            acc[g * 2 + 1] = value[:, L : 2 * L]

        loop(0, NN // 4, first)
        early()
        loop(NN // 4, NN // 2, first)
        between()
        loop(half_blocks, NW, arrived_expand)

        def second(g):
            value = pair_of(1, g * 2)
            for side in range(2):
                q = g * 2 + side
                total = acc[q] + value[:, side * L : side * L + L]
                for c in range(3):
                    out[q, c] = (rpos[q, pl.ds(c, 1), :] - CENTRE) * total[0:16] - total[16 + 16 * c : 32 + 16 * c]
            emit(g * 2)

        loop(0, NN // 2, second)

    def nothing(*_):
        return None

    def scatter(phase, parts, sums):
        def emit(q):
            row_copy(phase, parts.at[q], sums, q, True).start()

            @pl.when(q + 1 < OWN)
            def _():
                row_copy(phase, parts.at[q + 1], sums, q + 1, True).start()

        return emit

    def summed(phase, parts, sums):
        for q in range(OWN):
            row_copy(phase, parts.at[q], sums, q, True).wait_recv()
        return ((sums[0] + sums[1]) + (sums[2] + sums[3])) + ((sums[4] + sums[5]) + (sums[6] + parts[OWN]))

    lane = lax.broadcasted_iota(jnp.int32, (S, L), 1)

    product(1, xg0, pb1, nothing, nothing, scatter(1, pb1, rb1))
    xg1[0] = summed(1, pb1, rb1)
    block_send(2, xg1)

    part = jnp.zeros((2 * S, L), F32)
    for c in range(3):
        a, b = xg0[0, c], xg1[0, c]
        part = part + mt(jnp.concatenate([a, b], axis=0), jnp.concatenate([a, b, b, b, b, b, b, b], axis=0))
    ga1[n] = jnp.where(lane < 32, part[0:16], part[16:32])
    narrow_send(0, ga1)

    def forward1():
        narrow_recv(0, ga1)
        gb1[w] = all_of(ga1, NN)
        wide_send(0, gb1)

    product(2, xg1, pb2, forward1, nothing, scatter(2, pb2, rb2))

    wide_recv(0, gb1)
    total = all_of(gb1, NW)
    g00, g01, g11 = total[:, 0:16], total[:, 16:32], total[:, 32:48]
    upper0, inv0 = cholesky_pair(g00)

    def inside(g):
        return mt(mm(inv0, g), inv0)

    h1, c11, k1 = inside(g01), inside(g00), inside(g11)
    f1 = h1 + (h1 - mm(c11, h1))
    f1t = transposed(f1)
    fh = mm(f1t, h1)
    gram = k1 - fh - transposed(fh) + mm(f1t, mm(c11, f1))
    y1 = summed(2, pb2, rb2)
    xg2[0] = y1
    block_send(3, xg2)
    xr[OWN] = y1
    for q in range(OWN):
        row_copy(3, xr.at[OWN], xr, q, False).start()

    upper1, inv1 = cholesky_pair(gram)
    p21t = mm(inv1, inv0)
    p20t = -mm(mm(inv1, f1t), inv0)
    for c in range(3):
        a, y0 = xg0[0, c], xg1[0, c]
        vec_ref[c, 0:16] = mm(inv0, a)
        vec_ref[c, 16:32] = mm(p20t, a) + mm(p21t, y0)
        vec_ref[c, 32:48] = mm(p20t, y0)

    part = jnp.zeros((5 * S, L), F32)
    for c in range(3):
        y0, y1c = xg1[0, c], xg2[0, c]
        q1, q2 = vec_ref[c, 0:16], vec_ref[c, 16:32]
        wv = vec_ref[c, 32:48] + mm(p21t, y1c)
        vec_ref[c, 32:48] = wv
        part = part + mt(
            jnp.concatenate([q1, q2, wv, y0, y1c], axis=0), jnp.concatenate([q1, q2, wv, q2, wv, wv, y1c, y1c], axis=0)
        )
    packed = jnp.where(lane < 48, part[0:16], part[16:32])
    packed = jnp.where(lane < 80, packed, part[32:48])
    packed = jnp.where(lane < 96, packed, part[48:64])
    ga2[n] = jnp.where(lane < 112, packed, part[64:80])
    narrow_send(1, ga2)

    def forward2():
        narrow_recv(1, ga2)
        gb2[w] = all_of(ga2, NN)
        wide_send(1, gb2)

    product(3, xg2, pz, nothing, forward2, nothing)
    for q in range(OWN):
        row_copy(3, xr.at[OWN], xr, q, False).wait_recv()
    part = jnp.zeros((S, S), F32)
    for c in range(3):
        part = part + mt(
            jnp.concatenate([xr[b, c] for b in range(NN)], axis=1), jnp.concatenate([pz[b, c] for b in range(NN)], axis=1)
        )
    za[n, :, 0:16] = part
    narrow_send(2, za)

    wide_recv(1, gb2)
    total = all_of(gb2, NW)
    c11, c12, ha, c22, hb, k, g12, g22 = [total[:, 16 * i : 16 * i + 16] for i in range(8)]
    p20, p21 = transposed(p20t), transposed(p21t)
    c12t = transposed(c12)
    fa = ha + (ha - mm(c11, ha) - mm(c12, hb))
    fb = hb + (hb - mm(c12t, ha) - mm(c22, hb))
    fat, fbt = transposed(fa), transposed(fb)
    hat, hbt = transposed(ha), transposed(hb)
    fh = mm(fat, ha) + mm(fbt, hb)
    cf = mm(fat, mm(c11, fa) + mm(c12, fb)) + mm(fbt, mm(c12t, fa) + mm(c22, fb))
    upper2, inv2 = cholesky_pair(k - fh - transposed(fh) + cf)
    narrow_recv(2, za)
    zb[w] = all_of(za, NN)
    wide_send(2, zb)
    zz = mm(p20t, mm(g12, p20) + mm(g22, p21)) + mm(p21t, mm(g22, p20))
    wmq1 = mm(hat, f1) + mm(hbt, upper1)
    side = mm(wmq1, fa) + mm(k, fb)
    inner = zz - side - transposed(side) + mm(fat, mm(h1, fa) + mm(ha, fb)) + mm(fbt, mm(hat, fa) + mm(hb, fb))
    a3 = mt(mm(inv2, inner), inv2)

    def sym(value):
        return 0.5 * (value + transposed(value))

    order = 3 * S
    tri = jnp.zeros((order, order), F32)
    low = [
        (lax.broadcasted_iota(jnp.int32, (order, S), 0) == lax.broadcasted_iota(jnp.int32, (order, S), 1) + S * i).astype(F32)
        for i in range(3)
    ]
    blocks = [(0, 0, sym(h1)), (1, 1, sym(hb)), (2, 2, sym(a3)), (1, 0, upper1), (2, 1, upper2)]
    blocks += [(0, 1, transposed(upper1)), (1, 2, transposed(upper2))]
    for i, j, block in blocks:
        tri = tri + mt(mm(low[i], block), low[j])
    tri_ref[...] = tri
    mix_ref[...] = mm(low[2], mm(inv2, p21t))
    low_ref[...] = transposed(upper0)
    for c in range(3):
        q1, q2, wv = vec_ref[c, 0:16], vec_ref[c, 16:32], vec_ref[c, 32:48]
        vec_ref[c, 32:48] = mm(inv2, wv - mm(fat, q1) - mm(fbt, q2))
    wide_recv(2, zb)
    ztot_ref[...] = all_of(zb, NW)

    for phase, buffer in enumerate([cpos, xg0, xg1, xg2]):
        for p in range(1, NW):
            block_copy(phase, buffer, p).wait_send()
    for phase, buffer in enumerate([gb1, gb2, zb]):
        wide_sent(phase, buffer)
    for phase, buffer in enumerate([ga1, ga2, za]):
        narrow_sent(phase, buffer)
    for q in range(OWN):
        row_copy(0, cpos.at[0], rpos, q, False).wait_send()
        row_copy(1, pb1.at[q], rb1, q, True).wait_send()
        row_copy(2, pb2.at[q], rb2, q, True).wait_send()
        row_copy(3, xr.at[OWN], xr, q, False).wait_send()


def last_kernel(vec_ref, tri_ref, mix_ref, low_ref, ztot_ref, out_ref, y_ref, z_ref):
    zraw = ztot_ref[:, 0:16]
    mix = mix_ref[...]
    tri = tri_ref[...] + mt(mm(mix, 0.5 * (zraw + transposed(zraw))), mix)
    order = 3 * S
    scale = jnp.sqrt(jnp.sum(tri * tri))
    ident = eye(order)
    y_ref[...] = tri / scale
    z_ref[...] = ident

    def more(carry):
        step, gap = carry
        return jnp.logical_and(step < ROOT_STEPS, jnp.logical_not(gap < 1e-8))

    def newton(carry):
        step, _ = carry
        y, z = y_ref[...], z_ref[...]
        zy = mm(z, y)
        factor = 1.5 * ident - 0.5 * zy
        y_ref[...] = mm(y, factor)
        z_ref[...] = mm(factor, z)
        off = zy - ident
        return step + 1, jnp.sum(off * off)

    lax.while_loop(more, newton, (jnp.int32(0), jnp.float32(1.0)))
    root = y_ref[...] * jnp.sqrt(scale)
    first = (
        lax.broadcasted_iota(jnp.int32, (S, order), 0) == lax.broadcasted_iota(jnp.int32, (S, order), 1)
    ).astype(F32)
    mixing = mm(low_ref[...], mt(first, root))
    for c in range(3):
        out_ref[c] = mm(mixing, vec_ref[c])


def per_device(positions, noise):
    block = (3, S, L)
    order = 3 * S
    vmem = pl.BlockSpec(memory_space=pltpu.VMEM)
    middle = pl.pallas_call(
        main_kernel,
        out_shape=[
            jax.ShapeDtypeStruct((3, order, L), F32),
            jax.ShapeDtypeStruct((order, order), F32),
            jax.ShapeDtypeStruct((order, S), F32),
            jax.ShapeDtypeStruct((S, S), F32),
            jax.ShapeDtypeStruct((S, L), F32),
        ],
        in_specs=[pl.BlockSpec(memory_space=pl.ANY)] * 2,
        out_specs=[vmem] * 5,
        scratch_shapes=[
            pltpu.VMEM((NW, 3, L), F32),
            pltpu.VMEM((NN, 3, L), F32),
            pltpu.VMEM((NW, *block), F32),
            pltpu.VMEM((NW, *block), F32),
            pltpu.VMEM((NW, *block), F32),
            pltpu.VMEM((NN, *block), F32),
            pltpu.VMEM((NN, *block), F32),
            pltpu.VMEM((NN, *block), F32),
            pltpu.VMEM((NN, *block), F32),
            pltpu.VMEM((NN, *block), F32),
            pltpu.VMEM((NN, *block), F32),
            pltpu.VMEM((4, NN, NW * L, L), BF16),
            pltpu.VMEM((4, NN, NW * L, L), BF16),
            pltpu.VMEM((2, 4, L, NW * L // 2), BF16),
            pltpu.VMEM((NN, 64, L), F32),
            pltpu.VMEM((4, 3, L, L), F32),
            pltpu.VMEM((NN, S, L), F32),
            pltpu.VMEM((NW, S, L), F32),
            pltpu.VMEM((NN, S, L), F32),
            pltpu.VMEM((NW, S, L), F32),
            pltpu.VMEM((NN, S, L), F32),
            pltpu.VMEM((NW, S, L), F32),
            pltpu.SemaphoreType.DMA((4, NW)),
            pltpu.SemaphoreType.DMA((4, NW)),
            pltpu.SemaphoreType.DMA((3, NW)),
            pltpu.SemaphoreType.DMA((3, NW)),
            pltpu.SemaphoreType.DMA((3, NN)),
            pltpu.SemaphoreType.DMA((3, NN)),
            pltpu.SemaphoreType.DMA((4, NN)),
            pltpu.SemaphoreType.DMA((4, NN)),
            pltpu.SemaphoreType.DMA((2,)),
        ],
        compiler_params=pltpu.CompilerParams(
            collective_id=0, has_side_effects=True, vmem_limit_bytes=56 * 1024 * 1024
        ),
        name="lanczos",
    )(positions, noise)
    return pl.pallas_call(
        last_kernel,
        out_shape=jax.ShapeDtypeStruct(block, F32),
        in_specs=[vmem] * 5,
        out_specs=vmem,
        scratch_shapes=[pltpu.VMEM((order, order), F32), pltpu.VMEM((order, order), F32)],
        name="finish",
    )(*middle)


def solution(mesh):
    axes = ("wide", "narrow")
    return jax.shard_map(
        per_device,
        mesh=mesh,
        in_specs=(P(None, axes), P(None, None, axes)),
        out_specs=P(None, None, axes),
        check_vma=False,
    )
```

```python
import functools

import jax
import jax.numpy as jnp
from jax import lax
from jax.experimental import pallas as pl
from jax.experimental.pallas import tpu as pltpu
from jax.sharding import PartitionSpec as P

ROOT_STEPS = 30
NW = 16
NN = 8
S = 16
L = 128
CENTRE = 34.0
MESH = pl.DeviceIdType.MESH
HI = lax.Precision.HIGHEST
F32 = jnp.float32
BF16 = jnp.bfloat16


def mm(a, b):
    return lax.dot_general(a, b, (((1,), (0,)), ((), ())), precision=HI, preferred_element_type=F32)


def mt(a, b):
    return lax.dot_general(a, b, (((1,), (1,)), ((), ())), precision=HI, preferred_element_type=F32)


def eye(n):
    return (lax.broadcasted_iota(jnp.int32, (n, n), 0) == lax.broadcasted_iota(jnp.int32, (n, n), 1)).astype(F32)


def transposed(a):
    return mt(eye(a.shape[1]), a)


def cholesky_pair(gram):
    n = gram.shape[0]
    rows = lax.broadcasted_iota(jnp.int32, (n, n), 0)
    cols = lax.broadcasted_iota(jnp.int32, (n, n), 1)
    left, right = gram, eye(n)
    upper, inverse = jnp.zeros((n, n), F32), jnp.zeros((n, n), F32)
    for c in range(n):
        scale = lax.rsqrt(jnp.broadcast_to(left[c : c + 1, c : c + 1], (1, n)))
        row = left[c : c + 1, :] * scale
        other = right[c : c + 1, :] * scale
        upper = jnp.where((rows == c) & (cols >= c), jnp.broadcast_to(row, (n, n)), upper)
        inverse = jnp.where((rows == c) & (cols <= c), jnp.broadcast_to(other, (n, n)), inverse)
        if c + 1 < n:
            factor = jnp.broadcast_to(left[:, c : c + 1], (n, n)) * scale
            left = left - factor * row
            right = right - jnp.where(rows > c, factor * other, 0.0)
    return upper, inverse


def split(value):
    high = value.astype(BF16)
    low = (value - high.astype(F32)).astype(BF16)
    return high, low


def hops(offset):
    return sum(min(part, 4 - part) for part in offset)


OFFSETS = sorted([(a, b) for a in range(4) for b in range(4)], key=hops)
OWN = NN - 1


def row_place(q):
    g, side = q // 2, q % 2
    return (2 + g * (g + 1) // 2) % 4, (side + g // 3) % 2


def main_kernel(
    pos_hbm,
    noise_hbm,
    vec_ref,
    tri_ref,
    mix_ref,
    low_ref,
    ztot_ref,
    cpos,
    rpos,
    xg0,
    xg1,
    xg2,
    xr,
    pb1,
    pb2,
    rb1,
    rb2,
    pz,
    lhi,
    llo,
    rmat,
    acc,
    xjb,
    ga1,
    gb1,
    ga2,
    gb2,
    za,
    zb,
    send_b,
    recv_b,
    send_w,
    recv_w,
    send_n,
    recv_n,
    send_q,
    recv_q,
    load_sem,
):
    w = lax.axis_index("wide")
    n = lax.axis_index("narrow")

    def loop(begin, end, body):
        def step(i, carry):
            body(i)
            return carry

        lax.fori_loop(begin, end, step, 0)

    def block_copy(phase, buffer, p):
        a, b = OFFSETS[p]
        x = lax.rem(w // 4 + 4 - a, 4)
        z = lax.rem(lax.rem(w, 4) + 4 - b, 4)
        return pltpu.make_async_remote_copy(
            src_ref=buffer.at[0],
            dst_ref=buffer.at[p],
            send_sem=send_b.at[phase, p],
            recv_sem=recv_b.at[phase, p],
            device_id={"wide": x * 4 + z},
            device_id_type=MESH,
        )

    def block_send(phase, buffer):
        for p in range(1, NW):
            block_copy(phase, buffer, p).start()

    def block_arrived(phase, buffer, p):
        pltpu.make_async_remote_copy(
            src_ref=buffer.at[0],
            dst_ref=buffer.at[p],
            send_sem=send_b.at[phase, p],
            recv_sem=recv_b.at[phase, p],
            device_id={"wide": w},
            device_id_type=MESH,
        ).wait_recv()

    def wide_copy(phase, src, dst, target, slot):
        return pltpu.make_async_remote_copy(
            src_ref=src,
            dst_ref=dst.at[slot],
            send_sem=send_w.at[phase, target],
            recv_sem=recv_w.at[phase, slot],
            device_id={"wide": target},
            device_id_type=MESH,
        )

    def narrow_copy(phase, src, dst, target, slot):
        return pltpu.make_async_remote_copy(
            src_ref=src,
            dst_ref=dst.at[slot],
            send_sem=send_n.at[phase, target],
            recv_sem=recv_n.at[phase, slot],
            device_id={"narrow": target},
            device_id_type=MESH,
        )

    def row_copy(phase, src, dst, q, away):
        a, b = row_place(q)
        y = lax.rem(n // 2 + (a if away else 4 - a), 4)
        core = lax.rem(lax.rem(n, 2) + b, 2)
        return pltpu.make_async_remote_copy(
            src_ref=src,
            dst_ref=dst.at[q],
            send_sem=send_q.at[phase, q],
            recv_sem=recv_q.at[phase, q],
            device_id={"narrow": y * 2 + core},
            device_id_type=MESH,
        )

    def wide_send(phase, dst):
        loop(1, NW, lambda p: wide_copy(phase, dst.at[w], dst, lax.rem(w + p, NW), w).start())

    def wide_recv(phase, dst):
        def one(p):
            s = lax.rem(w + p, NW)
            wide_copy(phase, dst.at[s], dst, s, s).wait_recv()

        loop(1, NW, one)

    def wide_sent(phase, dst):
        def one(p):
            s = lax.rem(w + p, NW)
            wide_copy(phase, dst.at[w], dst, s, w).wait_send()

        loop(1, NW, one)

    def narrow_send(phase, dst):
        loop(1, NN, lambda p: narrow_copy(phase, dst.at[n], dst, lax.rem(n + p, NN), n).start())

    def narrow_recv(phase, dst):
        def one(p):
            s = lax.rem(n + p, NN)
            narrow_copy(phase, dst.at[s], dst, s, s).wait_recv()

        loop(1, NN, one)

    def narrow_sent(phase, dst):
        def one(p):
            s = lax.rem(n + p, NN)
            narrow_copy(phase, dst.at[n], dst, s, n).wait_send()

        loop(1, NN, one)

    def all_of(buffer, count):
        parts = [buffer[i] for i in range(count)]
        while len(parts) > 1:
            parts = [parts[i] + parts[i + 1] for i in range(0, len(parts), 2)]
        return parts[0]

    barrier = pltpu.get_barrier_semaphore()

    def greet_wide(p):
        along_x = lax.rem(w // 4 + p, 4) * 4 + lax.rem(w, 4)
        along_z = w // 4 * 4 + lax.rem(lax.rem(w, 4) + p, 4)
        pl.semaphore_signal(barrier, inc=1, device_id={"wide": along_x}, device_id_type=MESH)
        pl.semaphore_signal(barrier, inc=1, device_id={"wide": along_z}, device_id_type=MESH)

    def greet_narrow(p):
        pl.semaphore_signal(barrier, inc=1, device_id={"narrow": lax.rem(n + p, NN)}, device_id_type=MESH)

    loop(1, 4, greet_wide)
    loop(1, NN, greet_narrow)
    loads = [
        pltpu.make_async_copy(pos_hbm, cpos.at[0], load_sem.at[0]),
        pltpu.make_async_copy(noise_hbm, xg0.at[0], load_sem.at[1]),
    ]
    for load in loads:
        load.start()
    za[n] = jnp.zeros((S, L), F32)
    for load in loads:
        load.wait()
    rpos[OWN] = cpos[0]
    pl.semaphore_wait(barrier, 6 + NN - 1)

    for q in range(OWN):
        row_copy(0, cpos.at[0], rpos, q, False).start()
    for a in range(1, 4):
        block_copy(0, cpos, OFFSETS.index((a, 0))).start()
        block_copy(0, cpos, OFFSETS.index((0, a))).start()
    for a in range(1, 4):
        held = OFFSETS.index((a, 0))
        block_arrived(0, cpos, held)
        for b in range(1, 4):
            slot = OFFSETS.index((a, b))
            pltpu.make_async_remote_copy(
                src_ref=cpos.at[held],
                dst_ref=cpos.at[slot],
                send_sem=send_b.at[0, slot],
                recv_sem=recv_b.at[0, slot],
                device_id={"wide": w // 4 * 4 + lax.rem(lax.rem(w, 4) + 4 - b, 4)},
                device_id_type=MESH,
            ).start()
    for a in range(1, 4):
        block_arrived(0, cpos, OFFSETS.index((0, a)))
    for q in range(OWN):
        row_copy(0, cpos.at[0], rpos, q, False).wait_recv()

    def build(group):
        for i in range(4):
            columns = jnp.concatenate([cpos[group * 4 + i], jnp.zeros((5, L), F32)], axis=0).T
            for c in range(3):
                xjb[i, c] = jnp.broadcast_to(columns[:, c : c + 1], (L, L))

        def one(step):
            i = step // 4
            for half in range(2):
                ib = lax.rem(step, 4) * 2 + half
                xi = [jnp.broadcast_to(rpos[ib, c : c + 1, :], (16, L)) for c in range(3)]
                for jt in range(8):
                    d = [xi[c] - xjb[i, c, jt * 16 : jt * 16 + 16, :] for c in range(3)]
                    sq = jnp.maximum(d[0] * d[0] + d[1] * d[1] + d[2] * d[2], 1e-20)
                    inv = lax.rsqrt(sq)
                    inv2 = inv * inv
                    near = sq < 4.0
                    iso = jnp.where(near, 1.0 - 0.28125 * (sq * inv), inv * (0.75 + 0.5 * inv2))
                    outer = inv * jnp.where(near, 0.09375, inv2 * (0.75 - 1.5 * inv2))
                    places = pl.ds(pl.multiple_of((group * 4 + i) * L + jt * 16, 16), 16)
                    for k, value in enumerate([outer * d[0], outer * d[1], outer * d[2], iso]):
                        high, low = split(value)
                        lhi[k, ib, places, :] = high
                        llo[k, ib, places, :] = low

        loop(0, 16, one)

    build(0)
    for a in range(1, 4):
        for b in range(1, 4):
            block_arrived(0, cpos, OFFSETS.index((a, b)))
    block_send(1, xg0)
    loop(1, 4, build)

    half_blocks = NW // 2
    depth = half_blocks * L

    def product(phase, xg, out, early, between, emit):
        def expand(p):
            lanes = pl.ds(pl.multiple_of(lax.rem(p, half_blocks) * L, L), L)
            half = p // half_blocks
            x = [cpos[p, c : c + 1, :] - CENTRE for c in range(3)]
            v = [xg[p, e] for e in range(3)]
            pieces = [jnp.concatenate([v[e], x[0] * v[e], x[1] * v[e], x[2] * v[e]], axis=0) for e in range(3)]
            pieces.append(jnp.concatenate([jnp.zeros((S, L), F32), -v[0], -v[1], -v[2]], axis=0))
            for k in range(4):
                high, low = split(pieces[k])
                rmat[half, k, 0:64, lanes] = high
                rmat[half, k, 64:128, lanes] = low

        def arrived_expand(p):
            block_arrived(phase, xg, p)
            expand(p)

        def pair_of(half, q):
            rows = slice(half * depth, (half + 1) * depth)
            total, small = None, None
            for k in range(4):
                high = jnp.concatenate([lhi[k, q, rows, :], lhi[k, q + 1, rows, :]], axis=1)
                low = jnp.concatenate([llo[k, q, rows, :], llo[k, q + 1, rows, :]], axis=1)
                one = jnp.dot(rmat[half, k], high, preferred_element_type=F32)
                two = jnp.dot(rmat[half, k, 0:64, :], low, preferred_element_type=F32)
                total = one if total is None else total + one
                small = two if small is None else small + two
            return total[0:64] + (total[64:128] + small)

        expand(0)
        loop(1, half_blocks, arrived_expand)

        def first(g):
            value = pair_of(0, g * 2)
            acc[g * 2] = value[:, 0:L]
            acc[g * 2 + 1] = value[:, L : 2 * L]

        loop(0, NN // 4, first)
        early()
        loop(NN // 4, NN // 2, first)
        between()
        loop(half_blocks, NW, arrived_expand)

        def second(g):
            value = pair_of(1, g * 2)
            for side in range(2):
                q = g * 2 + side
                total = acc[q] + value[:, side * L : side * L + L]
                for c in range(3):
                    out[q, c] = (rpos[q, pl.ds(c, 1), :] - CENTRE) * total[0:16] - total[16 + 16 * c : 32 + 16 * c]
            emit(g * 2)

        loop(0, NN // 2, second)

    def nothing(*_):
        return None

    def scatter(phase, parts, sums):
        def emit(q):
            row_copy(phase, parts.at[q], sums, q, True).start()

            @pl.when(q + 1 < OWN)
            def _():
                row_copy(phase, parts.at[q + 1], sums, q + 1, True).start()

        return emit

    def summed(phase, parts, sums):
        for q in range(OWN):
            row_copy(phase, parts.at[q], sums, q, True).wait_recv()
        return ((sums[0] + sums[1]) + (sums[2] + sums[3])) + ((sums[4] + sums[5]) + (sums[6] + parts[OWN]))

    lane = lax.broadcasted_iota(jnp.int32, (S, L), 1)

    product(1, xg0, pb1, nothing, nothing, scatter(1, pb1, rb1))
    xg1[0] = summed(1, pb1, rb1)
    block_send(2, xg1)

    part = jnp.zeros((2 * S, L), F32)
    for c in range(3):
        a, b = xg0[0, c], xg1[0, c]
        part = part + mt(jnp.concatenate([a, b], axis=0), jnp.concatenate([a, b, b, b, b, b, b, b], axis=0))
    ga1[n] = jnp.where(lane < 32, part[0:16], part[16:32])
    narrow_send(0, ga1)

    def forward1():
        narrow_recv(0, ga1)
        gb1[w] = all_of(ga1, NN)
        wide_send(0, gb1)

    product(2, xg1, pb2, forward1, nothing, scatter(2, pb2, rb2))

    wide_recv(0, gb1)
    total = all_of(gb1, NW)
    g00, g01, g11 = total[:, 0:16], total[:, 16:32], total[:, 32:48]
    upper0, inv0 = cholesky_pair(g00)

    def inside(g):
        return mt(mm(inv0, g), inv0)

    h1, c11, k1 = inside(g01), inside(g00), inside(g11)
    f1 = h1 + (h1 - mm(c11, h1))
    f1t = transposed(f1)
    fh = mm(f1t, h1)
    gram = k1 - fh - transposed(fh) + mm(f1t, mm(c11, f1))
    y1 = summed(2, pb2, rb2)
    xg2[0] = y1
    block_send(3, xg2)
    xr[OWN] = y1
    for q in range(OWN):
        row_copy(3, xr.at[OWN], xr, q, False).start()

    upper1, inv1 = cholesky_pair(gram)
    p21t = mm(inv1, inv0)
    p20t = -mm(mm(inv1, f1t), inv0)
    for c in range(3):
        a, y0 = xg0[0, c], xg1[0, c]
        vec_ref[c, 0:16] = mm(inv0, a)
        vec_ref[c, 16:32] = mm(p20t, a) + mm(p21t, y0)
        vec_ref[c, 32:48] = mm(p20t, y0)

    part = jnp.zeros((5 * S, L), F32)
    for c in range(3):
        y0, y1c = xg1[0, c], xg2[0, c]
        q1, q2 = vec_ref[c, 0:16], vec_ref[c, 16:32]
        wv = vec_ref[c, 32:48] + mm(p21t, y1c)
        vec_ref[c, 32:48] = wv
        part = part + mt(
            jnp.concatenate([q1, q2, wv, y0, y1c], axis=0), jnp.concatenate([q1, q2, wv, q2, wv, wv, y1c, y1c], axis=0)
        )
    packed = jnp.where(lane < 48, part[0:16], part[16:32])
    packed = jnp.where(lane < 80, packed, part[32:48])
    packed = jnp.where(lane < 96, packed, part[48:64])
    ga2[n] = jnp.where(lane < 112, packed, part[64:80])
    narrow_send(1, ga2)

    def forward2():
        narrow_recv(1, ga2)
        gb2[w] = all_of(ga2, NN)
        wide_send(1, gb2)

    product(3, xg2, pz, nothing, forward2, nothing)
    for q in range(OWN):
        row_copy(3, xr.at[OWN], xr, q, False).wait_recv()
    part = jnp.zeros((S, S), F32)
    for c in range(3):
        part = part + mt(
            jnp.concatenate([xr[b, c] for b in range(NN)], axis=1), jnp.concatenate([pz[b, c] for b in range(NN)], axis=1)
        )
    za[n, :, 0:16] = part
    narrow_send(2, za)

    wide_recv(1, gb2)
    total = all_of(gb2, NW)
    c11, c12, ha, c22, hb, k, g12, g22 = [total[:, 16 * i : 16 * i + 16] for i in range(8)]
    p20, p21 = transposed(p20t), transposed(p21t)
    c12t = transposed(c12)
    fa = ha + (ha - mm(c11, ha) - mm(c12, hb))
    fb = hb + (hb - mm(c12t, ha) - mm(c22, hb))
    fat, fbt = transposed(fa), transposed(fb)
    hat, hbt = transposed(ha), transposed(hb)
    fh = mm(fat, ha) + mm(fbt, hb)
    cf = mm(fat, mm(c11, fa) + mm(c12, fb)) + mm(fbt, mm(c12t, fa) + mm(c22, fb))
    upper2, inv2 = cholesky_pair(k - fh - transposed(fh) + cf)
    narrow_recv(2, za)
    zb[w] = all_of(za, NN)
    wide_send(2, zb)
    zz = mm(p20t, mm(g12, p20) + mm(g22, p21)) + mm(p21t, mm(g22, p20))
    wmq1 = mm(hat, f1) + mm(hbt, upper1)
    side = mm(wmq1, fa) + mm(k, fb)
    inner = zz - side - transposed(side) + mm(fat, mm(h1, fa) + mm(ha, fb)) + mm(fbt, mm(hat, fa) + mm(hb, fb))
    a3 = mt(mm(inv2, inner), inv2)

    def sym(value):
        return 0.5 * (value + transposed(value))

    order = 3 * S
    tri = jnp.zeros((order, order), F32)
    low = [
        (lax.broadcasted_iota(jnp.int32, (order, S), 0) == lax.broadcasted_iota(jnp.int32, (order, S), 1) + S * i).astype(F32)
        for i in range(3)
    ]
    blocks = [(0, 0, sym(h1)), (1, 1, sym(hb)), (2, 2, sym(a3)), (1, 0, upper1), (2, 1, upper2)]
    blocks += [(0, 1, transposed(upper1)), (1, 2, transposed(upper2))]
    for i, j, block in blocks:
        tri = tri + mt(mm(low[i], block), low[j])
    tri_ref[...] = tri
    mix_ref[...] = mm(low[2], mm(inv2, p21t))
    low_ref[...] = transposed(upper0)
    for c in range(3):
        q1, q2, wv = vec_ref[c, 0:16], vec_ref[c, 16:32], vec_ref[c, 32:48]
        vec_ref[c, 32:48] = mm(inv2, wv - mm(fat, q1) - mm(fbt, q2))
    wide_recv(2, zb)
    ztot_ref[...] = all_of(zb, NW)

    for phase, buffer in enumerate([cpos, xg0, xg1, xg2]):
        for p in range(1, NW):
            block_copy(phase, buffer, p).wait_send()
    for phase, buffer in enumerate([gb1, gb2, zb]):
        wide_sent(phase, buffer)
    for phase, buffer in enumerate([ga1, ga2, za]):
        narrow_sent(phase, buffer)
    for q in range(OWN):
        row_copy(0, cpos.at[0], rpos, q, False).wait_send()
        row_copy(1, pb1.at[q], rb1, q, True).wait_send()
        row_copy(2, pb2.at[q], rb2, q, True).wait_send()
        row_copy(3, xr.at[OWN], xr, q, False).wait_send()


def last_kernel(vec_ref, tri_ref, mix_ref, low_ref, ztot_ref, out_ref, y_ref, z_ref):
    zraw = ztot_ref[:, 0:16]
    mix = mix_ref[...]
    tri = tri_ref[...] + mt(mm(mix, 0.5 * (zraw + transposed(zraw))), mix)
    order = 3 * S
    scale = jnp.sqrt(jnp.sum(tri * tri))
    ident = eye(order)
    y_ref[...] = tri / scale
    z_ref[...] = ident

    def more(carry):
        step, gap = carry
        return jnp.logical_and(step < ROOT_STEPS, jnp.logical_not(gap < 1e-8))

    def newton(carry):
        step, _ = carry
        y, z = y_ref[...], z_ref[...]
        zy = mm(z, y)
        factor = 1.5 * ident - 0.5 * zy
        y_ref[...] = mm(y, factor)
        z_ref[...] = mm(factor, z)
        off = zy - ident
        return step + 1, jnp.sum(off * off)

    lax.while_loop(more, newton, (jnp.int32(0), jnp.float32(1.0)))
    root = y_ref[...] * jnp.sqrt(scale)
    first = (
        lax.broadcasted_iota(jnp.int32, (S, order), 0) == lax.broadcasted_iota(jnp.int32, (S, order), 1)
    ).astype(F32)
    mixing = mm(low_ref[...], mt(first, root))
    for c in range(3):
        out_ref[c] = mm(mixing, vec_ref[c])


def per_device(positions, noise):
    block = (3, S, L)
    order = 3 * S
    vmem = pl.BlockSpec(memory_space=pltpu.VMEM)
    middle = pl.pallas_call(
        main_kernel,
        out_shape=[
            jax.ShapeDtypeStruct((3, order, L), F32),
            jax.ShapeDtypeStruct((order, order), F32),
            jax.ShapeDtypeStruct((order, S), F32),
            jax.ShapeDtypeStruct((S, S), F32),
            jax.ShapeDtypeStruct((S, L), F32),
        ],
        in_specs=[pl.BlockSpec(memory_space=pl.ANY)] * 2,
        out_specs=[vmem] * 5,
        scratch_shapes=[
            pltpu.VMEM((NW, 3, L), F32),
            pltpu.VMEM((NN, 3, L), F32),
            pltpu.VMEM((NW, *block), F32),
            pltpu.VMEM((NW, *block), F32),
            pltpu.VMEM((NW, *block), F32),
            pltpu.VMEM((NN, *block), F32),
            pltpu.VMEM((NN, *block), F32),
            pltpu.VMEM((NN, *block), F32),
            pltpu.VMEM((NN, *block), F32),
            pltpu.VMEM((NN, *block), F32),
            pltpu.VMEM((NN, *block), F32),
            pltpu.VMEM((4, NN, NW * L, L), BF16),
            pltpu.VMEM((4, NN, NW * L, L), BF16),
            pltpu.VMEM((2, 4, L, NW * L // 2), BF16),
            pltpu.VMEM((NN, 64, L), F32),
            pltpu.VMEM((4, 3, L, L), F32),
            pltpu.VMEM((NN, S, L), F32),
            pltpu.VMEM((NW, S, L), F32),
            pltpu.VMEM((NN, S, L), F32),
            pltpu.VMEM((NW, S, L), F32),
            pltpu.VMEM((NN, S, L), F32),
            pltpu.VMEM((NW, S, L), F32),
            pltpu.SemaphoreType.DMA((4, NW)),
            pltpu.SemaphoreType.DMA((4, NW)),
            pltpu.SemaphoreType.DMA((3, NW)),
            pltpu.SemaphoreType.DMA((3, NW)),
            pltpu.SemaphoreType.DMA((3, NN)),
            pltpu.SemaphoreType.DMA((3, NN)),
            pltpu.SemaphoreType.DMA((4, NN)),
            pltpu.SemaphoreType.DMA((4, NN)),
            pltpu.SemaphoreType.DMA((2,)),
        ],
        compiler_params=pltpu.CompilerParams(
            collective_id=0, has_side_effects=True, vmem_limit_bytes=56 * 1024 * 1024
        ),
        name="lanczos",
    )(positions, noise)
    return pl.pallas_call(
        last_kernel,
        out_shape=jax.ShapeDtypeStruct(block, F32),
        in_specs=[vmem] * 5,
        out_specs=vmem,
        scratch_shapes=[pltpu.VMEM((order, order), F32), pltpu.VMEM((order, order), F32)],
        name="finish",
    )(*middle)


def solution(mesh):
    axes = ("wide", "narrow")
    return jax.shard_map(
        per_device,
        mesh=mesh,
        in_specs=(P(None, axes), P(None, None, axes)),
        out_specs=P(None, None, axes),
        check_vma=False,
    )
```

```python
import functools

import jax
import jax.numpy as jnp
from jax import lax
from jax.experimental import pallas as pl
from jax.experimental.pallas import tpu as pltpu
from jax.sharding import PartitionSpec as P

ROOT_STEPS = 30
NW = 16
NN = 8
S = 16
L = 128
CENTRE = 34.0
MESH = pl.DeviceIdType.MESH
HI = lax.Precision.HIGHEST
F32 = jnp.float32
BF16 = jnp.bfloat16


def mm(a, b):
    return lax.dot_general(a, b, (((1,), (0,)), ((), ())), precision=HI, preferred_element_type=F32)


def mt(a, b):
    return lax.dot_general(a, b, (((1,), (1,)), ((), ())), precision=HI, preferred_element_type=F32)


def eye(n):
    return (lax.broadcasted_iota(jnp.int32, (n, n), 0) == lax.broadcasted_iota(jnp.int32, (n, n), 1)).astype(F32)


def transposed(a):
    return mt(eye(a.shape[1]), a)


def cholesky_pair(gram):
    n = gram.shape[0]
    rows = lax.broadcasted_iota(jnp.int32, (n, n), 0)
    cols = lax.broadcasted_iota(jnp.int32, (n, n), 1)
    left, right = gram, eye(n)
    upper, inverse = jnp.zeros((n, n), F32), jnp.zeros((n, n), F32)
    for c in range(n):
        scale = lax.rsqrt(jnp.broadcast_to(left[c : c + 1, c : c + 1], (1, n)))
        row = left[c : c + 1, :] * scale
        other = right[c : c + 1, :] * scale
        upper = jnp.where((rows == c) & (cols >= c), jnp.broadcast_to(row, (n, n)), upper)
        inverse = jnp.where((rows == c) & (cols <= c), jnp.broadcast_to(other, (n, n)), inverse)
        if c + 1 < n:
            factor = jnp.broadcast_to(left[:, c : c + 1], (n, n)) * scale
            left = left - factor * row
            right = right - jnp.where(rows > c, factor * other, 0.0)
    return upper, inverse


def split(value):
    high = value.astype(BF16)
    low = (value - high.astype(F32)).astype(BF16)
    return high, low


OFFSETS = [(0, 0), (2, 0), (1, 0), (0, 1), (1, 1), (1, 3), (2, 1), (1, 2), (0, 2), (2, 2)]
OFFSETS += [(0, 3), (3, 0), (3, 1), (3, 3), (2, 3), (3, 2)]
HALF = 10
OWN = NN - 1


def row_place(q):
    g, side = q // 2, q % 2
    return (2 + g * (g + 1) // 2) % 4, (side + g // 3) % 2


def main_kernel(
    pos_hbm,
    noise_hbm,
    vec_ref,
    tri_ref,
    mix_ref,
    low_ref,
    ztot_ref,
    cpos,
    rpos,
    xg0,
    xg1,
    xg2,
    xr,
    pb1,
    pb2,
    rb1,
    rb2,
    pz,
    lhi,
    llo,
    rmat,
    acc,
    xjb,
    ga1,
    gb1,
    ga2,
    gb2,
    za,
    zb,
    send_b,
    recv_b,
    send_w,
    recv_w,
    send_n,
    recv_n,
    send_q,
    recv_q,
    load_sem,
):
    w = lax.axis_index("wide")
    n = lax.axis_index("narrow")

    def loop(begin, end, body):
        def step(i, carry):
            body(i)
            return carry

        lax.fori_loop(begin, end, step, 0)

    def block_copy(phase, buffer, p):
        a, b = OFFSETS[p]
        x = lax.rem(w // 4 + 4 - a, 4)
        z = lax.rem(lax.rem(w, 4) + 4 - b, 4)
        return pltpu.make_async_remote_copy(
            src_ref=buffer.at[0],
            dst_ref=buffer.at[p],
            send_sem=send_b.at[phase, p],
            recv_sem=recv_b.at[phase, p],
            device_id={"wide": x * 4 + z},
            device_id_type=MESH,
        )

    def block_send(phase, buffer, count=NW):
        for p in range(1, count):
            block_copy(phase, buffer, p).start()

    def block_arrived(phase, buffer, p):
        pltpu.make_async_remote_copy(
            src_ref=buffer.at[0],
            dst_ref=buffer.at[p],
            send_sem=send_b.at[phase, p],
            recv_sem=recv_b.at[phase, p],
            device_id={"wide": w},
            device_id_type=MESH,
        ).wait_recv()

    def wide_copy(phase, src, dst, target, slot):
        return pltpu.make_async_remote_copy(
            src_ref=src,
            dst_ref=dst.at[slot],
            send_sem=send_w.at[phase, target],
            recv_sem=recv_w.at[phase, slot],
            device_id={"wide": target},
            device_id_type=MESH,
        )

    def narrow_copy(phase, src, dst, target, slot):
        return pltpu.make_async_remote_copy(
            src_ref=src,
            dst_ref=dst.at[slot],
            send_sem=send_n.at[phase, target],
            recv_sem=recv_n.at[phase, slot],
            device_id={"narrow": target},
            device_id_type=MESH,
        )

    def row_copy(phase, src, dst, q, away):
        a, b = row_place(q)
        y = lax.rem(n // 2 + (a if away else 4 - a), 4)
        core = lax.rem(lax.rem(n, 2) + b, 2)
        return pltpu.make_async_remote_copy(
            src_ref=src,
            dst_ref=dst.at[q],
            send_sem=send_q.at[phase, q],
            recv_sem=recv_q.at[phase, q],
            device_id={"narrow": y * 2 + core},
            device_id_type=MESH,
        )

    def wide_send(phase, dst):
        loop(1, NW, lambda p: wide_copy(phase, dst.at[w], dst, lax.rem(w + p, NW), w).start())

    def wide_recv(phase, dst):
        def one(p):
            s = lax.rem(w + p, NW)
            wide_copy(phase, dst.at[s], dst, s, s).wait_recv()

        loop(1, NW, one)

    def wide_sent(phase, dst):
        def one(p):
            s = lax.rem(w + p, NW)
            wide_copy(phase, dst.at[w], dst, s, w).wait_send()

        loop(1, NW, one)

    def narrow_send(phase, dst):
        loop(1, NN, lambda p: narrow_copy(phase, dst.at[n], dst, lax.rem(n + p, NN), n).start())

    def narrow_recv(phase, dst):
        def one(p):
            s = lax.rem(n + p, NN)
            narrow_copy(phase, dst.at[s], dst, s, s).wait_recv()

        loop(1, NN, one)

    def narrow_sent(phase, dst):
        def one(p):
            s = lax.rem(n + p, NN)
            narrow_copy(phase, dst.at[n], dst, s, n).wait_send()

        loop(1, NN, one)

    def all_of(buffer, count):
        parts = [buffer[i] for i in range(count)]
        while len(parts) > 1:
            parts = [parts[i] + parts[i + 1] for i in range(0, len(parts), 2)]
        return parts[0]

    barrier = pltpu.get_barrier_semaphore()

    def greet_wide(p):
        along_x = lax.rem(w // 4 + p, 4) * 4 + lax.rem(w, 4)
        along_z = w // 4 * 4 + lax.rem(lax.rem(w, 4) + p, 4)
        pl.semaphore_signal(barrier, inc=1, device_id={"wide": along_x}, device_id_type=MESH)
        pl.semaphore_signal(barrier, inc=1, device_id={"wide": along_z}, device_id_type=MESH)

    def greet_narrow(p):
        pl.semaphore_signal(barrier, inc=1, device_id={"narrow": lax.rem(n + p, NN)}, device_id_type=MESH)

    loop(1, 4, greet_wide)
    loop(1, NN, greet_narrow)
    loads = [
        pltpu.make_async_copy(pos_hbm, cpos.at[0], load_sem.at[0]),
        pltpu.make_async_copy(noise_hbm, xg0.at[0], load_sem.at[1]),
    ]
    for load in loads:
        load.start()
    za[n] = jnp.zeros((S, L), F32)
    for load in loads:
        load.wait()
    rpos[OWN] = cpos[0]
    pl.semaphore_wait(barrier, 6 + NN - 1)

    for q in range(OWN):
        row_copy(0, cpos.at[0], rpos, q, False).start()
    for a in range(1, 4):
        block_copy(0, cpos, OFFSETS.index((a, 0))).start()
        block_copy(0, cpos, OFFSETS.index((0, a))).start()
    for a in range(1, 4):
        held = OFFSETS.index((a, 0))
        block_arrived(0, cpos, held)
        for b in range(1, 4):
            slot = OFFSETS.index((a, b))
            pltpu.make_async_remote_copy(
                src_ref=cpos.at[held],
                dst_ref=cpos.at[slot],
                send_sem=send_b.at[0, slot],
                recv_sem=recv_b.at[0, slot],
                device_id={"wide": w // 4 * 4 + lax.rem(lax.rem(w, 4) + 4 - b, 4)},
                device_id_type=MESH,
            ).start()
    for a in range(1, 4):
        block_arrived(0, cpos, OFFSETS.index((0, a)))
    for q in range(OWN):
        row_copy(0, cpos.at[0], rpos, q, False).wait_recv()

    def build(group):
        for i in range(4):
            columns = jnp.concatenate([cpos[group * 4 + i], jnp.zeros((5, L), F32)], axis=0).T
            for c in range(3):
                xjb[i, c] = jnp.broadcast_to(columns[:, c : c + 1], (L, L))

        def one(step):
            i = step // 4
            for half in range(2):
                ib = lax.rem(step, 4) * 2 + half
                xi = [jnp.broadcast_to(rpos[ib, c : c + 1, :], (16, L)) for c in range(3)]
                for jt in range(8):
                    d = [xi[c] - xjb[i, c, jt * 16 : jt * 16 + 16, :] for c in range(3)]
                    sq = jnp.maximum(d[0] * d[0] + d[1] * d[1] + d[2] * d[2], 1e-20)
                    inv = lax.rsqrt(sq)
                    inv2 = inv * inv
                    near = sq < 4.0
                    iso = jnp.where(near, 1.0 - 0.28125 * (sq * inv), inv * (0.75 + 0.5 * inv2))
                    outer = inv * jnp.where(near, 0.09375, inv2 * (0.75 - 1.5 * inv2))
                    places = pl.ds(pl.multiple_of((group * 4 + i) * L + jt * 16, 16), 16)
                    for k, value in enumerate([outer * d[0], outer * d[1], outer * d[2], iso]):
                        high, low = split(value)
                        lhi[k, ib, places, :] = high
                        llo[k, ib, places, :] = low

        loop(0, 16, one)

    build(0)
    for a in range(1, 4):
        for b in range(1, 4):
            block_arrived(0, cpos, OFFSETS.index((a, b)))
    block_send(1, xg0)
    loop(1, 4, build)

    half_blocks = NW // 2
    depth = half_blocks * L

    def product(phase, xg, out, early, between, emit, symmetric=False):
        def expand(p, factor=None):
            lanes = pl.ds(pl.multiple_of(lax.rem(p, half_blocks) * L, L), L)
            half = p // half_blocks
            x = [cpos[p, c : c + 1, :] - CENTRE for c in range(3)]
            v = [xg[p, e] if factor is None else factor * xg[p, e] for e in range(3)]
            pieces = [jnp.concatenate([v[e], x[0] * v[e], x[1] * v[e], x[2] * v[e]], axis=0) for e in range(3)]
            pieces.append(jnp.concatenate([jnp.zeros((S, L), F32), -v[0], -v[1], -v[2]], axis=0))
            for k in range(4):
                high, low = split(pieces[k])
                rmat[half, k, 0:64, lanes] = high
                rmat[half, k, 64:128, lanes] = low

        def arrived_expand(p):
            block_arrived(phase, xg, p)
            expand(p)

        def arrived_double(p):
            block_arrived(phase, xg, p)
            expand(p, 2.0)

        columns = HALF if symmetric else NW

        def pair_of(half, q):
            size = min(depth, columns * L - half * depth)
            rows = slice(half * depth, half * depth + size)
            total, small = None, None
            for k in range(4):
                high = jnp.concatenate([lhi[k, q, rows, :], lhi[k, q + 1, rows, :]], axis=1)
                low = jnp.concatenate([llo[k, q, rows, :], llo[k, q + 1, rows, :]], axis=1)
                one = jnp.dot(rmat[half, k, :, 0:size], high, preferred_element_type=F32)
                two = jnp.dot(rmat[half, k, 0:64, 0:size], low, preferred_element_type=F32)
                total = one if total is None else total + one
                small = two if small is None else small + two
            return total[0:64] + (total[64:128] + small)

        expand(0)
        loop(1, 2, arrived_expand)
        loop(2, half_blocks, arrived_double if symmetric else arrived_expand)

        def first(g):
            value = pair_of(0, g * 2)
            acc[g * 2] = value[:, 0:L]
            acc[g * 2 + 1] = value[:, L : 2 * L]

        loop(0, NN // 4, first)
        early()
        loop(NN // 4, NN // 2, first)
        between()
        loop(half_blocks, columns, arrived_expand)

        def second(g):
            value = pair_of(1, g * 2)
            for side in range(2):
                q = g * 2 + side
                total = acc[q] + value[:, side * L : side * L + L]
                for c in range(3):
                    out[q, c] = (rpos[q, pl.ds(c, 1), :] - CENTRE) * total[0:16] - total[16 + 16 * c : 32 + 16 * c]
            emit(g * 2)

        loop(0, NN // 2, second)

    def nothing(*_):
        return None

    def scatter(phase, parts, sums):
        def emit(q):
            row_copy(phase, parts.at[q], sums, q, True).start()

            @pl.when(q + 1 < OWN)
            def _():
                row_copy(phase, parts.at[q + 1], sums, q + 1, True).start()

        return emit

    def summed(phase, parts, sums):
        for q in range(OWN):
            row_copy(phase, parts.at[q], sums, q, True).wait_recv()
        return ((sums[0] + sums[1]) + (sums[2] + sums[3])) + ((sums[4] + sums[5]) + (sums[6] + parts[OWN]))

    lane = lax.broadcasted_iota(jnp.int32, (S, L), 1)

    product(1, xg0, pb1, nothing, nothing, scatter(1, pb1, rb1))
    xg1[0] = summed(1, pb1, rb1)
    block_send(2, xg1)

    part = jnp.zeros((2 * S, L), F32)
    for c in range(3):
        a, b = xg0[0, c], xg1[0, c]
        part = part + mt(jnp.concatenate([a, b], axis=0), jnp.concatenate([a, b, b, b, b, b, b, b], axis=0))
    ga1[n] = jnp.where(lane < 32, part[0:16], part[16:32])
    narrow_send(0, ga1)

    def forward1():
        narrow_recv(0, ga1)
        gb1[w] = all_of(ga1, NN)
        wide_send(0, gb1)

    product(2, xg1, pb2, forward1, nothing, scatter(2, pb2, rb2))

    wide_recv(0, gb1)
    total = all_of(gb1, NW)
    g00, g01, g11 = total[:, 0:16], total[:, 16:32], total[:, 32:48]
    upper0, inv0 = cholesky_pair(g00)

    def inside(g):
        return mt(mm(inv0, g), inv0)

    h1, c11, k1 = inside(g01), inside(g00), inside(g11)
    f1 = h1 + (h1 - mm(c11, h1))
    f1t = transposed(f1)
    fh = mm(f1t, h1)
    gram = k1 - fh - transposed(fh) + mm(f1t, mm(c11, f1))
    y1 = summed(2, pb2, rb2)
    xg2[0] = y1
    block_send(3, xg2, HALF)
    xr[OWN] = y1
    for q in range(OWN):
        row_copy(3, xr.at[OWN], xr, q, False).start()

    upper1, inv1 = cholesky_pair(gram)
    p21t = mm(inv1, inv0)
    p20t = -mm(mm(inv1, f1t), inv0)
    for c in range(3):
        a, y0 = xg0[0, c], xg1[0, c]
        vec_ref[c, 0:16] = mm(inv0, a)
        vec_ref[c, 16:32] = mm(p20t, a) + mm(p21t, y0)
        vec_ref[c, 32:48] = mm(p20t, y0)

    part = jnp.zeros((5 * S, L), F32)
    for c in range(3):
        y0, y1c = xg1[0, c], xg2[0, c]
        q1, q2 = vec_ref[c, 0:16], vec_ref[c, 16:32]
        wv = vec_ref[c, 32:48] + mm(p21t, y1c)
        vec_ref[c, 32:48] = wv
        part = part + mt(
            jnp.concatenate([q1, q2, wv, y0, y1c], axis=0), jnp.concatenate([q1, q2, wv, q2, wv, wv, y1c, y1c], axis=0)
        )
    packed = jnp.where(lane < 48, part[0:16], part[16:32])
    packed = jnp.where(lane < 80, packed, part[32:48])
    packed = jnp.where(lane < 96, packed, part[48:64])
    ga2[n] = jnp.where(lane < 112, packed, part[64:80])
    narrow_send(1, ga2)

    def forward2():
        narrow_recv(1, ga2)
        gb2[w] = all_of(ga2, NN)
        wide_send(1, gb2)

    product(3, xg2, pz, nothing, forward2, nothing, True)
    for q in range(OWN):
        row_copy(3, xr.at[OWN], xr, q, False).wait_recv()
    part = jnp.zeros((S, S), F32)
    for c in range(3):
        part = part + mt(
            jnp.concatenate([xr[b, c] for b in range(NN)], axis=1), jnp.concatenate([pz[b, c] for b in range(NN)], axis=1)
        )
    za[n, :, 0:16] = part
    narrow_send(2, za)

    narrow_recv(2, za)
    zb[w] = all_of(za, NN)
    wide_send(2, zb)

    wide_recv(1, gb2)
    total = all_of(gb2, NW)
    c11, c12, ha, c22, hb, k, g12, g22 = [total[:, 16 * i : 16 * i + 16] for i in range(8)]
    p20, p21 = transposed(p20t), transposed(p21t)
    c12t = transposed(c12)
    fa = ha + (ha - mm(c11, ha) - mm(c12, hb))
    fb = hb + (hb - mm(c12t, ha) - mm(c22, hb))
    fat, fbt = transposed(fa), transposed(fb)
    hat, hbt = transposed(ha), transposed(hb)
    fh = mm(fat, ha) + mm(fbt, hb)
    cf = mm(fat, mm(c11, fa) + mm(c12, fb)) + mm(fbt, mm(c12t, fa) + mm(c22, fb))
    upper2, inv2 = cholesky_pair(k - fh - transposed(fh) + cf)
    zz = mm(p20t, mm(g12, p20) + mm(g22, p21)) + mm(p21t, mm(g22, p20))
    wmq1 = mm(hat, f1) + mm(hbt, upper1)
    side = mm(wmq1, fa) + mm(k, fb)
    inner = zz - side - transposed(side) + mm(fat, mm(h1, fa) + mm(ha, fb)) + mm(fbt, mm(hat, fa) + mm(hb, fb))
    a3 = mt(mm(inv2, inner), inv2)

    def sym(value):
        return 0.5 * (value + transposed(value))

    order = 3 * S
    tri = jnp.zeros((order, order), F32)
    low = [
        (lax.broadcasted_iota(jnp.int32, (order, S), 0) == lax.broadcasted_iota(jnp.int32, (order, S), 1) + S * i).astype(F32)
        for i in range(3)
    ]
    blocks = [(0, 0, sym(h1)), (1, 1, sym(hb)), (2, 2, sym(a3)), (1, 0, upper1), (2, 1, upper2)]
    blocks += [(0, 1, transposed(upper1)), (1, 2, transposed(upper2))]
    for i, j, block in blocks:
        tri = tri + mt(mm(low[i], block), low[j])
    tri_ref[...] = tri
    mix_ref[...] = mm(low[2], mm(inv2, p21t))
    low_ref[...] = transposed(upper0)
    for c in range(3):
        q1, q2, wv = vec_ref[c, 0:16], vec_ref[c, 16:32], vec_ref[c, 32:48]
        vec_ref[c, 32:48] = mm(inv2, wv - mm(fat, q1) - mm(fbt, q2))
    wide_recv(2, zb)
    ztot_ref[...] = all_of(zb, NW)

    for phase, buffer in enumerate([cpos, xg0, xg1, xg2]):
        for p in range(1, NW if phase < 3 else HALF):
            block_copy(phase, buffer, p).wait_send()
    for phase, buffer in enumerate([gb1, gb2, zb]):
        wide_sent(phase, buffer)
    for phase, buffer in enumerate([ga1, ga2, za]):
        narrow_sent(phase, buffer)
    for q in range(OWN):
        row_copy(0, cpos.at[0], rpos, q, False).wait_send()
        row_copy(1, pb1.at[q], rb1, q, True).wait_send()
        row_copy(2, pb2.at[q], rb2, q, True).wait_send()
        row_copy(3, xr.at[OWN], xr, q, False).wait_send()


def last_kernel(vec_ref, tri_ref, mix_ref, low_ref, ztot_ref, out_ref, y_ref, z_ref):
    zraw = ztot_ref[:, 0:16]
    mix = mix_ref[...]
    tri = tri_ref[...] + mt(mm(mix, 0.5 * (zraw + transposed(zraw))), mix)
    order = 3 * S
    scale = jnp.sqrt(jnp.sum(tri * tri))
    ident = eye(order)
    y_ref[...] = tri / scale
    z_ref[...] = ident

    def more(carry):
        step, gap = carry
        return jnp.logical_and(step < ROOT_STEPS, jnp.logical_not(gap < 1e-8))

    def newton(carry):
        step, _ = carry
        y, z = y_ref[...], z_ref[...]
        zy = mm(z, y)
        factor = 1.5 * ident - 0.5 * zy
        y_ref[...] = mm(y, factor)
        z_ref[...] = mm(factor, z)
        off = zy - ident
        return step + 1, jnp.sum(off * off)

    lax.while_loop(more, newton, (jnp.int32(0), jnp.float32(1.0)))
    root = y_ref[...] * jnp.sqrt(scale)
    first = (
        lax.broadcasted_iota(jnp.int32, (S, order), 0) == lax.broadcasted_iota(jnp.int32, (S, order), 1)
    ).astype(F32)
    mixing = mm(low_ref[...], mt(first, root))
    for c in range(3):
        out_ref[c] = mm(mixing, vec_ref[c])


def per_device(positions, noise):
    block = (3, S, L)
    order = 3 * S
    vmem = pl.BlockSpec(memory_space=pltpu.VMEM)
    middle = pl.pallas_call(
        main_kernel,
        out_shape=[
            jax.ShapeDtypeStruct((3, order, L), F32),
            jax.ShapeDtypeStruct((order, order), F32),
            jax.ShapeDtypeStruct((order, S), F32),
            jax.ShapeDtypeStruct((S, S), F32),
            jax.ShapeDtypeStruct((S, L), F32),
        ],
        in_specs=[pl.BlockSpec(memory_space=pl.ANY)] * 2,
        out_specs=[vmem] * 5,
        scratch_shapes=[
            pltpu.VMEM((NW, 3, L), F32),
            pltpu.VMEM((NN, 3, L), F32),
            pltpu.VMEM((NW, *block), F32),
            pltpu.VMEM((NW, *block), F32),
            pltpu.VMEM((NW, *block), F32),
            pltpu.VMEM((NN, *block), F32),
            pltpu.VMEM((NN, *block), F32),
            pltpu.VMEM((NN, *block), F32),
            pltpu.VMEM((NN, *block), F32),
            pltpu.VMEM((NN, *block), F32),
            pltpu.VMEM((NN, *block), F32),
            pltpu.VMEM((4, NN, NW * L, L), BF16),
            pltpu.VMEM((4, NN, NW * L, L), BF16),
            pltpu.VMEM((2, 4, L, NW * L // 2), BF16),
            pltpu.VMEM((NN, 64, L), F32),
            pltpu.VMEM((4, 3, L, L), F32),
            pltpu.VMEM((NN, S, L), F32),
            pltpu.VMEM((NW, S, L), F32),
            pltpu.VMEM((NN, S, L), F32),
            pltpu.VMEM((NW, S, L), F32),
            pltpu.VMEM((NN, S, L), F32),
            pltpu.VMEM((NW, S, L), F32),
            pltpu.SemaphoreType.DMA((4, NW)),
            pltpu.SemaphoreType.DMA((4, NW)),
            pltpu.SemaphoreType.DMA((3, NW)),
            pltpu.SemaphoreType.DMA((3, NW)),
            pltpu.SemaphoreType.DMA((3, NN)),
            pltpu.SemaphoreType.DMA((3, NN)),
            pltpu.SemaphoreType.DMA((4, NN)),
            pltpu.SemaphoreType.DMA((4, NN)),
            pltpu.SemaphoreType.DMA((2,)),
        ],
        compiler_params=pltpu.CompilerParams(
            collective_id=0, has_side_effects=True, vmem_limit_bytes=56 * 1024 * 1024
        ),
        name="lanczos",
    )(positions, noise)
    return pl.pallas_call(
        last_kernel,
        out_shape=jax.ShapeDtypeStruct(block, F32),
        in_specs=[vmem] * 5,
        out_specs=vmem,
        scratch_shapes=[pltpu.VMEM((order, order), F32), pltpu.VMEM((order, order), F32)],
        name="finish",
    )(*middle)


def solution(mesh):
    axes = ("wide", "narrow")
    return jax.shard_map(
        per_device,
        mesh=mesh,
        in_specs=(P(None, axes), P(None, None, axes)),
        out_specs=P(None, None, axes),
        check_vma=False,
    )
```

```python
import functools

import jax
import jax.numpy as jnp
from jax import lax
from jax.experimental import pallas as pl
from jax.experimental.pallas import tpu as pltpu
from jax.sharding import PartitionSpec as P

ROOT_STEPS = 30
NW = 16
NN = 8
S = 16
L = 128
CENTRE = 34.0
MESH = pl.DeviceIdType.MESH
HI = lax.Precision.HIGHEST
F32 = jnp.float32
BF16 = jnp.bfloat16


def mm(a, b):
    return lax.dot_general(a, b, (((1,), (0,)), ((), ())), precision=HI, preferred_element_type=F32)


def mt(a, b):
    return lax.dot_general(a, b, (((1,), (1,)), ((), ())), precision=HI, preferred_element_type=F32)


def eye(n):
    return (lax.broadcasted_iota(jnp.int32, (n, n), 0) == lax.broadcasted_iota(jnp.int32, (n, n), 1)).astype(F32)


def transposed(a):
    return mt(eye(a.shape[1]), a)


def cholesky_pair(gram):
    n = gram.shape[0]
    rows = lax.broadcasted_iota(jnp.int32, (n, n), 0)
    cols = lax.broadcasted_iota(jnp.int32, (n, n), 1)
    left, right = gram, eye(n)
    upper, inverse = jnp.zeros((n, n), F32), jnp.zeros((n, n), F32)
    for c in range(n):
        scale = lax.rsqrt(jnp.broadcast_to(left[c : c + 1, c : c + 1], (1, n)))
        row = left[c : c + 1, :] * scale
        other = right[c : c + 1, :] * scale
        upper = jnp.where((rows == c) & (cols >= c), jnp.broadcast_to(row, (n, n)), upper)
        inverse = jnp.where((rows == c) & (cols <= c), jnp.broadcast_to(other, (n, n)), inverse)
        if c + 1 < n:
            factor = jnp.broadcast_to(left[:, c : c + 1], (n, n)) * scale
            left = left - factor * row
            right = right - jnp.where(rows > c, factor * other, 0.0)
    return upper, inverse


def split(value):
    high = value.astype(BF16)
    low = (value - high.astype(F32)).astype(BF16)
    return high, low


OFFSETS = [(0, 0), (2, 0), (1, 0), (0, 1), (1, 1), (1, 3), (2, 1), (1, 2), (0, 2), (2, 2)]
OFFSETS += [(0, 3), (3, 0), (3, 1), (3, 3), (2, 3), (3, 2)]
HALF = 10
OWN = NN - 1


def row_place(q):
    g, side = q // 2, q % 2
    return (2 + g * (g + 1) // 2) % 4, (side + g // 3) % 2


def main_kernel(
    pos_hbm,
    noise_hbm,
    vec_ref,
    tri_ref,
    mix_ref,
    low_ref,
    ztot_ref,
    cpos,
    rpos,
    xg0,
    xg1,
    xg2,
    xr,
    pb1,
    pb2,
    rb1,
    rb2,
    pz,
    lhi,
    llo,
    rmat,
    acc,
    xjb,
    ga1,
    gb1,
    ga2,
    gb2,
    za,
    zb,
    send_b,
    recv_b,
    send_w,
    recv_w,
    send_n,
    recv_n,
    send_q,
    recv_q,
    load_sem,
):
    w = lax.axis_index("wide")
    n = lax.axis_index("narrow")

    def loop(begin, end, body):
        def step(i, carry):
            body(i)
            return carry

        lax.fori_loop(begin, end, step, 0)

    def block_copy(phase, buffer, p):
        a, b = OFFSETS[p]
        x = lax.rem(w // 4 + 4 - a, 4)
        z = lax.rem(lax.rem(w, 4) + 4 - b, 4)
        return pltpu.make_async_remote_copy(
            src_ref=buffer.at[0],
            dst_ref=buffer.at[p],
            send_sem=send_b.at[phase, p],
            recv_sem=recv_b.at[phase, p],
            device_id={"wide": x * 4 + z},
            device_id_type=MESH,
        )

    def block_send(phase, buffer, count=NW):
        for p in range(1, count):
            block_copy(phase, buffer, p).start()

    def block_arrived(phase, buffer, p):
        pltpu.make_async_remote_copy(
            src_ref=buffer.at[0],
            dst_ref=buffer.at[p],
            send_sem=send_b.at[phase, p],
            recv_sem=recv_b.at[phase, p],
            device_id={"wide": w},
            device_id_type=MESH,
        ).wait_recv()

    def wide_copy(phase, src, dst, target, slot):
        return pltpu.make_async_remote_copy(
            src_ref=src,
            dst_ref=dst.at[slot],
            send_sem=send_w.at[phase, target],
            recv_sem=recv_w.at[phase, slot],
            device_id={"wide": target},
            device_id_type=MESH,
        )

    def narrow_copy(phase, src, dst, target, slot):
        return pltpu.make_async_remote_copy(
            src_ref=src,
            dst_ref=dst.at[slot],
            send_sem=send_n.at[phase, target],
            recv_sem=recv_n.at[phase, slot],
            device_id={"narrow": target},
            device_id_type=MESH,
        )

    def row_copy(phase, src, dst, q, away):
        a, b = row_place(q)
        y = lax.rem(n // 2 + (a if away else 4 - a), 4)
        core = lax.rem(lax.rem(n, 2) + b, 2)
        return pltpu.make_async_remote_copy(
            src_ref=src,
            dst_ref=dst.at[q],
            send_sem=send_q.at[phase, q],
            recv_sem=recv_q.at[phase, q],
            device_id={"narrow": y * 2 + core},
            device_id_type=MESH,
        )

    def wide_send(phase, dst):
        loop(1, NW, lambda p: wide_copy(phase, dst.at[w], dst, lax.rem(w + p, NW), w).start())

    def wide_recv(phase, dst):
        def one(p):
            s = lax.rem(w + p, NW)
            wide_copy(phase, dst.at[s], dst, s, s).wait_recv()

        loop(1, NW, one)

    def wide_sent(phase, dst):
        def one(p):
            s = lax.rem(w + p, NW)
            wide_copy(phase, dst.at[w], dst, s, w).wait_send()

        loop(1, NW, one)

    def narrow_send(phase, dst):
        loop(1, NN, lambda p: narrow_copy(phase, dst.at[n], dst, lax.rem(n + p, NN), n).start())

    def narrow_recv(phase, dst):
        def one(p):
            s = lax.rem(n + p, NN)
            narrow_copy(phase, dst.at[s], dst, s, s).wait_recv()

        loop(1, NN, one)

    def narrow_sent(phase, dst):
        def one(p):
            s = lax.rem(n + p, NN)
            narrow_copy(phase, dst.at[n], dst, s, n).wait_send()

        loop(1, NN, one)

    def all_of(buffer, count):
        parts = [buffer[i] for i in range(count)]
        while len(parts) > 1:
            parts = [parts[i] + parts[i + 1] for i in range(0, len(parts), 2)]
        return parts[0]

    barrier = pltpu.get_barrier_semaphore()

    def greet_wide(p):
        along_x = lax.rem(w // 4 + p, 4) * 4 + lax.rem(w, 4)
        along_z = w // 4 * 4 + lax.rem(lax.rem(w, 4) + p, 4)
        pl.semaphore_signal(barrier, inc=1, device_id={"wide": along_x}, device_id_type=MESH)
        pl.semaphore_signal(barrier, inc=1, device_id={"wide": along_z}, device_id_type=MESH)

    def greet_narrow(p):
        pl.semaphore_signal(barrier, inc=1, device_id={"narrow": lax.rem(n + p, NN)}, device_id_type=MESH)

    loop(1, 4, greet_wide)
    loop(1, NN, greet_narrow)
    loads = [
        pltpu.make_async_copy(pos_hbm, cpos.at[0], load_sem.at[0]),
        pltpu.make_async_copy(noise_hbm, xg0.at[0], load_sem.at[1]),
    ]
    for load in loads:
        load.start()
    za[n] = jnp.zeros((S, L), F32)
    for load in loads:
        load.wait()
    rpos[OWN] = cpos[0]
    pl.semaphore_wait(barrier, 6 + NN - 1)

    for q in range(OWN):
        row_copy(0, cpos.at[0], rpos, q, False).start()
    for a in range(1, 4):
        block_copy(0, cpos, OFFSETS.index((a, 0))).start()
        block_copy(0, cpos, OFFSETS.index((0, a))).start()
    for a in range(1, 4):
        held = OFFSETS.index((a, 0))
        block_arrived(0, cpos, held)
        for b in range(1, 4):
            slot = OFFSETS.index((a, b))
            pltpu.make_async_remote_copy(
                src_ref=cpos.at[held],
                dst_ref=cpos.at[slot],
                send_sem=send_b.at[0, slot],
                recv_sem=recv_b.at[0, slot],
                device_id={"wide": w // 4 * 4 + lax.rem(lax.rem(w, 4) + 4 - b, 4)},
                device_id_type=MESH,
            ).start()
    for a in range(1, 4):
        block_arrived(0, cpos, OFFSETS.index((0, a)))
    for q in range(OWN):
        row_copy(0, cpos.at[0], rpos, q, False).wait_recv()

    def build(group):
        for i in range(4):
            columns = jnp.concatenate([cpos[group * 4 + i], jnp.zeros((5, L), F32)], axis=0).T
            for c in range(3):
                xjb[i, c] = jnp.broadcast_to(columns[:, c : c + 1], (L, L))

        def one(step):
            i = step // 4
            for half in range(2):
                ib = lax.rem(step, 4) * 2 + half
                xi = [jnp.broadcast_to(rpos[ib, c : c + 1, :], (16, L)) for c in range(3)]
                for jt in range(8):
                    d = [xi[c] - xjb[i, c, jt * 16 : jt * 16 + 16, :] for c in range(3)]
                    sq = jnp.maximum(d[0] * d[0] + d[1] * d[1] + d[2] * d[2], 1e-20)
                    inv = lax.rsqrt(sq)
                    inv2 = inv * inv
                    near = sq < 4.0
                    iso = jnp.where(near, 1.0 - 0.28125 * (sq * inv), inv * (0.75 + 0.5 * inv2))
                    outer = inv * jnp.where(near, 0.09375, inv2 * (0.75 - 1.5 * inv2))
                    places = pl.ds(pl.multiple_of((group * 4 + i) * L + jt * 16, 16), 16)
                    for k, value in enumerate([outer * d[0], outer * d[1], outer * d[2], iso]):
                        high, low = split(value)
                        lhi[k, ib, places, :] = high
                        llo[k, ib, places, :] = low

        loop(0, 16, one)

    build(0)
    for a in range(1, 4):
        for b in range(1, 4):
            block_arrived(0, cpos, OFFSETS.index((a, b)))
    block_send(1, xg0)
    loop(1, 4, build)

    half_blocks = NW // 2
    depth = half_blocks * L

    def product(phase, xg, out, early, between, emit, symmetric=False):
        def expand(p, factor=None):
            lanes = pl.ds(pl.multiple_of(lax.rem(p, half_blocks) * L, L), L)
            half = p // half_blocks
            x = [cpos[p, c : c + 1, :] - CENTRE for c in range(3)]
            v = [xg[p, e] if factor is None else factor * xg[p, e] for e in range(3)]
            pieces = [jnp.concatenate([v[e], x[0] * v[e], x[1] * v[e], x[2] * v[e]], axis=0) for e in range(3)]
            pieces.append(jnp.concatenate([jnp.zeros((S, L), F32), -v[0], -v[1], -v[2]], axis=0))
            for k in range(4):
                high, low = split(pieces[k])
                rmat[half, k, 0:64, lanes] = high
                rmat[half, k, 64:128, lanes] = low

        def arrived_expand(p):
            block_arrived(phase, xg, p)
            expand(p)

        def arrived_double(p):
            block_arrived(phase, xg, p)
            expand(p, 2.0)

        columns = HALF if symmetric else NW

        def pair_of(half, q, count=2):
            size = min(depth, columns * L - half * depth)
            rows = slice(half * depth, half * depth + size)
            total, small = None, None
            for k in range(4):
                high = jnp.concatenate([lhi[k, q + i, rows, :] for i in range(count)], axis=1)
                low = jnp.concatenate([llo[k, q + i, rows, :] for i in range(count)], axis=1)
                one = jnp.dot(rmat[half, k, :, 0:size], high, preferred_element_type=F32)
                two = jnp.dot(rmat[half, k, 0:64, 0:size], low, preferred_element_type=F32)
                total = one if total is None else total + one
                small = two if small is None else small + two
            return total[0:64] + (total[64:128] + small)

        expand(0)
        loop(1, 2, arrived_expand)
        loop(2, half_blocks, arrived_double if symmetric else arrived_expand)

        def first(g):
            value = pair_of(0, g * 4, 4)
            for side in range(4):
                acc[g * 4 + side] = value[:, side * L : side * L + L]

        def turn(g):
            first(g)

            @pl.when(g == 0)
            def _():
                early()

        loop(0, NN // 4, turn)
        between()
        loop(half_blocks, columns, arrived_expand)

        def second(g):
            value = pair_of(1, g * 2)
            for side in range(2):
                q = g * 2 + side
                total = acc[q] + value[:, side * L : side * L + L]
                for c in range(3):
                    out[q, c] = (rpos[q, pl.ds(c, 1), :] - CENTRE) * total[0:16] - total[16 + 16 * c : 32 + 16 * c]
            emit(g * 2)

        loop(0, NN // 2, second)

    def nothing(*_):
        return None

    def scatter(phase, parts, sums):
        def emit(q):
            row_copy(phase, parts.at[q], sums, q, True).start()

            @pl.when(q + 1 < OWN)
            def _():
                row_copy(phase, parts.at[q + 1], sums, q + 1, True).start()

        return emit

    def summed(phase, parts, sums):
        for q in range(OWN):
            row_copy(phase, parts.at[q], sums, q, True).wait_recv()
        return ((sums[0] + sums[1]) + (sums[2] + sums[3])) + ((sums[4] + sums[5]) + (sums[6] + parts[OWN]))

    lane = lax.broadcasted_iota(jnp.int32, (S, L), 1)

    product(1, xg0, pb1, nothing, nothing, scatter(1, pb1, rb1))
    xg1[0] = summed(1, pb1, rb1)
    block_send(2, xg1)

    part = jnp.zeros((2 * S, L), F32)
    for c in range(3):
        a, b = xg0[0, c], xg1[0, c]
        part = part + mt(jnp.concatenate([a, b], axis=0), jnp.concatenate([a, b, b, b, b, b, b, b], axis=0))
    ga1[n] = jnp.where(lane < 32, part[0:16], part[16:32])
    narrow_send(0, ga1)

    def forward1():
        narrow_recv(0, ga1)
        gb1[w] = all_of(ga1, NN)
        wide_send(0, gb1)

    product(2, xg1, pb2, forward1, nothing, scatter(2, pb2, rb2))

    wide_recv(0, gb1)
    total = all_of(gb1, NW)
    g00, g01, g11 = total[:, 0:16], total[:, 16:32], total[:, 32:48]
    upper0, inv0 = cholesky_pair(g00)

    def inside(g):
        return mt(mm(inv0, g), inv0)

    h1, c11, k1 = inside(g01), inside(g00), inside(g11)
    f1 = h1 + (h1 - mm(c11, h1))
    f1t = transposed(f1)
    fh = mm(f1t, h1)
    gram = k1 - fh - transposed(fh) + mm(f1t, mm(c11, f1))
    y1 = summed(2, pb2, rb2)
    xg2[0] = y1
    block_send(3, xg2, HALF)
    xr[OWN] = y1
    for q in range(OWN):
        row_copy(3, xr.at[OWN], xr, q, False).start()

    upper1, inv1 = cholesky_pair(gram)
    p21t = mm(inv1, inv0)
    p20t = -mm(mm(inv1, f1t), inv0)
    for c in range(3):
        a, y0 = xg0[0, c], xg1[0, c]
        vec_ref[c, 0:16] = mm(inv0, a)
        vec_ref[c, 16:32] = mm(p20t, a) + mm(p21t, y0)
        vec_ref[c, 32:48] = mm(p20t, y0)

    part = jnp.zeros((5 * S, L), F32)
    for c in range(3):
        y0, y1c = xg1[0, c], xg2[0, c]
        q1, q2 = vec_ref[c, 0:16], vec_ref[c, 16:32]
        wv = vec_ref[c, 32:48] + mm(p21t, y1c)
        vec_ref[c, 32:48] = wv
        part = part + mt(
            jnp.concatenate([q1, q2, wv, y0, y1c], axis=0), jnp.concatenate([q1, q2, wv, q2, wv, wv, y1c, y1c], axis=0)
        )
    packed = jnp.where(lane < 48, part[0:16], part[16:32])
    packed = jnp.where(lane < 80, packed, part[32:48])
    packed = jnp.where(lane < 96, packed, part[48:64])
    ga2[n] = jnp.where(lane < 112, packed, part[64:80])
    narrow_send(1, ga2)

    def forward2():
        narrow_recv(1, ga2)
        gb2[w] = all_of(ga2, NN)
        wide_send(1, gb2)

    product(3, xg2, pz, nothing, forward2, nothing, True)
    for q in range(OWN):
        row_copy(3, xr.at[OWN], xr, q, False).wait_recv()
    part = jnp.zeros((S, S), F32)
    for c in range(3):
        part = part + mt(
            jnp.concatenate([xr[b, c] for b in range(NN)], axis=1), jnp.concatenate([pz[b, c] for b in range(NN)], axis=1)
        )
    za[n, :, 0:16] = part
    narrow_send(2, za)

    narrow_recv(2, za)
    zb[w] = all_of(za, NN)
    wide_send(2, zb)

    wide_recv(1, gb2)
    total = all_of(gb2, NW)
    c11, c12, ha, c22, hb, k, g12, g22 = [total[:, 16 * i : 16 * i + 16] for i in range(8)]
    p20, p21 = transposed(p20t), transposed(p21t)
    c12t = transposed(c12)
    fa = ha + (ha - mm(c11, ha) - mm(c12, hb))
    fb = hb + (hb - mm(c12t, ha) - mm(c22, hb))
    fat, fbt = transposed(fa), transposed(fb)
    hat, hbt = transposed(ha), transposed(hb)
    fh = mm(fat, ha) + mm(fbt, hb)
    cf = mm(fat, mm(c11, fa) + mm(c12, fb)) + mm(fbt, mm(c12t, fa) + mm(c22, fb))
    upper2, inv2 = cholesky_pair(k - fh - transposed(fh) + cf)
    zz = mm(p20t, mm(g12, p20) + mm(g22, p21)) + mm(p21t, mm(g22, p20))
    wmq1 = mm(hat, f1) + mm(hbt, upper1)
    side = mm(wmq1, fa) + mm(k, fb)
    inner = zz - side - transposed(side) + mm(fat, mm(h1, fa) + mm(ha, fb)) + mm(fbt, mm(hat, fa) + mm(hb, fb))
    a3 = mt(mm(inv2, inner), inv2)

    def sym(value):
        return 0.5 * (value + transposed(value))

    order = 3 * S
    tri = jnp.zeros((order, order), F32)
    low = [
        (lax.broadcasted_iota(jnp.int32, (order, S), 0) == lax.broadcasted_iota(jnp.int32, (order, S), 1) + S * i).astype(F32)
        for i in range(3)
    ]
    blocks = [(0, 0, sym(h1)), (1, 1, sym(hb)), (2, 2, sym(a3)), (1, 0, upper1), (2, 1, upper2)]
    blocks += [(0, 1, transposed(upper1)), (1, 2, transposed(upper2))]
    for i, j, block in blocks:
        tri = tri + mt(mm(low[i], block), low[j])
    tri_ref[...] = tri
    mix_ref[...] = mm(low[2], mm(inv2, p21t))
    low_ref[...] = transposed(upper0)
    for c in range(3):
        q1, q2, wv = vec_ref[c, 0:16], vec_ref[c, 16:32], vec_ref[c, 32:48]
        vec_ref[c, 32:48] = mm(inv2, wv - mm(fat, q1) - mm(fbt, q2))
    wide_recv(2, zb)
    ztot_ref[...] = all_of(zb, NW)

    for phase, buffer in enumerate([cpos, xg0, xg1, xg2]):
        for p in range(1, NW if phase < 3 else HALF):
            block_copy(phase, buffer, p).wait_send()
    for phase, buffer in enumerate([gb1, gb2, zb]):
        wide_sent(phase, buffer)
    for phase, buffer in enumerate([ga1, ga2, za]):
        narrow_sent(phase, buffer)
    for q in range(OWN):
        row_copy(0, cpos.at[0], rpos, q, False).wait_send()
        row_copy(1, pb1.at[q], rb1, q, True).wait_send()
        row_copy(2, pb2.at[q], rb2, q, True).wait_send()
        row_copy(3, xr.at[OWN], xr, q, False).wait_send()


def last_kernel(vec_ref, tri_ref, mix_ref, low_ref, ztot_ref, out_ref, y_ref, z_ref):
    zraw = ztot_ref[:, 0:16]
    mix = mix_ref[...]
    tri = tri_ref[...] + mt(mm(mix, 0.5 * (zraw + transposed(zraw))), mix)
    order = 3 * S
    scale = jnp.sqrt(jnp.sum(tri * tri))
    ident = eye(order)
    y_ref[...] = tri / scale
    z_ref[...] = ident

    def more(carry):
        step, gap = carry
        return jnp.logical_and(step < ROOT_STEPS, jnp.logical_not(gap < 1e-8))

    def newton(carry):
        step, _ = carry
        y, z = y_ref[...], z_ref[...]
        zy = mm(z, y)
        factor = 1.5 * ident - 0.5 * zy
        y_ref[...] = mm(y, factor)
        z_ref[...] = mm(factor, z)
        off = zy - ident
        return step + 1, jnp.sum(off * off)

    lax.while_loop(more, newton, (jnp.int32(0), jnp.float32(1.0)))
    root = y_ref[...] * jnp.sqrt(scale)
    first = (
        lax.broadcasted_iota(jnp.int32, (S, order), 0) == lax.broadcasted_iota(jnp.int32, (S, order), 1)
    ).astype(F32)
    mixing = mm(low_ref[...], mt(first, root))
    for c in range(3):
        out_ref[c] = mm(mixing, vec_ref[c])


def per_device(positions, noise):
    block = (3, S, L)
    order = 3 * S
    vmem = pl.BlockSpec(memory_space=pltpu.VMEM)
    middle = pl.pallas_call(
        main_kernel,
        out_shape=[
            jax.ShapeDtypeStruct((3, order, L), F32),
            jax.ShapeDtypeStruct((order, order), F32),
            jax.ShapeDtypeStruct((order, S), F32),
            jax.ShapeDtypeStruct((S, S), F32),
            jax.ShapeDtypeStruct((S, L), F32),
        ],
        in_specs=[pl.BlockSpec(memory_space=pl.ANY)] * 2,
        out_specs=[vmem] * 5,
        scratch_shapes=[
            pltpu.VMEM((NW, 3, L), F32),
            pltpu.VMEM((NN, 3, L), F32),
            pltpu.VMEM((NW, *block), F32),
            pltpu.VMEM((NW, *block), F32),
            pltpu.VMEM((NW, *block), F32),
            pltpu.VMEM((NN, *block), F32),
            pltpu.VMEM((NN, *block), F32),
            pltpu.VMEM((NN, *block), F32),
            pltpu.VMEM((NN, *block), F32),
            pltpu.VMEM((NN, *block), F32),
            pltpu.VMEM((NN, *block), F32),
            pltpu.VMEM((4, NN, NW * L, L), BF16),
            pltpu.VMEM((4, NN, NW * L, L), BF16),
            pltpu.VMEM((2, 4, L, NW * L // 2), BF16),
            pltpu.VMEM((NN, 64, L), F32),
            pltpu.VMEM((4, 3, L, L), F32),
            pltpu.VMEM((NN, S, L), F32),
            pltpu.VMEM((NW, S, L), F32),
            pltpu.VMEM((NN, S, L), F32),
            pltpu.VMEM((NW, S, L), F32),
            pltpu.VMEM((NN, S, L), F32),
            pltpu.VMEM((NW, S, L), F32),
            pltpu.SemaphoreType.DMA((4, NW)),
            pltpu.SemaphoreType.DMA((4, NW)),
            pltpu.SemaphoreType.DMA((3, NW)),
            pltpu.SemaphoreType.DMA((3, NW)),
            pltpu.SemaphoreType.DMA((3, NN)),
            pltpu.SemaphoreType.DMA((3, NN)),
            pltpu.SemaphoreType.DMA((4, NN)),
            pltpu.SemaphoreType.DMA((4, NN)),
            pltpu.SemaphoreType.DMA((2,)),
        ],
        compiler_params=pltpu.CompilerParams(
            collective_id=0, has_side_effects=True, vmem_limit_bytes=56 * 1024 * 1024
        ),
        name="lanczos",
    )(positions, noise)
    return pl.pallas_call(
        last_kernel,
        out_shape=jax.ShapeDtypeStruct(block, F32),
        in_specs=[vmem] * 5,
        out_specs=vmem,
        scratch_shapes=[pltpu.VMEM((order, order), F32), pltpu.VMEM((order, order), F32)],
        name="finish",
    )(*middle)


def solution(mesh):
    axes = ("wide", "narrow")
    return jax.shard_map(
        per_device,
        mesh=mesh,
        in_specs=(P(None, axes), P(None, None, axes)),
        out_specs=P(None, None, axes),
        check_vma=False,
    )
```

```python
import functools

import jax
import jax.numpy as jnp
from jax import lax
from jax.experimental import pallas as pl
from jax.experimental.pallas import tpu as pltpu
from jax.sharding import PartitionSpec as P

ROOT_STEPS = 30
NW = 16
NN = 8
S = 16
L = 128
CENTRE = 34.0
MESH = pl.DeviceIdType.MESH
HI = lax.Precision.HIGHEST
F32 = jnp.float32
BF16 = jnp.bfloat16


def mm(a, b):
    return lax.dot_general(a, b, (((1,), (0,)), ((), ())), precision=HI, preferred_element_type=F32)


def mt(a, b):
    return lax.dot_general(a, b, (((1,), (1,)), ((), ())), precision=HI, preferred_element_type=F32)


def eye(n):
    return (lax.broadcasted_iota(jnp.int32, (n, n), 0) == lax.broadcasted_iota(jnp.int32, (n, n), 1)).astype(F32)


def transposed(a):
    return mt(eye(a.shape[1]), a)


def cholesky_pair(gram):
    n = gram.shape[0]
    rows = lax.broadcasted_iota(jnp.int32, (n, n), 0)
    cols = lax.broadcasted_iota(jnp.int32, (n, n), 1)
    left, right = gram, eye(n)
    upper, inverse = jnp.zeros((n, n), F32), jnp.zeros((n, n), F32)
    for c in range(n):
        scale = lax.rsqrt(jnp.broadcast_to(left[c : c + 1, c : c + 1], (1, n)))
        row = left[c : c + 1, :] * scale
        other = right[c : c + 1, :] * scale
        upper = jnp.where((rows == c) & (cols >= c), jnp.broadcast_to(row, (n, n)), upper)
        inverse = jnp.where((rows == c) & (cols <= c), jnp.broadcast_to(other, (n, n)), inverse)
        if c + 1 < n:
            factor = jnp.broadcast_to(left[:, c : c + 1], (n, n)) * scale
            left = left - factor * row
            right = right - jnp.where(rows > c, factor * other, 0.0)
    return upper, inverse


def split(value):
    high = value.astype(BF16)
    low = (value - high.astype(F32)).astype(BF16)
    return high, low


OFFSETS = [(0, 0), (2, 0), (1, 0), (0, 1), (3, 0), (0, 3), (1, 1), (0, 2)]
OFFSETS += [(1, 3), (2, 1), (1, 2), (2, 2), (3, 3), (3, 1), (2, 3), (3, 2)]
HALF = (0, 1, 2, 3, 6, 7, 8, 9, 10, 11)
SELF = (0, 1, 7, 11)
OWN = NN - 1


def row_place(q):
    g, side = q // 2, q % 2
    return (2 + g * (g + 1) // 2) % 4, (side + g // 3) % 2


def main_kernel(
    pos_hbm,
    noise_hbm,
    vec_ref,
    tri_ref,
    mix_ref,
    low_ref,
    ztot_ref,
    cpos,
    rpos,
    xg0,
    xg1,
    xg2,
    xr,
    pb1,
    pb2,
    rb1,
    rb2,
    pz,
    lhi,
    llo,
    rmat,
    acc,
    xjb,
    ga1,
    gb1,
    ga2,
    gb2,
    za,
    zb,
    send_b,
    recv_b,
    send_w,
    recv_w,
    send_n,
    recv_n,
    send_q,
    recv_q,
    load_sem,
):
    w = lax.axis_index("wide")
    n = lax.axis_index("narrow")

    def loop(begin, end, body):
        def step(i, carry):
            body(i)
            return carry

        lax.fori_loop(begin, end, step, 0)

    def block_copy(phase, buffer, p):
        a, b = OFFSETS[p]
        x = lax.rem(w // 4 + 4 - a, 4)
        z = lax.rem(lax.rem(w, 4) + 4 - b, 4)
        return pltpu.make_async_remote_copy(
            src_ref=buffer.at[0],
            dst_ref=buffer.at[p],
            send_sem=send_b.at[phase, p],
            recv_sem=recv_b.at[phase, p],
            device_id={"wide": x * 4 + z},
            device_id_type=MESH,
        )

    def block_send(phase, buffer, slots=range(NW)):
        for p in slots[1:]:
            block_copy(phase, buffer, p).start()

    def block_arrived(phase, buffer, p):
        pltpu.make_async_remote_copy(
            src_ref=buffer.at[0],
            dst_ref=buffer.at[p],
            send_sem=send_b.at[phase, p],
            recv_sem=recv_b.at[phase, p],
            device_id={"wide": w},
            device_id_type=MESH,
        ).wait_recv()

    def wide_copy(phase, src, dst, target, slot):
        return pltpu.make_async_remote_copy(
            src_ref=src,
            dst_ref=dst.at[slot],
            send_sem=send_w.at[phase, target],
            recv_sem=recv_w.at[phase, slot],
            device_id={"wide": target},
            device_id_type=MESH,
        )

    def narrow_copy(phase, src, dst, target, slot):
        return pltpu.make_async_remote_copy(
            src_ref=src,
            dst_ref=dst.at[slot],
            send_sem=send_n.at[phase, target],
            recv_sem=recv_n.at[phase, slot],
            device_id={"narrow": target},
            device_id_type=MESH,
        )

    def row_copy(phase, src, dst, q, away):
        a, b = row_place(q)
        y = lax.rem(n // 2 + (a if away else 4 - a), 4)
        core = lax.rem(lax.rem(n, 2) + b, 2)
        return pltpu.make_async_remote_copy(
            src_ref=src,
            dst_ref=dst.at[q],
            send_sem=send_q.at[phase, q],
            recv_sem=recv_q.at[phase, q],
            device_id={"narrow": y * 2 + core},
            device_id_type=MESH,
        )

    def wide_send(phase, dst):
        loop(1, NW, lambda p: wide_copy(phase, dst.at[w], dst, lax.rem(w + p, NW), w).start())

    def wide_recv(phase, dst):
        def one(p):
            s = lax.rem(w + p, NW)
            wide_copy(phase, dst.at[s], dst, s, s).wait_recv()

        loop(1, NW, one)

    def wide_sent(phase, dst):
        def one(p):
            s = lax.rem(w + p, NW)
            wide_copy(phase, dst.at[w], dst, s, w).wait_send()

        loop(1, NW, one)

    def narrow_send(phase, dst):
        loop(1, NN, lambda p: narrow_copy(phase, dst.at[n], dst, lax.rem(n + p, NN), n).start())

    def narrow_recv(phase, dst):
        def one(p):
            s = lax.rem(n + p, NN)
            narrow_copy(phase, dst.at[s], dst, s, s).wait_recv()

        loop(1, NN, one)

    def narrow_sent(phase, dst):
        def one(p):
            s = lax.rem(n + p, NN)
            narrow_copy(phase, dst.at[n], dst, s, n).wait_send()

        loop(1, NN, one)

    def all_of(buffer, count):
        parts = [buffer[i] for i in range(count)]
        while len(parts) > 1:
            parts = [parts[i] + parts[i + 1] for i in range(0, len(parts), 2)]
        return parts[0]

    barrier = pltpu.get_barrier_semaphore()

    def greet_wide(p):
        along_x = lax.rem(w // 4 + p, 4) * 4 + lax.rem(w, 4)
        along_z = w // 4 * 4 + lax.rem(lax.rem(w, 4) + p, 4)
        pl.semaphore_signal(barrier, inc=1, device_id={"wide": along_x}, device_id_type=MESH)
        pl.semaphore_signal(barrier, inc=1, device_id={"wide": along_z}, device_id_type=MESH)

    def greet_narrow(p):
        pl.semaphore_signal(barrier, inc=1, device_id={"narrow": lax.rem(n + p, NN)}, device_id_type=MESH)

    loop(1, 4, greet_wide)
    loop(1, NN, greet_narrow)
    loads = [
        pltpu.make_async_copy(pos_hbm, cpos.at[0], load_sem.at[0]),
        pltpu.make_async_copy(noise_hbm, xg0.at[0], load_sem.at[1]),
    ]
    for load in loads:
        load.start()
    za[n] = jnp.zeros((S, L), F32)
    for load in loads:
        load.wait()
    rpos[OWN] = cpos[0]
    pl.semaphore_wait(barrier, 6 + NN - 1)

    for q in range(OWN):
        row_copy(0, cpos.at[0], rpos, q, False).start()
    for a in range(1, 4):
        block_copy(0, cpos, OFFSETS.index((a, 0))).start()
        block_copy(0, cpos, OFFSETS.index((0, a))).start()
    for a in range(1, 4):
        held = OFFSETS.index((a, 0))
        block_arrived(0, cpos, held)
        for b in range(1, 4):
            slot = OFFSETS.index((a, b))
            pltpu.make_async_remote_copy(
                src_ref=cpos.at[held],
                dst_ref=cpos.at[slot],
                send_sem=send_b.at[0, slot],
                recv_sem=recv_b.at[0, slot],
                device_id={"wide": w // 4 * 4 + lax.rem(lax.rem(w, 4) + 4 - b, 4)},
                device_id_type=MESH,
            ).start()
    for a in range(1, 4):
        block_arrived(0, cpos, OFFSETS.index((0, a)))
    for q in range(OWN):
        row_copy(0, cpos.at[0], rpos, q, False).wait_recv()

    def build(group):
        for i in range(4):
            columns = jnp.concatenate([cpos[group * 4 + i], jnp.zeros((5, L), F32)], axis=0).T
            for c in range(3):
                xjb[i, c] = jnp.broadcast_to(columns[:, c : c + 1], (L, L))

        def one(step):
            i = step // 4
            for half in range(2):
                ib = lax.rem(step, 4) * 2 + half
                xi = [jnp.broadcast_to(rpos[ib, c : c + 1, :], (16, L)) for c in range(3)]
                for jt in range(8):
                    d = [xi[c] - xjb[i, c, jt * 16 : jt * 16 + 16, :] for c in range(3)]
                    sq = jnp.maximum(d[0] * d[0] + d[1] * d[1] + d[2] * d[2], 1e-20)
                    inv = lax.rsqrt(sq)
                    inv2 = inv * inv
                    near = sq < 4.0
                    iso = jnp.where(near, 1.0 - 0.28125 * (sq * inv), inv * (0.75 + 0.5 * inv2))
                    outer = inv * jnp.where(near, 0.09375, inv2 * (0.75 - 1.5 * inv2))
                    places = pl.ds(pl.multiple_of((group * 4 + i) * L + jt * 16, 16), 16)
                    for k, value in enumerate([outer * d[0], outer * d[1], outer * d[2], iso]):
                        high, low = split(value)
                        lhi[k, ib, places, :] = high
                        llo[k, ib, places, :] = low

        loop(0, 16, one)

    build(0)
    for a in range(1, 4):
        for b in range(1, 4):
            block_arrived(0, cpos, OFFSETS.index((a, b)))
    block_send(1, xg0)
    loop(1, 4, build)

    half_blocks = NW // 2
    depth = half_blocks * L

    def product(phase, xg, out, early, between, emit, symmetric=False):
        def expand(p, factor=None):
            lanes = pl.ds(pl.multiple_of(lax.rem(p, half_blocks) * L, L), L)
            half = p // half_blocks
            x = [cpos[p, c : c + 1, :] - CENTRE for c in range(3)]
            v = [xg[p, e] if factor is None else factor * xg[p, e] for e in range(3)]
            pieces = [jnp.concatenate([v[e], x[0] * v[e], x[1] * v[e], x[2] * v[e]], axis=0) for e in range(3)]
            pieces.append(jnp.concatenate([jnp.zeros((S, L), F32), -v[0], -v[1], -v[2]], axis=0))
            for k in range(4):
                high, low = split(pieces[k])
                rmat[half, k, 0:64, lanes] = high
                rmat[half, k, 64:128, lanes] = low

        def arrived_expand(p):
            block_arrived(phase, xg, p)
            expand(p)

        def arrived_double(p):
            block_arrived(phase, xg, p)
            expand(p, 2.0)

        def pair_of(half, q, count=2):
            if symmetric:
                spans = [[(0, 4), (6, 8)], [(0, 4)]][half]
            else:
                spans = [(0, half_blocks)]
            total, small = None, None
            for k, (begin, end) in [(k, span) for k in range(4) for span in spans]:
                rows = slice(half * depth + begin * L, half * depth + end * L)
                places = slice(begin * L, end * L)
                high = jnp.concatenate([lhi[k, q + i, rows, :] for i in range(count)], axis=1)
                low = jnp.concatenate([llo[k, q + i, rows, :] for i in range(count)], axis=1)
                one = jnp.dot(rmat[half, k, :, places], high, preferred_element_type=F32)
                two = jnp.dot(rmat[half, k, 0:64, places], low, preferred_element_type=F32)
                total = one if total is None else total + one
                small = two if small is None else small + two
            return total[0:64] + (total[64:128] + small)

        expand(0)
        def arrivals(half):
            begin, end = max(1, half * half_blocks), (half + 1) * half_blocks
            if not symmetric:
                loop(begin, end, arrived_expand)
                return
            for p in HALF:
                if begin <= p < end:
                    (arrived_expand if p in SELF else arrived_double)(p)

        arrivals(0)

        def first(g):
            value = pair_of(0, g * 4, 4)
            for side in range(4):
                acc[g * 4 + side] = value[:, side * L : side * L + L]

        def turn(g):
            first(g)

            @pl.when(g == 0)
            def _():
                early()

        loop(0, NN // 4, turn)
        between()
        arrivals(1)

        def second(g):
            value = pair_of(1, g * 2)
            for side in range(2):
                q = g * 2 + side
                total = acc[q] + value[:, side * L : side * L + L]
                for c in range(3):
                    out[q, c] = (rpos[q, pl.ds(c, 1), :] - CENTRE) * total[0:16] - total[16 + 16 * c : 32 + 16 * c]
            emit(g * 2)

        loop(0, NN // 2, second)

    def nothing(*_):
        return None

    def scatter(phase, parts, sums):
        def emit(q):
            row_copy(phase, parts.at[q], sums, q, True).start()

            @pl.when(q + 1 < OWN)
            def _():
                row_copy(phase, parts.at[q + 1], sums, q + 1, True).start()

        return emit

    def summed(phase, parts, sums):
        for q in range(OWN):
            row_copy(phase, parts.at[q], sums, q, True).wait_recv()
        return ((sums[0] + sums[1]) + (sums[2] + sums[3])) + ((sums[4] + sums[5]) + (sums[6] + parts[OWN]))

    lane = lax.broadcasted_iota(jnp.int32, (S, L), 1)

    product(1, xg0, pb1, nothing, nothing, scatter(1, pb1, rb1))
    xg1[0] = summed(1, pb1, rb1)
    block_send(2, xg1)

    part = jnp.zeros((2 * S, L), F32)
    for c in range(3):
        a, b = xg0[0, c], xg1[0, c]
        part = part + mt(jnp.concatenate([a, b], axis=0), jnp.concatenate([a, b, b, b, b, b, b, b], axis=0))
    ga1[n] = jnp.where(lane < 32, part[0:16], part[16:32])
    narrow_send(0, ga1)

    def forward1():
        narrow_recv(0, ga1)
        gb1[w] = all_of(ga1, NN)
        wide_send(0, gb1)

    product(2, xg1, pb2, forward1, nothing, scatter(2, pb2, rb2))

    wide_recv(0, gb1)
    total = all_of(gb1, NW)
    g00, g01, g11 = total[:, 0:16], total[:, 16:32], total[:, 32:48]
    upper0, inv0 = cholesky_pair(g00)

    def inside(g):
        return mt(mm(inv0, g), inv0)

    h1, c11, k1 = inside(g01), inside(g00), inside(g11)
    f1 = h1 + (h1 - mm(c11, h1))
    f1t = transposed(f1)
    fh = mm(f1t, h1)
    gram = k1 - fh - transposed(fh) + mm(f1t, mm(c11, f1))
    y1 = summed(2, pb2, rb2)
    xg2[0] = y1
    block_send(3, xg2, HALF)
    xr[OWN] = y1
    for q in range(OWN):
        row_copy(3, xr.at[OWN], xr, q, False).start()

    upper1, inv1 = cholesky_pair(gram)
    p21t = mm(inv1, inv0)
    p20t = -mm(mm(inv1, f1t), inv0)
    for c in range(3):
        a, y0 = xg0[0, c], xg1[0, c]
        vec_ref[c, 0:16] = mm(inv0, a)
        vec_ref[c, 16:32] = mm(p20t, a) + mm(p21t, y0)
        vec_ref[c, 32:48] = mm(p20t, y0)

    part = jnp.zeros((5 * S, L), F32)
    for c in range(3):
        y0, y1c = xg1[0, c], xg2[0, c]
        q1, q2 = vec_ref[c, 0:16], vec_ref[c, 16:32]
        wv = vec_ref[c, 32:48] + mm(p21t, y1c)
        vec_ref[c, 32:48] = wv
        part = part + mt(
            jnp.concatenate([q1, q2, wv, y0, y1c], axis=0), jnp.concatenate([q1, q2, wv, q2, wv, wv, y1c, y1c], axis=0)
        )
    packed = jnp.where(lane < 48, part[0:16], part[16:32])
    packed = jnp.where(lane < 80, packed, part[32:48])
    packed = jnp.where(lane < 96, packed, part[48:64])
    ga2[n] = jnp.where(lane < 112, packed, part[64:80])
    narrow_send(1, ga2)

    def forward2():
        narrow_recv(1, ga2)
        gb2[w] = all_of(ga2, NN)
        wide_send(1, gb2)

    product(3, xg2, pz, nothing, forward2, nothing, True)
    for q in range(OWN):
        row_copy(3, xr.at[OWN], xr, q, False).wait_recv()
    part = jnp.zeros((S, S), F32)
    for c in range(3):
        part = part + mt(
            jnp.concatenate([xr[b, c] for b in range(NN)], axis=1), jnp.concatenate([pz[b, c] for b in range(NN)], axis=1)
        )
    za[n, :, 0:16] = part
    narrow_send(2, za)

    narrow_recv(2, za)
    zb[w] = all_of(za, NN)
    wide_send(2, zb)

    wide_recv(1, gb2)
    total = all_of(gb2, NW)
    c11, c12, ha, c22, hb, k, g12, g22 = [total[:, 16 * i : 16 * i + 16] for i in range(8)]
    p20, p21 = transposed(p20t), transposed(p21t)
    c12t = transposed(c12)
    fa = ha + (ha - mm(c11, ha) - mm(c12, hb))
    fb = hb + (hb - mm(c12t, ha) - mm(c22, hb))
    fat, fbt = transposed(fa), transposed(fb)
    hat, hbt = transposed(ha), transposed(hb)
    fh = mm(fat, ha) + mm(fbt, hb)
    cf = mm(fat, mm(c11, fa) + mm(c12, fb)) + mm(fbt, mm(c12t, fa) + mm(c22, fb))
    upper2, inv2 = cholesky_pair(k - fh - transposed(fh) + cf)
    zz = mm(p20t, mm(g12, p20) + mm(g22, p21)) + mm(p21t, mm(g22, p20))
    wmq1 = mm(hat, f1) + mm(hbt, upper1)
    side = mm(wmq1, fa) + mm(k, fb)
    inner = zz - side - transposed(side) + mm(fat, mm(h1, fa) + mm(ha, fb)) + mm(fbt, mm(hat, fa) + mm(hb, fb))
    a3 = mt(mm(inv2, inner), inv2)

    def sym(value):
        return 0.5 * (value + transposed(value))

    order = 3 * S
    tri = jnp.zeros((order, order), F32)
    low = [
        (lax.broadcasted_iota(jnp.int32, (order, S), 0) == lax.broadcasted_iota(jnp.int32, (order, S), 1) + S * i).astype(F32)
        for i in range(3)
    ]
    blocks = [(0, 0, sym(h1)), (1, 1, sym(hb)), (2, 2, sym(a3)), (1, 0, upper1), (2, 1, upper2)]
    blocks += [(0, 1, transposed(upper1)), (1, 2, transposed(upper2))]
    for i, j, block in blocks:
        tri = tri + mt(mm(low[i], block), low[j])
    tri_ref[...] = tri
    mix_ref[...] = mm(low[2], mm(inv2, p21t))
    low_ref[...] = transposed(upper0)
    for c in range(3):
        q1, q2, wv = vec_ref[c, 0:16], vec_ref[c, 16:32], vec_ref[c, 32:48]
        vec_ref[c, 32:48] = mm(inv2, wv - mm(fat, q1) - mm(fbt, q2))
    wide_recv(2, zb)
    ztot_ref[...] = all_of(zb, NW)

    for phase, buffer in enumerate([cpos, xg0, xg1, xg2]):
        for p in (HALF[1:] if phase == 3 else range(1, NW)):
            block_copy(phase, buffer, p).wait_send()
    for phase, buffer in enumerate([gb1, gb2, zb]):
        wide_sent(phase, buffer)
    for phase, buffer in enumerate([ga1, ga2, za]):
        narrow_sent(phase, buffer)
    for q in range(OWN):
        row_copy(0, cpos.at[0], rpos, q, False).wait_send()
        row_copy(1, pb1.at[q], rb1, q, True).wait_send()
        row_copy(2, pb2.at[q], rb2, q, True).wait_send()
        row_copy(3, xr.at[OWN], xr, q, False).wait_send()


def last_kernel(vec_ref, tri_ref, mix_ref, low_ref, ztot_ref, out_ref, y_ref, z_ref):
    zraw = ztot_ref[:, 0:16]
    mix = mix_ref[...]
    tri = tri_ref[...] + mt(mm(mix, 0.5 * (zraw + transposed(zraw))), mix)
    order = 3 * S
    scale = jnp.sqrt(jnp.sum(tri * tri))
    ident = eye(order)
    y_ref[...] = tri / scale
    z_ref[...] = ident

    def more(carry):
        step, gap = carry
        return jnp.logical_and(step < ROOT_STEPS, jnp.logical_not(gap < 1e-8))

    def newton(carry):
        step, _ = carry
        y, z = y_ref[...], z_ref[...]
        zy = mm(z, y)
        factor = 1.5 * ident - 0.5 * zy
        y_ref[...] = mm(y, factor)
        z_ref[...] = mm(factor, z)
        off = zy - ident
        return step + 1, jnp.sum(off * off)

    lax.while_loop(more, newton, (jnp.int32(0), jnp.float32(1.0)))
    root = y_ref[...] * jnp.sqrt(scale)
    first = (
        lax.broadcasted_iota(jnp.int32, (S, order), 0) == lax.broadcasted_iota(jnp.int32, (S, order), 1)
    ).astype(F32)
    mixing = mm(low_ref[...], mt(first, root))
    for c in range(3):
        out_ref[c] = mm(mixing, vec_ref[c])


def per_device(positions, noise):
    block = (3, S, L)
    order = 3 * S
    vmem = pl.BlockSpec(memory_space=pltpu.VMEM)
    middle = pl.pallas_call(
        main_kernel,
        out_shape=[
            jax.ShapeDtypeStruct((3, order, L), F32),
            jax.ShapeDtypeStruct((order, order), F32),
            jax.ShapeDtypeStruct((order, S), F32),
            jax.ShapeDtypeStruct((S, S), F32),
            jax.ShapeDtypeStruct((S, L), F32),
        ],
        in_specs=[pl.BlockSpec(memory_space=pl.ANY)] * 2,
        out_specs=[vmem] * 5,
        scratch_shapes=[
            pltpu.VMEM((NW, 3, L), F32),
            pltpu.VMEM((NN, 3, L), F32),
            pltpu.VMEM((NW, *block), F32),
            pltpu.VMEM((NW, *block), F32),
            pltpu.VMEM((NW, *block), F32),
            pltpu.VMEM((NN, *block), F32),
            pltpu.VMEM((NN, *block), F32),
            pltpu.VMEM((NN, *block), F32),
            pltpu.VMEM((NN, *block), F32),
            pltpu.VMEM((NN, *block), F32),
            pltpu.VMEM((NN, *block), F32),
            pltpu.VMEM((4, NN, NW * L, L), BF16),
            pltpu.VMEM((4, NN, NW * L, L), BF16),
            pltpu.VMEM((2, 4, L, NW * L // 2), BF16),
            pltpu.VMEM((NN, 64, L), F32),
            pltpu.VMEM((4, 3, L, L), F32),
            pltpu.VMEM((NN, S, L), F32),
            pltpu.VMEM((NW, S, L), F32),
            pltpu.VMEM((NN, S, L), F32),
            pltpu.VMEM((NW, S, L), F32),
            pltpu.VMEM((NN, S, L), F32),
            pltpu.VMEM((NW, S, L), F32),
            pltpu.SemaphoreType.DMA((4, NW)),
            pltpu.SemaphoreType.DMA((4, NW)),
            pltpu.SemaphoreType.DMA((3, NW)),
            pltpu.SemaphoreType.DMA((3, NW)),
            pltpu.SemaphoreType.DMA((3, NN)),
            pltpu.SemaphoreType.DMA((3, NN)),
            pltpu.SemaphoreType.DMA((4, NN)),
            pltpu.SemaphoreType.DMA((4, NN)),
            pltpu.SemaphoreType.DMA((2,)),
        ],
        compiler_params=pltpu.CompilerParams(
            collective_id=0, has_side_effects=True, vmem_limit_bytes=56 * 1024 * 1024
        ),
        name="lanczos",
    )(positions, noise)
    return pl.pallas_call(
        last_kernel,
        out_shape=jax.ShapeDtypeStruct(block, F32),
        in_specs=[vmem] * 5,
        out_specs=vmem,
        scratch_shapes=[pltpu.VMEM((order, order), F32), pltpu.VMEM((order, order), F32)],
        name="finish",
    )(*middle)


def solution(mesh):
    axes = ("wide", "narrow")
    return jax.shard_map(
        per_device,
        mesh=mesh,
        in_specs=(P(None, axes), P(None, None, axes)),
        out_specs=P(None, None, axes),
        check_vma=False,
    )
```

```python
import functools

import jax
import jax.numpy as jnp
from jax import lax
from jax.experimental import pallas as pl
from jax.experimental.pallas import tpu as pltpu
from jax.sharding import PartitionSpec as P

ROOT_STEPS = 30
NW = 16
NN = 8
S = 16
L = 128
CENTRE = 34.0
MESH = pl.DeviceIdType.MESH
HI = lax.Precision.HIGHEST
F32 = jnp.float32
BF16 = jnp.bfloat16


def mm(a, b):
    return lax.dot_general(a, b, (((1,), (0,)), ((), ())), precision=HI, preferred_element_type=F32)


def mt(a, b):
    return lax.dot_general(a, b, (((1,), (1,)), ((), ())), precision=HI, preferred_element_type=F32)


def eye(n):
    return (lax.broadcasted_iota(jnp.int32, (n, n), 0) == lax.broadcasted_iota(jnp.int32, (n, n), 1)).astype(F32)


def transposed(a):
    return mt(eye(a.shape[1]), a)


def cholesky_pair(gram):
    n = gram.shape[0]
    rows = lax.broadcasted_iota(jnp.int32, (n, n), 0)
    cols = lax.broadcasted_iota(jnp.int32, (n, n), 1)
    left, right = gram, eye(n)
    upper, inverse = jnp.zeros((n, n), F32), jnp.zeros((n, n), F32)
    for c in range(n):
        scale = lax.rsqrt(jnp.broadcast_to(left[c : c + 1, c : c + 1], (1, n)))
        row = left[c : c + 1, :] * scale
        other = right[c : c + 1, :] * scale
        upper = jnp.where((rows == c) & (cols >= c), jnp.broadcast_to(row, (n, n)), upper)
        inverse = jnp.where((rows == c) & (cols <= c), jnp.broadcast_to(other, (n, n)), inverse)
        if c + 1 < n:
            factor = jnp.broadcast_to(left[:, c : c + 1], (n, n)) * scale
            left = left - factor * row
            right = right - jnp.where(rows > c, factor * other, 0.0)
    return upper, inverse


def split(value):
    high = value.astype(BF16)
    low = (value - high.astype(F32)).astype(BF16)
    return high, low


OFFSETS = [(0, 0), (2, 0), (1, 0), (0, 1), (3, 0), (0, 3), (1, 1), (0, 2)]
OFFSETS += [(1, 3), (2, 1), (1, 2), (2, 2), (3, 3), (3, 1), (2, 3), (3, 2)]
HALF = (0, 1, 2, 3, 6, 7, 8, 9, 10, 11)
SELF = (0, 1, 7, 11)
OWN = NN - 1


def row_place(q):
    g, side = q // 2, q % 2
    return (2 + g * (g + 1) // 2) % 4, (side + g // 3) % 2


def main_kernel(
    pos_hbm,
    noise_hbm,
    vec_ref,
    tri_ref,
    mix_ref,
    low_ref,
    ztot_ref,
    cpos,
    rpos,
    xg0,
    xg1,
    xg2,
    xr,
    pb1,
    pb2,
    rb1,
    rb2,
    pz,
    lhi,
    llo,
    rmat,
    acc,
    xjb,
    ga1,
    gb1,
    ga2,
    gb2,
    za,
    zb,
    send_b,
    recv_b,
    send_w,
    recv_w,
    send_n,
    recv_n,
    send_q,
    recv_q,
    load_sem,
):
    w = lax.axis_index("wide")
    n = lax.axis_index("narrow")

    def loop(begin, end, body):
        def step(i, carry):
            body(i)
            return carry

        lax.fori_loop(begin, end, step, 0)

    def block_copy(phase, buffer, p):
        a, b = OFFSETS[p]
        x = lax.rem(w // 4 + 4 - a, 4)
        z = lax.rem(lax.rem(w, 4) + 4 - b, 4)
        return pltpu.make_async_remote_copy(
            src_ref=buffer.at[0],
            dst_ref=buffer.at[p],
            send_sem=send_b.at[phase, p],
            recv_sem=recv_b.at[phase, p],
            device_id={"wide": x * 4 + z},
            device_id_type=MESH,
        )

    def block_send(phase, buffer, slots=range(NW)):
        for p in slots[1:]:
            block_copy(phase, buffer, p).start()

    def block_arrived(phase, buffer, p):
        pltpu.make_async_remote_copy(
            src_ref=buffer.at[0],
            dst_ref=buffer.at[p],
            send_sem=send_b.at[phase, p],
            recv_sem=recv_b.at[phase, p],
            device_id={"wide": w},
            device_id_type=MESH,
        ).wait_recv()

    def wide_copy(phase, src, dst, target, slot):
        return pltpu.make_async_remote_copy(
            src_ref=src,
            dst_ref=dst.at[slot],
            send_sem=send_w.at[phase, target],
            recv_sem=recv_w.at[phase, slot],
            device_id={"wide": target},
            device_id_type=MESH,
        )

    def narrow_copy(phase, src, dst, target, slot):
        return pltpu.make_async_remote_copy(
            src_ref=src,
            dst_ref=dst.at[slot],
            send_sem=send_n.at[phase, target],
            recv_sem=recv_n.at[phase, slot],
            device_id={"narrow": target},
            device_id_type=MESH,
        )

    def row_copy(phase, src, dst, q, away):
        a, b = row_place(q)
        y = lax.rem(n // 2 + (a if away else 4 - a), 4)
        core = lax.rem(lax.rem(n, 2) + b, 2)
        return pltpu.make_async_remote_copy(
            src_ref=src,
            dst_ref=dst.at[q],
            send_sem=send_q.at[phase, q],
            recv_sem=recv_q.at[phase, q],
            device_id={"narrow": y * 2 + core},
            device_id_type=MESH,
        )

    def wide_send(phase, dst):
        loop(1, NW, lambda p: wide_copy(phase, dst.at[w], dst, lax.rem(w + p, NW), w).start())

    def wide_recv(phase, dst):
        def one(p):
            s = lax.rem(w + p, NW)
            wide_copy(phase, dst.at[s], dst, s, s).wait_recv()

        loop(1, NW, one)

    def wide_sent(phase, dst):
        def one(p):
            s = lax.rem(w + p, NW)
            wide_copy(phase, dst.at[w], dst, s, w).wait_send()

        loop(1, NW, one)

    def narrow_send(phase, dst):
        loop(1, NN, lambda p: narrow_copy(phase, dst.at[n], dst, lax.rem(n + p, NN), n).start())

    def narrow_recv(phase, dst):
        def one(p):
            s = lax.rem(n + p, NN)
            narrow_copy(phase, dst.at[s], dst, s, s).wait_recv()

        loop(1, NN, one)

    def narrow_sent(phase, dst):
        def one(p):
            s = lax.rem(n + p, NN)
            narrow_copy(phase, dst.at[n], dst, s, n).wait_send()

        loop(1, NN, one)

    def all_of(buffer, count):
        parts = [buffer[i] for i in range(count)]
        while len(parts) > 1:
            parts = [parts[i] + parts[i + 1] for i in range(0, len(parts), 2)]
        return parts[0]

    barrier = pltpu.get_barrier_semaphore()

    def greet_wide(p):
        along_x = lax.rem(w // 4 + p, 4) * 4 + lax.rem(w, 4)
        along_z = w // 4 * 4 + lax.rem(lax.rem(w, 4) + p, 4)
        pl.semaphore_signal(barrier, inc=1, device_id={"wide": along_x}, device_id_type=MESH)
        pl.semaphore_signal(barrier, inc=1, device_id={"wide": along_z}, device_id_type=MESH)

    def greet_narrow(p):
        pl.semaphore_signal(barrier, inc=1, device_id={"narrow": lax.rem(n + p, NN)}, device_id_type=MESH)

    loop(1, 4, greet_wide)
    loop(1, NN, greet_narrow)
    loads = [
        pltpu.make_async_copy(pos_hbm, cpos.at[0], load_sem.at[0]),
        pltpu.make_async_copy(noise_hbm, xg0.at[0], load_sem.at[1]),
    ]
    for load in loads:
        load.start()
    za[n] = jnp.zeros((S, L), F32)
    for load in loads:
        load.wait()
    rpos[OWN] = cpos[0]
    pl.semaphore_wait(barrier, 6 + NN - 1)

    for q in range(OWN):
        row_copy(0, cpos.at[0], rpos, q, False).start()
    for a in range(1, 4):
        block_copy(0, cpos, OFFSETS.index((a, 0))).start()
        block_copy(0, cpos, OFFSETS.index((0, a))).start()
    for a in range(1, 4):
        held = OFFSETS.index((a, 0))
        block_arrived(0, cpos, held)
        for b in range(1, 4):
            slot = OFFSETS.index((a, b))
            pltpu.make_async_remote_copy(
                src_ref=cpos.at[held],
                dst_ref=cpos.at[slot],
                send_sem=send_b.at[0, slot],
                recv_sem=recv_b.at[0, slot],
                device_id={"wide": w // 4 * 4 + lax.rem(lax.rem(w, 4) + 4 - b, 4)},
                device_id_type=MESH,
            ).start()
    for a in range(1, 4):
        block_arrived(0, cpos, OFFSETS.index((0, a)))
    for q in range(OWN):
        row_copy(0, cpos.at[0], rpos, q, False).wait_recv()

    def build(group):
        for i in range(4):
            columns = jnp.concatenate([cpos[group * 4 + i], jnp.zeros((5, L), F32)], axis=0).T
            for c in range(3):
                xjb[i, c] = jnp.broadcast_to(columns[:, c : c + 1], (L, L))

        def one(step):
            i = step // 4
            for half in range(2):
                ib = lax.rem(step, 4) * 2 + half
                xi = [jnp.broadcast_to(rpos[ib, c : c + 1, :], (16, L)) for c in range(3)]
                for jt in range(8):
                    d = [xi[c] - xjb[i, c, jt * 16 : jt * 16 + 16, :] for c in range(3)]
                    sq = jnp.maximum(d[0] * d[0] + d[1] * d[1] + d[2] * d[2], 1e-20)
                    inv = lax.rsqrt(sq)
                    inv2 = inv * inv
                    near = sq < 4.0
                    iso = jnp.where(near, 1.0 - 0.28125 * (sq * inv), inv * (0.75 + 0.5 * inv2))
                    outer = inv * jnp.where(near, 0.09375, inv2 * (0.75 - 1.5 * inv2))
                    places = pl.ds(pl.multiple_of((group * 4 + i) * L + jt * 16, 16), 16)
                    for k, value in enumerate([outer * d[0], outer * d[1], outer * d[2], iso]):
                        high, low = split(value)
                        lhi[k, ib, places, :] = high
                        llo[k, ib, places, :] = low

        loop(0, 16, one)

    build(0)
    for a in range(1, 4):
        for b in range(1, 4):
            block_arrived(0, cpos, OFFSETS.index((a, b)))
    block_send(1, xg0)
    loop(1, 4, build)

    half_blocks = NW // 2
    depth = half_blocks * L

    def product(phase, xg, out, early, between, emit, symmetric=False):
        def expand(p, factor=None):
            lanes = pl.ds(pl.multiple_of(lax.rem(p, half_blocks) * L, L), L)
            half = p // half_blocks
            x = [cpos[p, c : c + 1, :] - CENTRE for c in range(3)]
            v = [xg[p, e] if factor is None else factor * xg[p, e] for e in range(3)]
            pieces = [jnp.concatenate([v[e], x[0] * v[e], x[1] * v[e], x[2] * v[e]], axis=0) for e in range(3)]
            pieces.append(jnp.concatenate([jnp.zeros((S, L), F32), -v[0], -v[1], -v[2]], axis=0))
            for k in range(4):
                high, low = split(pieces[k])
                rmat[half, k, 0:64, lanes] = high
                rmat[half, k, 64:128, lanes] = low

        def arrived_expand(p):
            block_arrived(phase, xg, p)
            expand(p)

        def arrived_double(p):
            block_arrived(phase, xg, p)
            expand(p, 2.0)

        def pair_of(half, q, count=2):
            if symmetric:
                spans = [[(0, 4), (6, 8)], [(0, 4)]][half]
            else:
                spans = [(0, half_blocks)]
            total, small = None, None
            for k, (begin, end) in [(k, span) for k in range(4) for span in spans]:
                rows = slice(half * depth + begin * L, half * depth + end * L)
                places = slice(begin * L, end * L)
                high = jnp.concatenate([lhi[k, q + i, rows, :] for i in range(count)], axis=1)
                low = jnp.concatenate([llo[k, q + i, rows, :] for i in range(count)], axis=1)
                one = jnp.dot(rmat[half, k, :, places], high, preferred_element_type=F32)
                two = jnp.dot(rmat[half, k, 0:64, places], low, preferred_element_type=F32)
                total = one if total is None else total + one
                small = two if small is None else small + two
            return total[0:64] + (total[64:128] + small)

        expand(0)
        def arrivals(half):
            begin, end = max(1, half * half_blocks), (half + 1) * half_blocks
            if not symmetric:
                loop(begin, end, arrived_expand)
                return
            for p in HALF:
                if begin <= p < end:
                    (arrived_expand if p in SELF else arrived_double)(p)

        arrivals(0)

        def first(g):
            value = pair_of(0, g * 4, 4)
            for side in range(4):
                acc[g * 4 + side] = value[:, side * L : side * L + L]

        def turn(g):
            first(g)

            @pl.when(g == 0)
            def _():
                early()

        loop(0, NN // 4, turn)
        between()
        arrivals(1)

        wide = 4 if symmetric else 2

        def second(g):
            value = pair_of(1, g * wide, wide)
            for side in range(wide):
                q = g * wide + side
                total = acc[q] + value[:, side * L : side * L + L]
                for c in range(3):
                    out[q, c] = (rpos[q, pl.ds(c, 1), :] - CENTRE) * total[0:16] - total[16 + 16 * c : 32 + 16 * c]
            for side in range(0, wide, 2):
                emit(g * wide + side)

        loop(0, NN // wide, second)

    def nothing(*_):
        return None

    def scatter(phase, parts, sums):
        def emit(q):
            row_copy(phase, parts.at[q], sums, q, True).start()

            @pl.when(q + 1 < OWN)
            def _():
                row_copy(phase, parts.at[q + 1], sums, q + 1, True).start()

        return emit

    def summed(phase, parts, sums):
        for q in range(OWN):
            row_copy(phase, parts.at[q], sums, q, True).wait_recv()
        return ((sums[0] + sums[1]) + (sums[2] + sums[3])) + ((sums[4] + sums[5]) + (sums[6] + parts[OWN]))

    lane = lax.broadcasted_iota(jnp.int32, (S, L), 1)

    product(1, xg0, pb1, nothing, nothing, scatter(1, pb1, rb1))
    xg1[0] = summed(1, pb1, rb1)
    block_send(2, xg1)

    part = jnp.zeros((2 * S, L), F32)
    for c in range(3):
        a, b = xg0[0, c], xg1[0, c]
        part = part + mt(jnp.concatenate([a, b], axis=0), jnp.concatenate([a, b, b, b, b, b, b, b], axis=0))
    ga1[n] = jnp.where(lane < 32, part[0:16], part[16:32])
    narrow_send(0, ga1)

    def forward1():
        narrow_recv(0, ga1)
        gb1[w] = all_of(ga1, NN)
        wide_send(0, gb1)

    product(2, xg1, pb2, forward1, nothing, scatter(2, pb2, rb2))

    wide_recv(0, gb1)
    total = all_of(gb1, NW)
    g00, g01, g11 = total[:, 0:16], total[:, 16:32], total[:, 32:48]
    upper0, inv0 = cholesky_pair(g00)

    def inside(g):
        return mt(mm(inv0, g), inv0)

    h1, c11, k1 = inside(g01), inside(g00), inside(g11)
    f1 = h1 + (h1 - mm(c11, h1))
    f1t = transposed(f1)
    fh = mm(f1t, h1)
    gram = k1 - fh - transposed(fh) + mm(f1t, mm(c11, f1))
    y1 = summed(2, pb2, rb2)
    xg2[0] = y1
    block_send(3, xg2, HALF)
    xr[OWN] = y1
    for q in range(OWN):
        row_copy(3, xr.at[OWN], xr, q, False).start()

    upper1, inv1 = cholesky_pair(gram)
    p21t = mm(inv1, inv0)
    p20t = -mm(mm(inv1, f1t), inv0)
    for c in range(3):
        a, y0 = xg0[0, c], xg1[0, c]
        vec_ref[c, 0:16] = mm(inv0, a)
        vec_ref[c, 16:32] = mm(p20t, a) + mm(p21t, y0)
        vec_ref[c, 32:48] = mm(p20t, y0)

    part = jnp.zeros((5 * S, L), F32)
    for c in range(3):
        y0, y1c = xg1[0, c], xg2[0, c]
        q1, q2 = vec_ref[c, 0:16], vec_ref[c, 16:32]
        wv = vec_ref[c, 32:48] + mm(p21t, y1c)
        vec_ref[c, 32:48] = wv
        part = part + mt(
            jnp.concatenate([q1, q2, wv, y0, y1c], axis=0), jnp.concatenate([q1, q2, wv, q2, wv, wv, y1c, y1c], axis=0)
        )
    packed = jnp.where(lane < 48, part[0:16], part[16:32])
    packed = jnp.where(lane < 80, packed, part[32:48])
    packed = jnp.where(lane < 96, packed, part[48:64])
    ga2[n] = jnp.where(lane < 112, packed, part[64:80])
    narrow_send(1, ga2)

    def forward2():
        narrow_recv(1, ga2)
        gb2[w] = all_of(ga2, NN)
        wide_send(1, gb2)

    product(3, xg2, pz, nothing, forward2, nothing, True)
    for q in range(OWN):
        row_copy(3, xr.at[OWN], xr, q, False).wait_recv()
    part = jnp.zeros((S, S), F32)
    for c in range(3):
        part = part + mt(
            jnp.concatenate([xr[b, c] for b in range(NN)], axis=1), jnp.concatenate([pz[b, c] for b in range(NN)], axis=1)
        )
    za[n, :, 0:16] = part
    narrow_send(2, za)

    narrow_recv(2, za)
    zb[w] = all_of(za, NN)
    wide_send(2, zb)

    wide_recv(1, gb2)
    total = all_of(gb2, NW)
    c11, c12, ha, c22, hb, k, g12, g22 = [total[:, 16 * i : 16 * i + 16] for i in range(8)]
    p20, p21 = transposed(p20t), transposed(p21t)
    c12t = transposed(c12)
    fa = ha + (ha - mm(c11, ha) - mm(c12, hb))
    fb = hb + (hb - mm(c12t, ha) - mm(c22, hb))
    fat, fbt = transposed(fa), transposed(fb)
    hat, hbt = transposed(ha), transposed(hb)
    fh = mm(fat, ha) + mm(fbt, hb)
    cf = mm(fat, mm(c11, fa) + mm(c12, fb)) + mm(fbt, mm(c12t, fa) + mm(c22, fb))
    upper2, inv2 = cholesky_pair(k - fh - transposed(fh) + cf)
    zz = mm(p20t, mm(g12, p20) + mm(g22, p21)) + mm(p21t, mm(g22, p20))
    wmq1 = mm(hat, f1) + mm(hbt, upper1)
    side = mm(wmq1, fa) + mm(k, fb)
    inner = zz - side - transposed(side) + mm(fat, mm(h1, fa) + mm(ha, fb)) + mm(fbt, mm(hat, fa) + mm(hb, fb))
    a3 = mt(mm(inv2, inner), inv2)

    def sym(value):
        return 0.5 * (value + transposed(value))

    order = 3 * S
    tri = jnp.zeros((order, order), F32)
    low = [
        (lax.broadcasted_iota(jnp.int32, (order, S), 0) == lax.broadcasted_iota(jnp.int32, (order, S), 1) + S * i).astype(F32)
        for i in range(3)
    ]
    blocks = [(0, 0, sym(h1)), (1, 1, sym(hb)), (2, 2, sym(a3)), (1, 0, upper1), (2, 1, upper2)]
    blocks += [(0, 1, transposed(upper1)), (1, 2, transposed(upper2))]
    for i, j, block in blocks:
        tri = tri + mt(mm(low[i], block), low[j])
    tri_ref[...] = tri
    mix_ref[...] = mm(low[2], mm(inv2, p21t))
    low_ref[...] = transposed(upper0)
    for c in range(3):
        q1, q2, wv = vec_ref[c, 0:16], vec_ref[c, 16:32], vec_ref[c, 32:48]
        vec_ref[c, 32:48] = mm(inv2, wv - mm(fat, q1) - mm(fbt, q2))
    wide_recv(2, zb)
    ztot_ref[...] = all_of(zb, NW)

    for phase, buffer in enumerate([cpos, xg0, xg1, xg2]):
        for p in (HALF[1:] if phase == 3 else range(1, NW)):
            block_copy(phase, buffer, p).wait_send()
    for phase, buffer in enumerate([gb1, gb2, zb]):
        wide_sent(phase, buffer)
    for phase, buffer in enumerate([ga1, ga2, za]):
        narrow_sent(phase, buffer)
    for q in range(OWN):
        row_copy(0, cpos.at[0], rpos, q, False).wait_send()
        row_copy(1, pb1.at[q], rb1, q, True).wait_send()
        row_copy(2, pb2.at[q], rb2, q, True).wait_send()
        row_copy(3, xr.at[OWN], xr, q, False).wait_send()


def last_kernel(vec_ref, tri_ref, mix_ref, low_ref, ztot_ref, out_ref, y_ref, z_ref):
    zraw = ztot_ref[:, 0:16]
    mix = mix_ref[...]
    tri = tri_ref[...] + mt(mm(mix, 0.5 * (zraw + transposed(zraw))), mix)
    order = 3 * S
    scale = jnp.sqrt(jnp.sum(tri * tri))
    ident = eye(order)
    y_ref[...] = tri / scale
    z_ref[...] = ident

    def more(carry):
        step, gap = carry
        return jnp.logical_and(step < ROOT_STEPS, jnp.logical_not(gap < 1e-8))

    def newton(carry):
        step, _ = carry
        y, z = y_ref[...], z_ref[...]
        zy = mm(z, y)
        factor = 1.5 * ident - 0.5 * zy
        y_ref[...] = mm(y, factor)
        z_ref[...] = mm(factor, z)
        off = zy - ident
        return step + 1, jnp.sum(off * off)

    lax.while_loop(more, newton, (jnp.int32(0), jnp.float32(1.0)))
    root = y_ref[...] * jnp.sqrt(scale)
    first = (
        lax.broadcasted_iota(jnp.int32, (S, order), 0) == lax.broadcasted_iota(jnp.int32, (S, order), 1)
    ).astype(F32)
    mixing = mm(low_ref[...], mt(first, root))
    for c in range(3):
        out_ref[c] = mm(mixing, vec_ref[c])


def per_device(positions, noise):
    block = (3, S, L)
    order = 3 * S
    vmem = pl.BlockSpec(memory_space=pltpu.VMEM)
    middle = pl.pallas_call(
        main_kernel,
        out_shape=[
            jax.ShapeDtypeStruct((3, order, L), F32),
            jax.ShapeDtypeStruct((order, order), F32),
            jax.ShapeDtypeStruct((order, S), F32),
            jax.ShapeDtypeStruct((S, S), F32),
            jax.ShapeDtypeStruct((S, L), F32),
        ],
        in_specs=[pl.BlockSpec(memory_space=pl.ANY)] * 2,
        out_specs=[vmem] * 5,
        scratch_shapes=[
            pltpu.VMEM((NW, 3, L), F32),
            pltpu.VMEM((NN, 3, L), F32),
            pltpu.VMEM((NW, *block), F32),
            pltpu.VMEM((NW, *block), F32),
            pltpu.VMEM((NW, *block), F32),
            pltpu.VMEM((NN, *block), F32),
            pltpu.VMEM((NN, *block), F32),
            pltpu.VMEM((NN, *block), F32),
            pltpu.VMEM((NN, *block), F32),
            pltpu.VMEM((NN, *block), F32),
            pltpu.VMEM((NN, *block), F32),
            pltpu.VMEM((4, NN, NW * L, L), BF16),
            pltpu.VMEM((4, NN, NW * L, L), BF16),
            pltpu.VMEM((2, 4, L, NW * L // 2), BF16),
            pltpu.VMEM((NN, 64, L), F32),
            pltpu.VMEM((4, 3, L, L), F32),
            pltpu.VMEM((NN, S, L), F32),
            pltpu.VMEM((NW, S, L), F32),
            pltpu.VMEM((NN, S, L), F32),
            pltpu.VMEM((NW, S, L), F32),
            pltpu.VMEM((NN, S, L), F32),
            pltpu.VMEM((NW, S, L), F32),
            pltpu.SemaphoreType.DMA((4, NW)),
            pltpu.SemaphoreType.DMA((4, NW)),
            pltpu.SemaphoreType.DMA((3, NW)),
            pltpu.SemaphoreType.DMA((3, NW)),
            pltpu.SemaphoreType.DMA((3, NN)),
            pltpu.SemaphoreType.DMA((3, NN)),
            pltpu.SemaphoreType.DMA((4, NN)),
            pltpu.SemaphoreType.DMA((4, NN)),
            pltpu.SemaphoreType.DMA((2,)),
        ],
        compiler_params=pltpu.CompilerParams(
            collective_id=0, has_side_effects=True, vmem_limit_bytes=56 * 1024 * 1024
        ),
        name="lanczos",
    )(positions, noise)
    return pl.pallas_call(
        last_kernel,
        out_shape=jax.ShapeDtypeStruct(block, F32),
        in_specs=[vmem] * 5,
        out_specs=vmem,
        scratch_shapes=[pltpu.VMEM((order, order), F32), pltpu.VMEM((order, order), F32)],
        name="finish",
    )(*middle)


def solution(mesh):
    axes = ("wide", "narrow")
    return jax.shard_map(
        per_device,
        mesh=mesh,
        in_specs=(P(None, axes), P(None, None, axes)),
        out_specs=P(None, None, axes),
        check_vma=False,
    )
```

```python
import functools

import jax
import jax.numpy as jnp
from jax import lax
from jax.experimental import pallas as pl
from jax.experimental.pallas import tpu as pltpu
from jax.sharding import PartitionSpec as P

ROOT_STEPS = 30
NW = 16
NN = 8
S = 16
L = 128
CENTRE = 34.0
MESH = pl.DeviceIdType.MESH
HI = lax.Precision.HIGHEST
F32 = jnp.float32
BF16 = jnp.bfloat16


def mm(a, b):
    return lax.dot_general(a, b, (((1,), (0,)), ((), ())), precision=HI, preferred_element_type=F32)


def mt(a, b):
    return lax.dot_general(a, b, (((1,), (1,)), ((), ())), precision=HI, preferred_element_type=F32)


def eye(n):
    return (lax.broadcasted_iota(jnp.int32, (n, n), 0) == lax.broadcasted_iota(jnp.int32, (n, n), 1)).astype(F32)


def transposed(a):
    return mt(eye(a.shape[1]), a)


def cholesky_pair(gram):
    n = gram.shape[0]
    rows = lax.broadcasted_iota(jnp.int32, (n, n), 0)
    cols = lax.broadcasted_iota(jnp.int32, (n, n), 1)
    left, right = gram, eye(n)
    upper, inverse = jnp.zeros((n, n), F32), jnp.zeros((n, n), F32)
    for c in range(n):
        scale = lax.rsqrt(jnp.broadcast_to(left[c : c + 1, c : c + 1], (1, n)))
        row = left[c : c + 1, :] * scale
        other = right[c : c + 1, :] * scale
        upper = jnp.where((rows == c) & (cols >= c), jnp.broadcast_to(row, (n, n)), upper)
        inverse = jnp.where((rows == c) & (cols <= c), jnp.broadcast_to(other, (n, n)), inverse)
        if c + 1 < n:
            factor = jnp.broadcast_to(left[:, c : c + 1], (n, n)) * scale
            left = left - factor * row
            right = right - jnp.where(rows > c, factor * other, 0.0)
    return upper, inverse


def split(value):
    high = value.astype(BF16)
    low = (value - high.astype(F32)).astype(BF16)
    return high, low


OFFSETS = [(0, 0), (2, 0), (1, 0), (0, 1), (3, 0), (0, 3), (1, 1), (0, 2)]
OFFSETS += [(1, 3), (2, 1), (1, 2), (2, 2), (3, 3), (3, 1), (2, 3), (3, 2)]
HALF = (0, 1, 2, 3, 6, 7, 8, 9, 10, 11)
SELF = (0, 1, 7, 11)
OWN = NN - 1


def row_place(q):
    g, side = q // 2, q % 2
    return (2 + g * (g + 1) // 2) % 4, (side + g // 3) % 2


def main_kernel(
    pos_hbm,
    noise_hbm,
    vec_ref,
    tri_ref,
    mix_ref,
    low_ref,
    ztot_ref,
    cpos,
    rpos,
    xg0,
    xg1,
    xg2,
    xr,
    pb1,
    pb2,
    rb1,
    rb2,
    pz,
    lhi,
    llo,
    rmat,
    acc,
    xjb,
    ga1,
    gb1,
    ga2,
    gb2,
    za,
    zb,
    send_b,
    recv_b,
    send_w,
    recv_w,
    send_n,
    recv_n,
    send_q,
    recv_q,
    load_sem,
):
    w = lax.axis_index("wide")
    n = lax.axis_index("narrow")

    def loop(begin, end, body):
        def step(i, carry):
            body(i)
            return carry

        lax.fori_loop(begin, end, step, 0)

    def block_copy(phase, buffer, p):
        a, b = OFFSETS[p]
        x = lax.rem(w // 4 + 4 - a, 4)
        z = lax.rem(lax.rem(w, 4) + 4 - b, 4)
        return pltpu.make_async_remote_copy(
            src_ref=buffer.at[0],
            dst_ref=buffer.at[p],
            send_sem=send_b.at[phase, p],
            recv_sem=recv_b.at[phase, p],
            device_id={"wide": x * 4 + z},
            device_id_type=MESH,
        )

    def block_send(phase, buffer, slots=range(NW)):
        for p in slots[1:]:
            block_copy(phase, buffer, p).start()

    def block_arrived(phase, buffer, p):
        pltpu.make_async_remote_copy(
            src_ref=buffer.at[0],
            dst_ref=buffer.at[p],
            send_sem=send_b.at[phase, p],
            recv_sem=recv_b.at[phase, p],
            device_id={"wide": w},
            device_id_type=MESH,
        ).wait_recv()

    def wide_copy(phase, src, dst, target, slot):
        return pltpu.make_async_remote_copy(
            src_ref=src,
            dst_ref=dst.at[slot],
            send_sem=send_w.at[phase, target],
            recv_sem=recv_w.at[phase, slot],
            device_id={"wide": target},
            device_id_type=MESH,
        )

    def narrow_copy(phase, src, dst, target, slot):
        return pltpu.make_async_remote_copy(
            src_ref=src,
            dst_ref=dst.at[slot],
            send_sem=send_n.at[phase, target],
            recv_sem=recv_n.at[phase, slot],
            device_id={"narrow": target},
            device_id_type=MESH,
        )

    def row_copy(phase, src, dst, q, away):
        a, b = row_place(q)
        y = lax.rem(n // 2 + (a if away else 4 - a), 4)
        core = lax.rem(lax.rem(n, 2) + b, 2)
        return pltpu.make_async_remote_copy(
            src_ref=src,
            dst_ref=dst.at[q],
            send_sem=send_q.at[phase, q],
            recv_sem=recv_q.at[phase, q],
            device_id={"narrow": y * 2 + core},
            device_id_type=MESH,
        )

    def wide_send(phase, dst):
        loop(1, NW, lambda p: wide_copy(phase, dst.at[w], dst, lax.rem(w + p, NW), w).start())

    def wide_recv(phase, dst):
        def one(p):
            s = lax.rem(w + p, NW)
            wide_copy(phase, dst.at[s], dst, s, s).wait_recv()

        loop(1, NW, one)

    def wide_sent(phase, dst):
        def one(p):
            s = lax.rem(w + p, NW)
            wide_copy(phase, dst.at[w], dst, s, w).wait_send()

        loop(1, NW, one)

    def narrow_send(phase, dst):
        loop(1, NN, lambda p: narrow_copy(phase, dst.at[n], dst, lax.rem(n + p, NN), n).start())

    def narrow_recv(phase, dst):
        def one(p):
            s = lax.rem(n + p, NN)
            narrow_copy(phase, dst.at[s], dst, s, s).wait_recv()

        loop(1, NN, one)

    def narrow_sent(phase, dst):
        def one(p):
            s = lax.rem(n + p, NN)
            narrow_copy(phase, dst.at[n], dst, s, n).wait_send()

        loop(1, NN, one)

    def all_of(buffer, count):
        parts = [buffer[i] for i in range(count)]
        while len(parts) > 1:
            parts = [parts[i] + parts[i + 1] for i in range(0, len(parts), 2)]
        return parts[0]

    barrier = pltpu.get_barrier_semaphore()

    def greet_wide(p):
        along_x = lax.rem(w // 4 + p, 4) * 4 + lax.rem(w, 4)
        along_z = w // 4 * 4 + lax.rem(lax.rem(w, 4) + p, 4)
        pl.semaphore_signal(barrier, inc=1, device_id={"wide": along_x}, device_id_type=MESH)
        pl.semaphore_signal(barrier, inc=1, device_id={"wide": along_z}, device_id_type=MESH)

    def greet_narrow(p):
        pl.semaphore_signal(barrier, inc=1, device_id={"narrow": lax.rem(n + p, NN)}, device_id_type=MESH)

    loop(1, 4, greet_wide)
    loop(1, NN, greet_narrow)
    loads = [
        pltpu.make_async_copy(pos_hbm, cpos.at[0], load_sem.at[0]),
        pltpu.make_async_copy(noise_hbm, xg0.at[0], load_sem.at[1]),
    ]
    for load in loads:
        load.start()
    za[n] = jnp.zeros((S, L), F32)
    for load in loads:
        load.wait()
    rpos[OWN] = cpos[0]
    pl.semaphore_wait(barrier, 6 + NN - 1)

    for q in range(OWN):
        row_copy(0, cpos.at[0], rpos, q, False).start()
    for a in range(1, 4):
        block_copy(0, cpos, OFFSETS.index((a, 0))).start()
        block_copy(0, cpos, OFFSETS.index((0, a))).start()
    for a in range(1, 4):
        held = OFFSETS.index((a, 0))
        block_arrived(0, cpos, held)
        for b in range(1, 4):
            slot = OFFSETS.index((a, b))
            pltpu.make_async_remote_copy(
                src_ref=cpos.at[held],
                dst_ref=cpos.at[slot],
                send_sem=send_b.at[0, slot],
                recv_sem=recv_b.at[0, slot],
                device_id={"wide": w // 4 * 4 + lax.rem(lax.rem(w, 4) + 4 - b, 4)},
                device_id_type=MESH,
            ).start()
    for a in range(1, 4):
        block_arrived(0, cpos, OFFSETS.index((0, a)))
    for q in range(OWN):
        row_copy(0, cpos.at[0], rpos, q, False).wait_recv()

    def build(group):
        for i in range(4):
            columns = jnp.concatenate([cpos[group * 4 + i], jnp.zeros((5, L), F32)], axis=0).T
            for c in range(3):
                xjb[i, c] = jnp.broadcast_to(columns[:, c : c + 1], (L, L))

        def one(step):
            i = step // 4
            for half in range(2):
                ib = lax.rem(step, 4) * 2 + half
                xi = [jnp.broadcast_to(rpos[ib, c : c + 1, :], (16, L)) for c in range(3)]
                for jt in range(8):
                    d = [xi[c] - xjb[i, c, jt * 16 : jt * 16 + 16, :] for c in range(3)]
                    sq = jnp.maximum(d[0] * d[0] + d[1] * d[1] + d[2] * d[2], 1e-20)
                    inv = lax.rsqrt(sq)
                    inv2 = inv * inv
                    near = sq < 4.0
                    iso = jnp.where(near, 1.0 - 0.28125 * (sq * inv), inv * (0.75 + 0.5 * inv2))
                    outer = inv * jnp.where(near, 0.09375, inv2 * (0.75 - 1.5 * inv2))
                    places = pl.ds(pl.multiple_of((group * 4 + i) * L + jt * 16, 16), 16)
                    for k, value in enumerate([outer * d[0], outer * d[1], outer * d[2], iso]):
                        high, low = split(value)
                        lhi[k, ib, places, :] = high
                        llo[k, ib, places, :] = low

        loop(0, 16, one)

    build(0)
    for a in range(1, 4):
        for b in range(1, 4):
            block_arrived(0, cpos, OFFSETS.index((a, b)))
    block_send(1, xg0)
    loop(1, 4, build)

    half_blocks = NW // 2
    depth = half_blocks * L

    def product(phase, xg, out, early, between, emit, symmetric=False):
        def expand(p, factor=None):
            lanes = pl.ds(pl.multiple_of(lax.rem(p, half_blocks) * L, L), L)
            half = p // half_blocks
            x = [cpos[p, c : c + 1, :] - CENTRE for c in range(3)]
            v = [xg[p, e] if factor is None else factor * xg[p, e] for e in range(3)]
            pieces = [jnp.concatenate([v[e], x[0] * v[e], x[1] * v[e], x[2] * v[e]], axis=0) for e in range(3)]
            pieces.append(jnp.concatenate([jnp.zeros((S, L), F32), -v[0], -v[1], -v[2]], axis=0))
            for k in range(4):
                high, low = split(pieces[k])
                rmat[half, k, 0:64, lanes] = high
                rmat[half, k, 64:128, lanes] = low

        def arrived_expand(p):
            block_arrived(phase, xg, p)
            expand(p)

        def arrived_double(p):
            block_arrived(phase, xg, p)
            expand(p, 2.0)

        def pair_of(half, q, count=2):
            if symmetric:
                spans = [[(0, 4), (6, 8)], [(0, 4)]][half]
            else:
                spans = [(0, half_blocks)]
            total, small = None, None
            for k, (begin, end) in [(k, span) for k in range(4) for span in spans]:
                rows = slice(half * depth + begin * L, half * depth + end * L)
                places = slice(begin * L, end * L)
                high = jnp.concatenate([lhi[k, q + i, rows, :] for i in range(count)], axis=1)
                low = jnp.concatenate([llo[k, q + i, rows, :] for i in range(count)], axis=1)
                one = jnp.dot(rmat[half, k, :, places], high, preferred_element_type=F32)
                two = jnp.dot(rmat[half, k, 0:64, places], low, preferred_element_type=F32)
                total = one if total is None else total + one
                small = two if small is None else small + two
            return total[0:64] + (total[64:128] + small)

        expand(0)
        def arrivals(half):
            begin, end = max(1, half * half_blocks), (half + 1) * half_blocks
            if not symmetric:
                loop(begin, end, arrived_expand)
                return
            for p in HALF:
                if begin <= p < end:
                    (arrived_expand if p in SELF else arrived_double)(p)

        arrivals(0)

        def first(g):
            value = pair_of(0, g * 4, 4)
            for side in range(4):
                acc[g * 4 + side] = value[:, side * L : side * L + L]

        def turn(g):
            first(g)

            @pl.when(g == 0)
            def _():
                early()

        loop(0, NN // 4, turn)
        between()
        arrivals(1)

        wide = 4 if symmetric else 2

        def second(g):
            value = pair_of(1, g * wide, wide)
            for side in range(wide):
                q = g * wide + side
                total = acc[q] + value[:, side * L : side * L + L]
                for c in range(3):
                    out[q, c] = (rpos[q, pl.ds(c, 1), :] - CENTRE) * total[0:16] - total[16 + 16 * c : 32 + 16 * c]
            for side in range(0, wide, 2):
                emit(g * wide + side)

        loop(0, NN // wide, second)

    def nothing(*_):
        return None

    def scatter(phase, parts, sums):
        def emit(q):
            row_copy(phase, parts.at[q], sums, q, True).start()

            @pl.when(q + 1 < OWN)
            def _():
                row_copy(phase, parts.at[q + 1], sums, q + 1, True).start()

        return emit

    def summed(phase, parts, sums):
        for q in range(OWN):
            row_copy(phase, parts.at[q], sums, q, True).wait_recv()
        return ((sums[0] + sums[1]) + (sums[2] + sums[3])) + ((sums[4] + sums[5]) + (sums[6] + parts[OWN]))

    lane = lax.broadcasted_iota(jnp.int32, (S, L), 1)

    product(1, xg0, pb1, nothing, nothing, scatter(1, pb1, rb1))
    xg1[0] = summed(1, pb1, rb1)
    block_send(2, xg1)

    part = jnp.zeros((2 * S, L), F32)
    for c in range(3):
        a, b = xg0[0, c], xg1[0, c]
        part = part + mt(jnp.concatenate([a, b], axis=0), jnp.concatenate([a, b, b, b, b, b, b, b], axis=0))
    ga1[n] = jnp.where(lane < 32, part[0:16], part[16:32])
    narrow_send(0, ga1)

    def forward1():
        narrow_recv(0, ga1)
        gb1[w] = all_of(ga1, NN)
        wide_send(0, gb1)

    product(2, xg1, pb2, forward1, nothing, scatter(2, pb2, rb2))

    wide_recv(0, gb1)
    total = all_of(gb1, NW)
    g00, g01, g11 = total[:, 0:16], total[:, 16:32], total[:, 32:48]
    upper0, inv0 = cholesky_pair(g00)

    def inside(g):
        return mt(mm(inv0, g), inv0)

    h1, c11, k1 = inside(g01), inside(g00), inside(g11)
    f1 = h1 + (h1 - mm(c11, h1))
    f1t = transposed(f1)
    fh = mm(f1t, h1)
    gram = k1 - fh - transposed(fh) + mm(f1t, mm(c11, f1))
    y1 = summed(2, pb2, rb2)
    xg2[0] = y1
    block_send(3, xg2, HALF)
    xr[OWN] = y1
    for q in range(OWN):
        row_copy(3, xr.at[OWN], xr, q, False).start()

    upper1, inv1 = cholesky_pair(gram)
    p21t = mm(inv1, inv0)
    p20t = -mm(mm(inv1, f1t), inv0)
    for c in range(3):
        a, y0 = xg0[0, c], xg1[0, c]
        vec_ref[c, 0:16] = mm(inv0, a)
        vec_ref[c, 16:32] = mm(p20t, a) + mm(p21t, y0)
        vec_ref[c, 32:48] = mm(p20t, y0)

    part = jnp.zeros((5 * S, L), F32)
    for c in range(3):
        y0, y1c = xg1[0, c], xg2[0, c]
        q1, q2 = vec_ref[c, 0:16], vec_ref[c, 16:32]
        wv = vec_ref[c, 32:48] + mm(p21t, y1c)
        vec_ref[c, 32:48] = wv
        part = part + mt(
            jnp.concatenate([q1, q2, wv, y0, y1c], axis=0), jnp.concatenate([q1, q2, wv, q2, wv, wv, y1c, y1c], axis=0)
        )
    packed = jnp.where(lane < 48, part[0:16], part[16:32])
    packed = jnp.where(lane < 80, packed, part[32:48])
    packed = jnp.where(lane < 96, packed, part[48:64])
    ga2[n] = jnp.where(lane < 112, packed, part[64:80])
    narrow_send(1, ga2)

    def forward2():
        narrow_recv(1, ga2)
        gb2[w] = all_of(ga2, NN)
        wide_send(1, gb2)

    product(3, xg2, pz, nothing, forward2, nothing, True)
    for q in range(OWN):
        row_copy(3, xr.at[OWN], xr, q, False).wait_recv()
    part = jnp.zeros((S, S), F32)
    for c in range(3):
        part = part + mt(
            jnp.concatenate([xr[b, c] for b in range(NN)], axis=1), jnp.concatenate([pz[b, c] for b in range(NN)], axis=1)
        )
    za[n, :, 0:16] = part
    narrow_send(2, za)

    narrow_recv(2, za)
    zb[w] = all_of(za, NN)
    wide_send(2, zb)

    wide_recv(1, gb2)
    total = all_of(gb2, NW)
    c11, c12, ha, c22, hb, k, g12, g22 = [total[:, 16 * i : 16 * i + 16] for i in range(8)]
    p20, p21 = transposed(p20t), transposed(p21t)
    c12t = transposed(c12)
    fa = ha + (ha - mm(c11, ha) - mm(c12, hb))
    fb = hb + (hb - mm(c12t, ha) - mm(c22, hb))
    fat, fbt = transposed(fa), transposed(fb)
    hat, hbt = transposed(ha), transposed(hb)
    fh = mm(fat, ha) + mm(fbt, hb)
    cf = mm(fat, mm(c11, fa) + mm(c12, fb)) + mm(fbt, mm(c12t, fa) + mm(c22, fb))
    upper2, inv2 = cholesky_pair(k - fh - transposed(fh) + cf)
    zz = mm(p20t, mm(g12, p20) + mm(g22, p21)) + mm(p21t, mm(g22, p20))
    wmq1 = mm(hat, f1) + mm(hbt, upper1)
    side = mm(wmq1, fa) + mm(k, fb)
    inner = zz - side - transposed(side) + mm(fat, mm(h1, fa) + mm(ha, fb)) + mm(fbt, mm(hat, fa) + mm(hb, fb))
    a3 = mt(mm(inv2, inner), inv2)

    def sym(value):
        return 0.5 * (value + transposed(value))

    order = 3 * S
    tri = jnp.zeros((order, order), F32)
    low = [
        (lax.broadcasted_iota(jnp.int32, (order, S), 0) == lax.broadcasted_iota(jnp.int32, (order, S), 1) + S * i).astype(F32)
        for i in range(3)
    ]
    blocks = [(0, 0, sym(h1)), (1, 1, sym(hb)), (2, 2, sym(a3)), (1, 0, upper1), (2, 1, upper2)]
    blocks += [(0, 1, transposed(upper1)), (1, 2, transposed(upper2))]
    for i, j, block in blocks:
        tri = tri + mt(mm(low[i], block), low[j])
    tri_ref[...] = tri
    mix_ref[...] = mm(low[2], mm(inv2, p21t))
    low_ref[...] = transposed(upper0)
    for c in range(3):
        q1, q2, wv = vec_ref[c, 0:16], vec_ref[c, 16:32], vec_ref[c, 32:48]
        vec_ref[c, 32:48] = mm(inv2, wv - mm(fat, q1) - mm(fbt, q2))

    for phase, buffer in enumerate([cpos, xg0, xg1, xg2]):
        for p in (HALF[1:] if phase == 3 else range(1, NW)):
            block_copy(phase, buffer, p).wait_send()
    for phase, buffer in enumerate([gb1, gb2]):
        wide_sent(phase, buffer)
    for phase, buffer in enumerate([ga1, ga2, za]):
        narrow_sent(phase, buffer)
    for q in range(OWN):
        row_copy(0, cpos.at[0], rpos, q, False).wait_send()
        row_copy(1, pb1.at[q], rb1, q, True).wait_send()
        row_copy(2, pb2.at[q], rb2, q, True).wait_send()
        row_copy(3, xr.at[OWN], xr, q, False).wait_send()
    wide_recv(2, zb)
    ztot_ref[...] = all_of(zb, NW)
    wide_sent(2, zb)


def last_kernel(vec_ref, tri_ref, mix_ref, low_ref, ztot_ref, out_ref, y_ref, z_ref):
    zraw = ztot_ref[:, 0:16]
    mix = mix_ref[...]
    tri = tri_ref[...] + mt(mm(mix, 0.5 * (zraw + transposed(zraw))), mix)
    order = 3 * S
    scale = jnp.sqrt(jnp.sum(tri * tri))
    ident = eye(order)
    y_ref[...] = tri / scale
    z_ref[...] = ident

    def more(carry):
        step, gap = carry
        return jnp.logical_and(step < ROOT_STEPS, jnp.logical_not(gap < 1e-8))

    def newton(carry):
        step, _ = carry
        y, z = y_ref[...], z_ref[...]
        zy = mm(z, y)
        factor = 1.5 * ident - 0.5 * zy
        y_ref[...] = mm(y, factor)
        z_ref[...] = mm(factor, z)
        off = zy - ident
        return step + 1, jnp.sum(off * off)

    lax.while_loop(more, newton, (jnp.int32(0), jnp.float32(1.0)))
    root = y_ref[...] * jnp.sqrt(scale)
    first = (
        lax.broadcasted_iota(jnp.int32, (S, order), 0) == lax.broadcasted_iota(jnp.int32, (S, order), 1)
    ).astype(F32)
    mixing = mm(low_ref[...], mt(first, root))
    for c in range(3):
        out_ref[c] = mm(mixing, vec_ref[c])


def per_device(positions, noise):
    block = (3, S, L)
    order = 3 * S
    vmem = pl.BlockSpec(memory_space=pltpu.VMEM)
    middle = pl.pallas_call(
        main_kernel,
        out_shape=[
            jax.ShapeDtypeStruct((3, order, L), F32),
            jax.ShapeDtypeStruct((order, order), F32),
            jax.ShapeDtypeStruct((order, S), F32),
            jax.ShapeDtypeStruct((S, S), F32),
            jax.ShapeDtypeStruct((S, L), F32),
        ],
        in_specs=[pl.BlockSpec(memory_space=pl.ANY)] * 2,
        out_specs=[vmem] * 5,
        scratch_shapes=[
            pltpu.VMEM((NW, 3, L), F32),
            pltpu.VMEM((NN, 3, L), F32),
            pltpu.VMEM((NW, *block), F32),
            pltpu.VMEM((NW, *block), F32),
            pltpu.VMEM((NW, *block), F32),
            pltpu.VMEM((NN, *block), F32),
            pltpu.VMEM((NN, *block), F32),
            pltpu.VMEM((NN, *block), F32),
            pltpu.VMEM((NN, *block), F32),
            pltpu.VMEM((NN, *block), F32),
            pltpu.VMEM((NN, *block), F32),
            pltpu.VMEM((4, NN, NW * L, L), BF16),
            pltpu.VMEM((4, NN, NW * L, L), BF16),
            pltpu.VMEM((2, 4, L, NW * L // 2), BF16),
            pltpu.VMEM((NN, 64, L), F32),
            pltpu.VMEM((4, 3, L, L), F32),
            pltpu.VMEM((NN, S, L), F32),
            pltpu.VMEM((NW, S, L), F32),
            pltpu.VMEM((NN, S, L), F32),
            pltpu.VMEM((NW, S, L), F32),
            pltpu.VMEM((NN, S, L), F32),
            pltpu.VMEM((NW, S, L), F32),
            pltpu.SemaphoreType.DMA((4, NW)),
            pltpu.SemaphoreType.DMA((4, NW)),
            pltpu.SemaphoreType.DMA((3, NW)),
            pltpu.SemaphoreType.DMA((3, NW)),
            pltpu.SemaphoreType.DMA((3, NN)),
            pltpu.SemaphoreType.DMA((3, NN)),
            pltpu.SemaphoreType.DMA((4, NN)),
            pltpu.SemaphoreType.DMA((4, NN)),
            pltpu.SemaphoreType.DMA((2,)),
        ],
        compiler_params=pltpu.CompilerParams(
            collective_id=0, has_side_effects=True, vmem_limit_bytes=56 * 1024 * 1024
        ),
        name="lanczos",
    )(positions, noise)
    return pl.pallas_call(
        last_kernel,
        out_shape=jax.ShapeDtypeStruct(block, F32),
        in_specs=[vmem] * 5,
        out_specs=vmem,
        scratch_shapes=[pltpu.VMEM((order, order), F32), pltpu.VMEM((order, order), F32)],
        name="finish",
    )(*middle)


def solution(mesh):
    axes = ("wide", "narrow")
    return jax.shard_map(
        per_device,
        mesh=mesh,
        in_specs=(P(None, axes), P(None, None, axes)),
        out_specs=P(None, None, axes),
        check_vma=False,
    )
```
